32 devices in a mesh: dp: 4 (over y, core), tensor: 8 (over z, x).
Axes of the slice: x: 2, y: 2, z: 4, core: 2. Of those that a mesh axis runs over, the one named last changes fastest.
Arguments:
- tokens: bfloat16 [8192, 1024], P('dp'), may hold values from -6 to 6
- cotangent: bfloat16 [8192, 1024], P('dp'), may hold values from -6 to 6
- gain_attn: float32 [1024], replicated, may hold values from 0.1 to 1.9
- gain_moe: float32 [1024], replicated, may hold values from 0.1 to 1.9
- w_qkv: bfloat16 [1024, 3, 1024], P(None, None, 'tensor'), may hold values from -0.1875 to 0.1875
- w_out: bfloat16 [1024, 1024], P('tensor'), may hold values from -0.75 to 0.75
- rel_bias: bfloat16 [32, 16], P(None, 'tensor'), may hold values from -6 to 6
- w_router: bfloat16 [1024, 8], replicated, may hold values from -0.375 to 0.375
- w_in: bfloat16 [8, 2, 1024, 2816], P(None, None, None, 'tensor'), may hold values from -0.1875 to 0.1875
- w_down: bfloat16 [8, 2816, 1024], P(None, 'tensor'), may hold values from -0.109375 to 0.109375
- segment_ids: int32 [8, 1024], P('dp'), may hold values from 0 to 15, never falling along the last dimension, each value on 1 to 512 neighbouring positions
- routes: int32 [8192, 2], P('dp'), may hold values from 0 to 7, all different within a row
- order: int32 [4, 2048], P('dp'), may hold values from 0 to 2047, each once within a row
Outputs:
- result: float32 [8192, 1024], P('dp')
- input_grad: float32 [8192, 1024], P('dp')
- gain_attn_grad: float32 [1024], P('dp')
- gain_moe_grad: float32 [1024], P('dp')
- w_qkv_grad: float32 [1024, 3, 1024], P('dp', None, 'tensor')
- w_out_grad: float32 [1024, 1024], P('tensor', 'dp')
- rel_bias_grad: float32 [32, 16], P('dp', 'tensor')
- w_router_grad: float32 [1024, 8], P('dp')
- w_in_grad: float32 [8, 2, 1024, 2816], P(None, None, 'dp', 'tensor')
- w_down_grad: float32 [8, 2816, 1024], P(None, 'tensor', 'dp')
The draws below stay inside these ranges and needn't reach their ends.
Inputs may be any that keep to these rules, and one draw needn't show every extreme that they name: `segment_ids`: within a sequence the ids never fall; each document has at most 512 tokens. `routes`: the two experts of a token differ. `order`: each row holds every token index of its group once.
All inputs are finite; a program needn't handle non-finite values.
Results may differ from the reference program's by a relative error of at most 0.015.
The reference program's roundings to bfloat16 on the way count: a program that leaves them out, or rounds other values in their place, can miss the bound.
Values sent between devices are 32-bit elements; how exact they have to be, the bound alone decides.
A program may use at most 320 MiB of HBM per device.

```python
import math
import jax
import jax.numpy as jnp
import numpy as np
from jax import lax

D = 1024
H = 16
HD = 64
FF = 2816
NB = 32
MAXDIST = 128
EXPERTS = 8
LEN = 1024
DOCS = 16
SEQS_DEV = 2
GROUPS = 4
TOK_DEV = 2048
TOKENS = 8192
SEQS = 8
CAP = 576
HHD = 1024


def block_levels(stream_key, shape, split, low, high):
    level, own = 1.0, jax.random.fold_in(stream_key, 6)
    for dim, blocks in split:
        steps = jnp.exp(jax.random.uniform(jax.random.fold_in(own, dim), (blocks,), jnp.float32, low / len(split), high / len(split)))
        level = level * jnp.repeat(steps, shape[dim] // blocks).reshape([-1 if axis == dim else 1 for axis in range(len(shape))])
    return level


def distinct(rng, rows, count, top, lift):
    sequence = jax.random.permutation(jax.random.fold_in(rng, 1), count)
    favour = sequence
    for power in range(3):
        favour = favour * favour // count
    favour = favour * lift // count
    chance = jax.random.randint(jax.random.fold_in(rng, 2), (rows, count), 0, 4096) + favour
    holders = jax.random.permutation(jax.random.fold_in(rng, 3), rows)[jnp.arange(count) % rows]
    chance = jnp.where(jnp.arange(rows)[:, None] == holders[None, :], 1 << 14, chance)
    score = chance * count + jnp.arange(count)
    return lax.top_k(score.astype(jnp.int32), top)[1].astype(jnp.int32)


def split_up(amount, total, limit, slope):
    weights = [(1 << 20) // math.isqrt(standing ** slope) + 1 for standing in range(2, amount + 1)]
    rest, counts = total - limit - (amount - 1), [1] * (amount - 1)
    while rest > 0:
        free = [i for i in range(amount - 1) if counts[i] < limit]
        mass, budget = sum([weights[i] for i in free]), rest
        for i in free:
            addition = min(limit - counts[i], max(1, budget * weights[i] // mass), rest)
            counts[i] = counts[i] + addition
            rest = rest - addition
    return np.array([limit] + counts)


def uneven_parts(rng, number_of, total, limit, slope):
    if number_of == 2:
        one = jax.random.randint(rng, (), max(1, total - limit), min(limit, total - 1) + 1)
        return jnp.stack([one, total - one])
    sizes = jnp.asarray(split_up(number_of, total, limit, slope), jnp.int32)
    twos = (number_of - 1) // 2
    donor, receiver = sizes[1:1 + 2 * twos:2], sizes[2:2 + 2 * twos:2]
    slack = jnp.minimum(donor - 1, limit - receiver)
    passed = jax.random.randint(jax.random.fold_in(rng, 1), (twos,), 0, 1 << 20) % (slack + 1)
    sizes = sizes.at[1:1 + 2 * twos:2].set(donor - passed).at[2:2 + 2 * twos:2].set(receiver + passed)
    return sizes[jax.random.permutation(jax.random.fold_in(rng, 2), number_of)]


def noise(rng, shape, scale, bound, shards=(), held_as=jnp.bfloat16):
    drawn = scale * jax.random.normal(rng, shape, jnp.float32)
    if shards:
        drawn = drawn * block_levels(rng, shape, shards, -0.22, 0.18)
    return jnp.clip(drawn, -bound, bound).astype(held_as)


def setup_inputs(seed: int = 0) -> dict:
    key_list = jax.random.split(jax.random.key(seed), 14)
    tokens = noise(key_list[0], (TOKENS, D), 1.0, 6.0, ((0, 4),))
    cotangent = noise(key_list[1], (TOKENS, D), 1.0, 6.0, ((0, 4),))
    gain_attn = jnp.clip(1.0 + 0.18 * jax.random.normal(key_list[2], (D,), jnp.float32), 0.1, 1.9)
    gain_moe = jnp.clip(1.0 + 0.18 * jax.random.normal(key_list[3], (D,), jnp.float32), 0.1, 1.9)
    w_qkv = noise(key_list[4], (D, 3, HHD), D ** -0.5, 0.1875, ((2, 8),))
    w_out = noise(key_list[5], (HHD, D), (HHD // 16) ** -0.5, 0.75, ((0, 8),))
    rel_bias = noise(key_list[6], (NB, H), 1.0, 6.0, ((1, 8),))
    w_router = noise(key_list[7], (D, EXPERTS), (D // 4) ** -0.5, 0.375)
    w_in = noise(key_list[8], (EXPERTS, 2, D, FF), D ** -0.5, 0.1875, ((3, 8),))
    w_down = noise(key_list[9], (EXPERTS, FF, D), FF ** -0.5, 0.109375, ((1, 8),))
    segment_ids = jax.vmap(lambda own: jnp.searchsorted(jnp.cumsum(uneven_parts(own, DOCS, LEN, LEN // 2, 2)), jnp.arange(LEN), side="right"))(jax.random.split(key_list[10], SEQS)).reshape((SEQS, LEN)).astype(jnp.int32)
    routes = distinct(key_list[11], TOKENS, EXPERTS, 2, 2048)
    order = jax.vmap(lambda own: jax.random.permutation(own, TOK_DEV))(jax.random.split(key_list[12], GROUPS)).reshape((GROUPS, TOK_DEV)).astype(jnp.int32)
    return {"tokens": tokens, "cotangent": cotangent, "gain_attn": gain_attn, "gain_moe": gain_moe, "w_qkv": w_qkv, "w_out": w_out, "rel_bias": rel_bias, "w_router": w_router, "w_in": w_in, "w_down": w_down, "segment_ids": segment_ids, "routes": routes, "order": order}


@jax.custom_vjp
def low(v):
    return lax.optimization_barrier(v.astype(jnp.bfloat16)).astype(jnp.float32)

@jax.custom_vjp
def low_back(v):
    return v

def low_keep(v):
    return (low(v), None)

def low_pass(kept, grad):
    return (grad,)

def back_keep(v):
    return (v, None)

def back_low(kept, grad):
    return (low(grad),)
low.defvjp(low_keep, low_pass)
low_back.defvjp(back_keep, back_low)
EPSILON = 1e-06
PRECISE = lax.Precision.HIGHEST

def thresholds(bucket_count, reach):
    half_count = bucket_count // 2
    exact_count = half_count // 2
    listing = []
    for bucket_level in range(1, half_count):
        if bucket_level <= exact_count:
            listing.append(bucket_level)
        else:
            distance = exact_count
            while exact_count + int(np.floor(np.log(distance / exact_count) / np.log(reach / exact_count) * (half_count - exact_count))) < bucket_level:
                distance += 1
            listing.append(distance)
    return listing

def bucket_of(query_pos, key_pos):
    relative = key_pos[None, :] - query_pos[:, None]
    magnitude = jnp.abs(relative)
    bucket_ids = jnp.where(relative > 0, NB // 2, 0).astype(jnp.int32)
    for boundary in thresholds(NB, MAXDIST):
        bucket_ids = bucket_ids + (magnitude >= boundary).astype(jnp.int32)
    return bucket_ids.astype(jnp.int32)

def slot_tables(routes, order):
    tok_dev = routes.shape[0]
    ordered = jnp.take(routes, order, axis=0)
    pair_expert = jnp.concatenate([ordered[:, 0], ordered[:, 1]]).astype(jnp.int32)
    pair_token = jnp.concatenate([order, order]).astype(jnp.int32)
    pair_choice = jnp.concatenate([jnp.zeros((tok_dev,), jnp.int32), jnp.ones((tok_dev,), jnp.int32)])
    onehot = (pair_expert[:, None] == jnp.arange(EXPERTS, dtype=jnp.int32)[None, :]).astype(jnp.int32)
    before = jnp.cumsum(onehot, axis=0).astype(jnp.int32) - onehot
    position = lax.optimization_barrier(jnp.sum(before * onehot, axis=1)).astype(jnp.int32)
    target = jnp.where(position < CAP, pair_expert * CAP + position, EXPERTS * CAP).astype(jnp.int32)
    slot_token = jnp.full((EXPERTS * CAP + 1,), -1, jnp.int32).at[target].set(pair_token)[:EXPERTS * CAP]
    slot_choice = jnp.zeros((EXPERTS * CAP + 1,), jnp.int32).at[target].set(pair_choice)[:EXPERTS * CAP]
    token_target = jnp.zeros((tok_dev, 2), jnp.int32).at[pair_token, pair_choice].set(target)
    return (slot_token, slot_choice, token_target)

def rms_norm(values, gain):
    return values * lax.rsqrt(lax.optimization_barrier(jnp.mean(values * values, axis=-1, keepdims=True)) + EPSILON) * gain

def geglu(gate, upper):
    return jax.nn.gelu(gate, approximate=True) * upper

def layer_forward(inputs, gain_attn, gain_moe, w_qkv, w_out, rel_bias, w_router, w_in, w_down, segment_ids, routes, order):
    tok_dev = inputs.shape[0]
    seq_count = tok_dev // LEN
    attn_input = low(rms_norm(inputs, gain_attn))
    projected = low_back(low(jnp.einsum('td,dgn->tgn', attn_input, w_qkv, precision=PRECISE)))
    qkv_seq = projected.reshape(seq_count, LEN, 3, H, HD)
    block_rows = min(512, LEN)
    score_scale = 1.0 / math.sqrt(HD)
    positions = jnp.arange(LEN, dtype=jnp.int32)

    def attend(packed):
        qkv_one, seg_one = packed
        queries, key_vecs, value_vecs = (qkv_one[:, 0], qkv_one[:, 1], qkv_one[:, 2])

        def one_block(offset):
            query_rows = lax.dynamic_slice_in_dim(queries, offset, block_rows, 0)
            query_seg = lax.dynamic_slice_in_dim(seg_one, offset, block_rows, 0)
            query_pos = offset + jnp.arange(block_rows, dtype=jnp.int32)
            buckets = bucket_of(query_pos, positions)
            bias = jnp.transpose(rel_bias[buckets], (2, 0, 1))
            scores = jnp.einsum('qhd,khd->hqk', query_rows, key_vecs, precision=PRECISE) * score_scale + bias
            scores = jnp.where((query_seg[:, None] == seg_one[None, :])[None], scores, -1000000000.0)
            scores = low_back(scores)
            attn_probs = low(jax.nn.softmax(scores, axis=-1))
            return jnp.einsum('hqk,khd->qhd', attn_probs, value_vecs, precision=PRECISE)
        offsets = jnp.arange(0, LEN, block_rows, dtype=jnp.int32)
        pieces = lax.map(jax.checkpoint(one_block), offsets)
        return pieces.reshape(LEN, H, HD)
    attended = lax.map(attend, (qkv_seq, segment_ids))
    attended = low_back(low(attended.reshape(tok_dev, H * HD)))
    attn_out = low_back(jnp.dot(attended, w_out, precision=PRECISE))
    hidden_one = inputs + attn_out
    moe_input = low(rms_norm(hidden_one, gain_moe))
    logits = jnp.dot(moe_input, w_router, precision=PRECISE)
    router_probs = jax.nn.softmax(logits, axis=-1)
    picked = (routes[:, :, None] == jnp.arange(EXPERTS, dtype=jnp.int32)[None, None, :]).astype(router_probs.dtype)
    chosen = lax.optimization_barrier(jnp.sum(router_probs[:, None, :] * picked, axis=-1))
    pair_share = chosen / lax.optimization_barrier(jnp.sum(chosen, axis=-1, keepdims=True))
    slot_token, slot_choice, token_target = slot_tables(routes, order)
    filled = slot_token >= 0
    source_row = jnp.maximum(slot_token, 0)
    dispatched = jnp.where(filled[:, None], moe_input[source_row], 0.0).reshape(EXPERTS, CAP, D)
    gate_up = low_back(jnp.einsum('ecd,egdf->ecgf', dispatched, w_in, precision=PRECISE))
    activated = low(geglu(gate_up[:, :, 0], gate_up[:, :, 1]))
    expert_out = low_back(jnp.einsum('ecf,efd->ecd', activated, w_down, precision=PRECISE)).reshape(EXPERTS * CAP, D)
    out_rows = jnp.concatenate([expert_out, jnp.zeros((1, D), expert_out.dtype)], axis=0)
    moe_out = lax.optimization_barrier(jnp.sum(pair_share[:, :, None] * out_rows[token_target], axis=1))
    return hidden_one + moe_out

def reference(tokens, cotangent, gain_attn, gain_moe, w_qkv, w_out, rel_bias, w_router, w_in, w_down, segment_ids, routes, order):
    weights = tuple((array.astype(jnp.float32) for array in (gain_attn, gain_moe, w_qkv, w_out, rel_bias, w_router, w_in, w_down)))
    token_groups = tokens.astype(jnp.float32).reshape(GROUPS, TOK_DEV, D)
    upstream_groups = cotangent.astype(jnp.float32).reshape(GROUPS, TOK_DEV, D)
    seg_groups = segment_ids.reshape(GROUPS, SEQS_DEV, LEN)
    route_groups = routes.reshape(GROUPS, TOK_DEV, 2)

    def group_step(totals, packed):
        inputs, upstream, seg_group, route_group, order_group = packed

        def forward(inputs_in, *weights_in):
            return layer_forward(inputs_in, *weights_in, seg_group, route_group, order_group)
        result, pullback = jax.vjp(forward, inputs, *weights)
        gradients = pullback(upstream)
        totals = tuple((total + gradient for total, gradient in zip(totals, gradients[1:])))
        return (totals, (result, gradients[0]))
    initial = tuple((jnp.zeros_like(weight) for weight in weights))
    totals, (results, input_grads) = lax.scan(group_step, initial, (token_groups, upstream_groups, seg_groups, route_groups, order))
    return (results.reshape(TOKENS, D), input_grads.reshape(TOKENS, D), totals[0], totals[1], totals[2], totals[3], totals[4], totals[5], totals[6], totals[7])
```

```python
import functools
import math

import jax
import jax.numpy as jnp
import numpy as np
from jax import lax
from jax.experimental import pallas as pl
from jax.experimental.pallas import tpu as pltpu
from jax.sharding import PartitionSpec as P

F32 = jnp.float32
BF16 = jnp.bfloat16


def dot(a, b, ca, cb):
    return lax.dot_general(a, b, (((ca,), (cb,)), ((), ())), preferred_element_type=F32)


NB=32; MAXDIST=128; HD=64; NEG=-1000000000.0

def thresholds(bucket_count, reach):
    half_count = bucket_count // 2
    exact_count = half_count // 2
    listing = []
    for bucket_level in range(1, half_count):
        if bucket_level <= exact_count:
            listing.append(bucket_level)
        else:
            distance = exact_count
            while (exact_count + int(np.floor(np.log(distance / exact_count) / np.log(reach / exact_count) * (half_count - exact_count))) < bucket_level):
                distance += 1
            listing.append(distance)
    return listing

THRESH = thresholds(NB, MAXDIST)
HALF = NB // 2
CH = 128

def distance(row0, rows, cols, origin):
    r = lax.broadcasted_iota(jnp.int32, (rows, cols), 0)
    c = lax.broadcasted_iota(jnp.int32, (rows, cols), 1)
    return r + (row0 - origin) - c

def build_bias(rb_ref, bias, heads, length, block):
    total = 2 * length - block
    origin = length - block
    low_end = (origin - THRESH[-1] + 1) // CH * CH
    high_start = -(-(origin + block - 1 + THRESH[-1]) // CH) * CH
    for h in range(heads):
        bias[h, 0:low_end, :] = jnp.full((low_end, block), rb_ref[(HALF - 1) * heads + h], F32)
        bias[h, high_start:total, :] = jnp.full((total - high_start, block), rb_ref[(NB - 1) * heads + h], F32)

        def chunk(i, carry):
            row0 = pl.multiple_of(low_end + i * CH, CH)
            d = distance(row0, CH, block, origin)
            mag = jnp.abs(d)
            back = jnp.full((CH, block), rb_ref[h], F32)
            ahead = jnp.full((CH, block), rb_ref[HALF * heads + h], F32)
            for level, t in enumerate(THRESH):
                far = mag >= t
                back = jnp.where(far, rb_ref[(level + 1) * heads + h], back)
                ahead = jnp.where(far, rb_ref[(HALF + level + 1) * heads + h], ahead)
            bias[h, pl.ds(row0, CH), :] = jnp.where(d > 0, ahead, back)
            return carry
        lax.fori_loop(0, (high_start - low_end) // CH, chunk, 0)

def fwd_kernel(heads, length, block, rb_ref, q_ref, k_ref, vt_ref, segr_ref, segc_ref, o_ref, bias):
    @pl.when(pl.program_id(0) == 0)
    def _():
        build_bias(rb_ref, bias, heads, length, block)
    lanes = heads * HD
    lane = lax.broadcasted_iota(jnp.int32, (block, lanes), 1) // HD
    def step(i, carry):
        q0 = pl.multiple_of(i * block, block)
        start = pl.multiple_of(length - block - q0, block)
        qb = q_ref[pl.ds(q0, block), :] * 0.125
        same = segc_ref[...] == segr_ref[0, :, pl.ds(q0, block)]
        pieces = []
        for h in range(heads):
            qm = jnp.where(lane == h, qb, jnp.zeros_like(qb)) if heads > 1 else qb
            s = dot(k_ref[...], qm, 1, 1) + bias[h, pl.ds(start, length), :]
            s = jnp.where(same, s, NEG)
            p = jnp.exp(s - jnp.max(s, axis=0, keepdims=True))
            total = jnp.sum(p, axis=0, keepdims=True)
            p = (p * (1.0 / total)).astype(BF16)
            pieces.append(dot(vt_ref[h * HD:(h + 1) * HD, :], p, 1, 0))
        o = jnp.concatenate(pieces, axis=0) if heads > 1 else pieces[0]
        o_ref[pl.ds(q0, block), :] = o.T.astype(BF16).astype(F32)
        return carry
    lax.fori_loop(0, length // block, step, 0)

def bwd_kernel(heads, length, block, rb_ref, q_ref, k_ref, v_ref, kt_ref, do_ref, segr_ref, segc_ref,
               dq_ref, dk_ref, dv_ref, db_ref, bias, dbias, dk, dv):
    step_id = pl.program_id(0)
    total_rows = 2 * length - block
    @pl.when(step_id == 0)
    def _():
        build_bias(rb_ref, bias, heads, length, block)
        dbias[...] = jnp.zeros_like(dbias)
    dk[...] = jnp.zeros_like(dk)
    dv[...] = jnp.zeros_like(dv)
    lanes = heads * HD
    lane = lax.broadcasted_iota(jnp.int32, (block, lanes), 1) // HD
    def step(i, carry):
        q0 = pl.multiple_of(i * block, block)
        start = pl.multiple_of(length - block - q0, block)
        qb = q_ref[pl.ds(q0, block), :] * 0.125
        dob = do_ref[pl.ds(q0, block), :].astype(BF16)
        same = segc_ref[...] == segr_ref[0, :, pl.ds(q0, block)]
        pieces = []
        for h in range(heads):
            qm = jnp.where(lane == h, qb, jnp.zeros_like(qb)) if heads > 1 else qb
            dom = jnp.where(lane == h, dob, jnp.zeros_like(dob)) if heads > 1 else dob
            s = dot(k_ref[...], qm, 1, 1) + bias[h, pl.ds(start, length), :]
            s = jnp.where(same, s, NEG)
            p = jnp.exp(s - jnp.max(s, axis=0, keepdims=True))
            p = p * (1.0 / jnp.sum(p, axis=0, keepdims=True))
            dp = dot(v_ref[...], dom, 1, 1)
            ds = (p * (dp - jnp.sum(p * dp, axis=0, keepdims=True))).astype(BF16)
            dbias[h, pl.ds(start, length), :] += ds.astype(F32)
            dk[...] += dot(ds, qm, 1, 0)
            dv[...] += dot(p.astype(BF16), dom, 1, 0)
            pieces.append(dot(kt_ref[h * HD:(h + 1) * HD, :], ds, 1, 0))
        dq = jnp.concatenate(pieces, axis=0) if heads > 1 else pieces[0]
        dq_ref[pl.ds(q0, block), :] = (dq * 0.125).T.astype(BF16)
        return carry
    lax.fori_loop(0, length // block, step, 0)
    dk_ref[...] = dk[...].astype(BF16)
    dv_ref[...] = dv[...].astype(BF16)

    @pl.when(step_id == pl.num_programs(0) - 1)
    def _():
        origin = length - block
        low_end = (origin - THRESH[-1] + 1) // CH * CH
        high_start = -(-(origin + block - 1 + THRESH[-1]) // CH) * CH
        def fold(x):
            return jnp.sum(x, axis=0, keepdims=True)
        for h in range(heads):
            def rows(lo, hi):
                def body(i, acc):
                    r0 = pl.multiple_of(lo + i * CH, CH)
                    return acc + fold(dbias[h, pl.ds(r0, CH), :])
                return lax.fori_loop(0, (hi - lo) // CH, body, jnp.zeros((1, block), F32))
            def chunk(i, sums):
                r0 = pl.multiple_of(low_end + i * CH, CH)
                g = dbias[h, pl.ds(r0, CH), :]
                d = distance(r0, CH, block, origin)
                mag = jnp.abs(d)
                gb = jnp.where(d > 0, 0.0, g)
                ga = jnp.where(d > 0, g, 0.0)
                out = [sums[0] + fold(gb), sums[HALF] + fold(ga)]
                tb, ta = [], []
                for t in THRESH:
                    far = mag >= t
                    tb.append(fold(jnp.where(far, gb, 0.0)))
                    ta.append(fold(jnp.where(far, ga, 0.0)))
                new = [out[0]] + [sums[1 + n] + tb[n] for n in range(HALF - 1)]
                new += [out[1]] + [sums[HALF + 1 + n] + ta[n] for n in range(HALF - 1)]
                return tuple(new)
            sums = lax.fori_loop(0, (high_start - low_end) // CH, chunk,
                                 tuple(jnp.zeros((1, block), F32) for _ in range(NB)))
            left, right = rows(0, low_end), rows(high_start, total_rows)
            for b in range(NB):
                val = sums[b]
                if b not in (HALF - 1, NB - 1):
                    val = val - sums[b + 1]
                else:
                    val = val + (left if b == HALF - 1 else right)
                db_ref[h, b:b + 1, :] = jnp.broadcast_to(jnp.sum(val, axis=1, keepdims=True), (1, 128))

def attention_fwd(q, k, vt, seg, rb, block=256):
    tok, lanes = q.shape
    seqs, length = seg.shape
    heads = lanes // HD
    full = pl.BlockSpec((length, lanes), lambda s: (s, 0))
    return pl.pallas_call(
        functools.partial(fwd_kernel, heads, length, block),
        grid=(seqs,),
        out_shape=jax.ShapeDtypeStruct((tok, lanes), F32),
        in_specs=[pl.BlockSpec(memory_space=pltpu.SMEM), full, full,
                  pl.BlockSpec((lanes, length), lambda s: (0, s)),
                  pl.BlockSpec((1, 1, length), lambda s: (s, 0, 0)),
                  pl.BlockSpec((length, 1), lambda s: (s, 0))],
        out_specs=full,
        scratch_shapes=[pltpu.VMEM((heads, 2 * length - block, block), F32)],
        compiler_params=pltpu.CompilerParams(vmem_limit_bytes=56 << 20),
        cost_estimate=pl.CostEstimate(flops=4 * tok * length * lanes, bytes_accessed=tok * lanes * 10, transcendentals=tok * length * heads),
        name="attn_fwd",
    )(rb, q, k, vt, seg.reshape(seqs, 1, length), seg.reshape(tok, 1))

def attention_bwd(q, k, v, kt, do, seg, rb, block=256):
    tok, lanes = q.shape
    seqs, length = seg.shape
    heads = lanes // HD
    full = pl.BlockSpec((length, lanes), lambda s: (s, 0))
    sh = jax.ShapeDtypeStruct((tok, lanes), BF16)
    return pl.pallas_call(
        functools.partial(bwd_kernel, heads, length, block),
        grid=(seqs,),
        out_shape=(sh, sh, sh, jax.ShapeDtypeStruct((heads, NB, 128), F32)),
        in_specs=[pl.BlockSpec(memory_space=pltpu.SMEM), full, full, full,
                  pl.BlockSpec((lanes, length), lambda s: (0, s)), full,
                  pl.BlockSpec((1, 1, length), lambda s: (s, 0, 0)),
                  pl.BlockSpec((length, 1), lambda s: (s, 0))],
        out_specs=(full, full, full, pl.BlockSpec((heads, NB, 128), lambda s: (0, 0, 0))),
        scratch_shapes=[pltpu.VMEM((heads, 2 * length - block, block), F32)] * 2
        + [pltpu.VMEM((length, lanes), F32)] * 2,
        compiler_params=pltpu.CompilerParams(vmem_limit_bytes=56 << 20),
        cost_estimate=pl.CostEstimate(flops=10 * tok * length * lanes, bytes_accessed=tok * lanes * 20, transcendentals=tok * length * heads),
        name="attn_bwd",
    )(rb, q, k, v, kt, do, seg.reshape(seqs, 1, length), seg.reshape(tok, 1))


EXPERTS=8; CAP=576; SLOTS=EXPERTS*CAP; LN=128
GC = math.sqrt(2.0/math.pi)

def spread(dst, row0, sub, src, rows, width, dtype=None):
    for j in range(sub):
        dst[pl.ds(row0 * sub + j, rows, stride=sub), :] = src[:, j * LN:(j + 1) * LN].astype(F32)

def dispatch_kernel(tok, sub, step_slots, with_share, tgt, src, *rest):
    if with_share:
        share, out, share_out, rows_in, rows_out, share_rows = rest
    else:
        out, rows_in, rows_out = rest
    step = pl.program_id(0)
    @pl.when(step == 0)
    def _():
        def load(i, c):
            t0 = pl.multiple_of(i * 64, 64)
            spread(rows_in, t0, sub, src.at[pl.ds(t0, 64), :], 64, sub * LN)
            return c
        lax.fori_loop(0, tok // 64, load, 0)
        def zero(i, c):
            r0 = pl.multiple_of(i * 8 * sub, 8 * sub)
            rows_out[pl.ds(r0, 8 * sub), :] = jnp.zeros((8 * sub, LN), F32)
            if with_share:
                share_rows[pl.ds(pl.multiple_of(i * 8, 8), 8), :] = jnp.zeros((8, LN), F32)
            return c
        lax.fori_loop(0, SLOTS // 8, zero, 0)
        def move(i, c):
            for u in range(8):
                t = i * 8 + u
                row = rows_in[pl.ds(pl.multiple_of(t * sub, sub), sub), :]
                for choice in range(2):
                    slot = tgt[choice * tok + t]
                    rows_out[pl.ds(pl.multiple_of(slot * sub, sub), sub), :] = row
                    if with_share:
                        share_rows[pl.ds(slot, 1), :] = share[pl.ds(choice * tok + t, 1), :]
            return c
        lax.fori_loop(0, tok // 8, move, 0)
    base = step * step_slots
    def emit(i, c):
        s0 = pl.multiple_of(i * 64, 64)
        for j in range(sub):
            out[pl.ds(s0, 64), j * LN:(j + 1) * LN] = rows_out[pl.ds((base + s0) * sub + j, 64, stride=sub), :].astype(BF16)
        return c
    lax.fori_loop(0, step_slots // 64, emit, 0)
    if with_share:
        share_out[...] = share_rows[pl.ds(pl.multiple_of(base, step_slots), step_slots), :]

def dispatch(tgt, src, share=None, step_slots=512):
    tok, width = src.shape
    sub = width // LN
    ws = share is not None
    steps = SLOTS // step_slots
    whole = lambda shape: pl.BlockSpec(shape, lambda i, t: (0, 0), pipeline_mode=pl.Buffered(1))
    out_shape = [jax.ShapeDtypeStruct((SLOTS, width), BF16)]
    out_specs = [pl.BlockSpec((step_slots, width), lambda i, t: (i, 0))]
    scratch = [pltpu.VMEM((tok * sub, LN), F32), pltpu.VMEM(((SLOTS + 1) * sub, LN), F32)]
    in_specs = [whole((tok, width))]
    args = [src]
    if ws:
        in_specs.append(whole((2 * tok, LN)))
        args.append(share)
        out_shape.append(jax.ShapeDtypeStruct((SLOTS, LN), F32))
        out_specs.append(pl.BlockSpec((step_slots, LN), lambda i, t: (i, 0)))
        scratch.append(pltpu.VMEM((SLOTS + 8, LN), F32))
    r = pl.pallas_call(
        functools.partial(dispatch_kernel, tok, sub, step_slots, ws),
        grid_spec=pltpu.PrefetchScalarGridSpec(num_scalar_prefetch=1, grid=(steps,), in_specs=in_specs,
                                               out_specs=out_specs, scratch_shapes=scratch),
        out_shape=out_shape,
        compiler_params=pltpu.CompilerParams(vmem_limit_bytes=56 << 20),
        cost_estimate=pl.CostEstimate(flops=0, bytes_accessed=tok * width * 4 + SLOTS * width * 2, transcendentals=0),
        name="dispatch",
    )(tgt, *args)
    return r if ws else r[0]

def combine_rows(tgt, rows, mix, out, tok, sub, t0, count):
    def body(i, c):
        for u in range(8):
            r = i * 8 + u
            a = rows[pl.ds(pl.multiple_of(tgt[t0 + r] * sub, sub), sub), :]
            b = rows[pl.ds(pl.multiple_of(tgt[tok + t0 + r] * sub, sub), sub), :]
            mix[pl.ds(pl.multiple_of(r * sub, sub), sub), :] = a + b
        return c
    lax.fori_loop(0, count // 8, body, 0)
    for j in range(sub):
        out[:, j * LN:(j + 1) * LN] = mix[pl.ds(j, count, stride=sub), :]

def k1_kernel(tok, sub, count, tgt, x, y, sh, win, wdn, act, dgu, mi, sg, rows, sgr, mix):
    step = pl.program_id(0)
    width = sub * LN
    @pl.when(step == 0)
    def _():
        rows[SLOTS * sub:, :] = jnp.zeros((sub, LN), F32)
        sgr[SLOTS:, :] = jnp.zeros((8, LN), F32)
    @pl.when(step < EXPERTS)
    def _():
        g = dot(x[...], win[0, 0], 1, 0)
        u = dot(x[...], win[0, 1], 1, 0)
        h = dot(y[...], wdn[0], 1, 1)
        g2 = g * g
        t = jnp.tanh(GC * (g + 0.044715 * g2 * g))
        half = 0.5 * (1.0 + t)
        gel = g * half
        a = (gel * u).astype(BF16)
        act[0] = a
        sgrow = jnp.sum(a.astype(F32) * h, axis=1, keepdims=True)
        da = sh[:, 0:1] * h
        slope = half + (0.5 * GC) * g * (1.0 - t * t) * (1.0 + (3 * 0.044715) * g2)
        dg = (da * u * slope).astype(BF16)
        du = (da * gel).astype(BF16)
        dgu[0, 0] = dg
        dgu[0, 1] = du
        dx = dot(dg, win[0, 0], 1, 1) + dot(du, win[0, 1], 1, 1)
        row0 = step * CAP
        spread(rows, row0, sub, dx, CAP, width)
        sgr[pl.ds(pl.multiple_of(row0, 8), CAP), :] = jnp.broadcast_to(sgrow, (CAP, LN))
    @pl.when(step >= EXPERTS)
    def _():
        t0 = (step - EXPERTS) * count
        combine_rows(tgt, rows, mix, mi, tok, sub, t0, count)
        def body(i, c):
            for n in range(8):
                r = i * 8 + n
                for choice in range(2):
                    sg[choice, pl.ds(r, 1), :] = sgr[pl.ds(tgt[choice * tok + t0 + r], 1), :]
            return c
        lax.fori_loop(0, count // 8, body, 0)

def k1(tgt, x, y, sh, win, wdn, tok, count=256):
    width = x.shape[1]; sub = width // LN; ff = wdn.shape[1]
    e = lambda i: jnp.minimum(i, EXPERTS - 1)
    c = lambda i: jnp.maximum(i - EXPERTS, 0)
    return pl.pallas_call(
        functools.partial(k1_kernel, tok, sub, count),
        grid_spec=pltpu.PrefetchScalarGridSpec(
            num_scalar_prefetch=1, grid=(EXPERTS + tok // count,),
            in_specs=[pl.BlockSpec((CAP, width), lambda i, t: (e(i), 0)),
                      pl.BlockSpec((CAP, width), lambda i, t: (e(i), 0)),
                      pl.BlockSpec((CAP, LN), lambda i, t: (e(i), 0)),
                      pl.BlockSpec((1, 2, width, ff), lambda i, t: (e(i), 0, 0, 0)),
                      pl.BlockSpec((1, ff, width), lambda i, t: (e(i), 0, 0))],
            out_specs=[pl.BlockSpec((1, CAP, ff), lambda i, t: (e(i), 0, 0)),
                       pl.BlockSpec((1, 2, CAP, ff), lambda i, t: (e(i), 0, 0, 0)),
                       pl.BlockSpec((count, width), lambda i, t: (c(i), 0)),
                       pl.BlockSpec((2, count, LN), lambda i, t: (0, c(i), 0))],
            scratch_shapes=[pltpu.VMEM(((SLOTS + 1) * sub, LN), F32), pltpu.VMEM((SLOTS + 8, LN), F32),
                            pltpu.VMEM((count * sub, LN), F32)]),
        out_shape=[jax.ShapeDtypeStruct((EXPERTS, CAP, ff), BF16), jax.ShapeDtypeStruct((EXPERTS, 2, CAP, ff), BF16),
                   jax.ShapeDtypeStruct((tok, width), F32), jax.ShapeDtypeStruct((2, tok, LN), F32)],
        compiler_params=pltpu.CompilerParams(vmem_limit_bytes=60 << 20),
        cost_estimate=pl.CostEstimate(flops=10 * SLOTS * width * ff, bytes_accessed=60 << 20, transcendentals=SLOTS * ff),
        name="experts_back",
    )(tgt, x, y, sh, win, wdn)

def k2_kernel(tok, sub, count, parts, tgt, x, y, sh, act, dgu, wdn, dwin, dwdn, mo, rows, mix):
    step = pl.program_id(0)
    width = sub * LN
    @pl.when(step == 0)
    def _():
        rows[SLOTS * sub:, :] = jnp.zeros((sub, LN), F32)
    @pl.when(step < EXPERTS)
    def _():
        a = act[0]
        share = sh[:, 0:1]
        eo = dot(a, wdn[0], 1, 0) * share
        spread(rows, step * CAP, sub, eo, CAP, width)
        og = (y[...].astype(F32) * share).astype(BF16)
        wide = width // parts
        dd = dot(a, og, 0, 0)
        for p in range(parts):
            dwdn[p, 0] = dd[:, p * wide:(p + 1) * wide]
        for g in range(2):
            dw = dot(x[...], dgu[0, g], 0, 0)
            for p in range(parts):
                dwin[p, 0, g] = dw[p * wide:(p + 1) * wide, :]
    @pl.when(step >= EXPERTS)
    def _():
        combine_rows(tgt, rows, mix, mo, tok, sub, (step - EXPERTS) * count, count)

def k2(tgt, x, y, sh, act, dgu, wdn, tok, parts, count=256):
    width = x.shape[1]; sub = width // LN; ff = wdn.shape[1]; wide = width // parts
    e = lambda i: jnp.minimum(i, EXPERTS - 1)
    c = lambda i: jnp.maximum(i - EXPERTS, 0)
    return pl.pallas_call(
        functools.partial(k2_kernel, tok, sub, count, parts),
        grid_spec=pltpu.PrefetchScalarGridSpec(
            num_scalar_prefetch=1, grid=(EXPERTS + tok // count,),
            in_specs=[pl.BlockSpec((CAP, width), lambda i, t: (e(i), 0)),
                      pl.BlockSpec((CAP, width), lambda i, t: (e(i), 0)),
                      pl.BlockSpec((CAP, LN), lambda i, t: (e(i), 0)),
                      pl.BlockSpec((1, CAP, ff), lambda i, t: (e(i), 0, 0)),
                      pl.BlockSpec((1, 2, CAP, ff), lambda i, t: (e(i), 0, 0, 0)),
                      pl.BlockSpec((1, ff, width), lambda i, t: (e(i), 0, 0))],
            out_specs=[pl.BlockSpec((parts, 1, 2, wide, ff), lambda i, t: (0, e(i), 0, 0, 0)),
                       pl.BlockSpec((parts, 1, ff, wide), lambda i, t: (0, e(i), 0, 0)),
                       pl.BlockSpec((count, width), lambda i, t: (c(i), 0))],
            scratch_shapes=[pltpu.VMEM(((SLOTS + 1) * sub, LN), F32), pltpu.VMEM((count * sub, LN), F32)]),
        out_shape=[jax.ShapeDtypeStruct((parts, EXPERTS, 2, wide, ff), F32), jax.ShapeDtypeStruct((parts, EXPERTS, ff, wide), F32),
                   jax.ShapeDtypeStruct((tok, width), F32)],
        compiler_params=pltpu.CompilerParams(vmem_limit_bytes=60 << 20),
        cost_estimate=pl.CostEstimate(flops=8 * SLOTS * width * ff, bytes_accessed=80 << 20, transcendentals=0),
        name="experts_weights",
    )(tgt, x, y, sh, act, dgu, wdn)

def slot_targets(routes, order):
    tok = routes.shape[0]
    pos = jnp.arange(tok, dtype=jnp.int32)
    rank = jnp.sum(jnp.where(order[:, None] == pos[None, :], pos[:, None], 0), axis=0)
    earlier = (rank[:, None] > rank[None, :]).astype(BF16)
    ex = jnp.arange(EXPERTS, dtype=jnp.int32)
    onehot = (routes[:, :, None] == ex[None, None, :]).astype(BF16)
    before = dot(earlier, onehot.reshape(tok, 2 * EXPERTS), 1, 0).reshape(tok, 2, EXPERTS)
    first = jnp.sum(onehot[:, 0].astype(F32), axis=0)
    before = before + jnp.stack([jnp.zeros((EXPERTS,), F32), first])[None]
    slot = jnp.sum(before * onehot.astype(F32), axis=2).astype(jnp.int32)
    return jnp.where(slot < CAP, routes * CAP + slot, SLOTS).T.reshape(-1)


MESH = pl.DeviceIdType.MESH


class Ring:
    def __init__(self, n, rows):
        self.n = n
        self.inner = 1
        while (self.inner * 2) ** 2 <= n:
            self.inner *= 2
        self.outer = n // self.inner
        self.rows = rows
        self.rows_b = max(rows // 8 // 8 * 8, 8)
        self.rows_a = rows - self.rows_b
        self.count = next(c for c in (4, 2, 1) if self.rows_a % (8 * c) == 0)
        self.piece = self.rows_a // self.count
        self.pieces = [(p * self.piece, self.piece) for p in range(self.count)]

    def place(self):
        me = lax.axis_index("tensor")
        self.o, self.i = lax.div(me, self.inner), lax.rem(me, self.inner)

    def shard(self, back, side=0):
        return (lax.rem(self.o - back + 2 * self.outer, self.outer) * self.inner
                + lax.rem(self.i - side + self.inner, self.inner))

    def barrier(self):
        peers = [self.shard(-1)] + ([self.shard(1)] if self.outer > 2 else [])
        peers += [self.shard(0, j) for j in range(1, self.inner)]
        sem = pltpu.get_barrier_semaphore()
        for peer in peers:
            pl.semaphore_signal(sem, inc=1, device_id={"tensor": peer}, device_id_type=MESH)
        pl.semaphore_wait(sem, len(peers))

    def gather_semaphores(self):
        dma = pltpu.SemaphoreType.DMA
        one = [dma((self.outer - 1, self.count)), dma((self.inner - 1, self.outer, self.count)),
               dma((self.inner, self.outer - 1)), dma((self.inner - 1,))]
        return one + one

    def reduce_scratch(self, width):
        dma = pltpu.SemaphoreType.DMA
        one = [dma((self.inner - 1, self.outer, self.count)), dma((self.outer - 1, self.count)),
               dma((self.inner, self.outer - 1)), dma((self.inner - 1,))]
        return [pltpu.VMEM((self.inner - 1, self.outer, self.rows_a, width), F32),
                pltpu.VMEM((self.outer - 1, self.rows_a, width), F32),
                pltpu.VMEM((self.inner, self.outer - 1, self.rows_b, width), F32),
                pltpu.VMEM((self.inner - 1, self.rows_b, width), F32)] + one + one


def remote(src, dst, send, recv, peer):
    return pltpu.make_async_remote_copy(src_ref=src, dst_ref=dst, send_sem=send, recv_sem=recv,
                                        device_id={"tensor": peer}, device_id_type=MESH)


class Gather:
    def __init__(self, ring, view, own, sems):
        self.r, self.view, self.own = ring, view, own
        (self.s_oa, self.s_ia, self.s_ob, self.s_ib, self.r_oa, self.r_ia, self.r_ob, self.r_ib) = sems
        self.sent = []

    def outer_a(self, step, p):
        r = self.r
        row, rows = r.pieces[p]
        shard = r.shard(step)
        src = self.own(row, rows) if step == 0 else self.view(shard, row, rows)
        return remote(src, self.view(shard, row, rows), self.s_oa.at[step, p], self.r_oa.at[step, p], r.shard(-1))

    def inner_a(self, j, step, p):
        r = self.r
        row, rows = r.pieces[p]
        shard = r.shard(step)
        src = self.own(row, rows) if step == 0 else self.view(shard, row, rows)
        return remote(src, self.view(shard, row, rows), self.s_ia.at[j - 1, step, p], self.r_ia.at[j - 1, step, p],
                      r.shard(0, -j))

    def outer_b(self, j, step):
        r = self.r
        shard = r.shard(step, j)
        src = self.own(r.rows_a, r.rows_b) if step == 0 and j == 0 else self.view(shard, r.rows_a, r.rows_b)
        return remote(src, self.view(shard, r.rows_a, r.rows_b), self.s_ob.at[j, step], self.r_ob.at[j, step], r.shard(-1))

    def inner_b(self, j):
        r = self.r
        return remote(self.own(r.rows_a, r.rows_b), self.view(r.shard(0), r.rows_a, r.rows_b),
                      self.s_ib.at[j - 1], self.r_ib.at[j - 1], r.shard(0, -j))

    def go(self, copy):
        copy.start()
        self.sent.append(copy)

    def start_a(self, p):
        self.go(self.outer_a(0, p))
        for j in range(1, self.r.inner):
            self.go(self.inner_a(j, 0, p))

    def start_b(self):
        for j in range(1, self.r.inner):
            self.go(self.inner_b(j))
        self.go(self.outer_b(0, 0))

    def middle(self):
        r = self.r
        for j in range(1, r.inner):
            self.inner_b(j).wait_recv()
            self.go(self.outer_b(j, 0))
        for step in range(1, r.outer):
            for p in range(r.count):
                self.outer_a(step - 1, p).wait_recv()
                if step < r.outer - 1:
                    self.go(self.outer_a(step, p))
                for j in range(1, r.inner):
                    self.go(self.inner_a(j, step, p))
            for j in range(r.inner):
                self.outer_b(j, step - 1).wait_recv()
                if step < r.outer - 1:
                    self.go(self.outer_b(j, step))

    def finish(self):
        r = self.r
        for step in range(r.outer):
            for p in range(r.count):
                for j in range(1, r.inner):
                    self.inner_a(j, step, p).wait_recv()
        for copy in self.sent:
            copy.wait_send()


class Reduce:
    def __init__(self, ring, src, scratch):
        self.r, self.src = ring, src
        (self.ia, self.oa, self.ob, self.ib, self.s_ia, self.s_oa, self.s_ob, self.s_ib,
         self.r_ia, self.r_oa, self.r_ob, self.r_ib) = scratch
        self.sent = []

    def part(self, shard, row, rows):
        return self.src.at[pl.ds(pl.multiple_of(shard * self.r.rows + row, 8), rows), :]

    def inner_a(self, j, step, p):
        r = self.r
        row, rows = r.pieces[p]
        return remote(self.part(r.shard(step + 1, -j), row, rows), self.ia.at[j - 1, step, pl.ds(row, rows), :],
                      self.s_ia.at[j - 1, step, p], self.r_ia.at[j - 1, step, p], r.shard(0, -j))

    def outer_a(self, step, p):
        r = self.r
        row, rows = r.pieces[p]
        src = self.ia.at[0, 0, pl.ds(row, rows), :] if step == 0 else self.oa.at[step - 1, pl.ds(row, rows), :]
        return remote(src, self.oa.at[step, pl.ds(row, rows), :], self.s_oa.at[step, p], self.r_oa.at[step, p], r.shard(-1))

    def outer_b(self, j, step):
        r = self.r
        src = self.part(r.shard(1, j), r.rows_a, r.rows_b) if step == 0 else self.ob.at[j, step - 1]
        return remote(src, self.ob.at[j, step], self.s_ob.at[j, step], self.r_ob.at[j, step], r.shard(-1))

    def inner_b(self, j):
        r = self.r
        return remote(self.ob.at[j, r.outer - 2], self.ib.at[j - 1], self.s_ib.at[j - 1], self.r_ib.at[j - 1], r.shard(0, j))

    def go(self, copy):
        copy.start()
        self.sent.append(copy)

    def start(self):
        r = self.r
        for j in range(r.inner):
            self.go(self.outer_b(j, 0))
        for step in range(r.outer):
            for p in range(r.count):
                for j in range(1, r.inner):
                    self.go(self.inner_a(j, step, p))

    def run(self, done_a, done_b):
        r = self.r
        for step in range(r.outer):
            last = step == r.outer - 1
            for p in range(r.count):
                row, rows = r.pieces[p]
                for j in range(1, r.inner):
                    self.inner_a(j, step, p).wait_recv()
                total = self.part(r.shard(step + 1), row, rows)[...]
                for j in range(1, r.inner):
                    total = total + self.ia[j - 1, step, pl.ds(row, rows), :]
                if step == 0:
                    self.ia[0, 0, pl.ds(row, rows), :] = total
                else:
                    self.outer_a(step - 1, p).wait_recv()
                    total = total + self.oa[step - 1, pl.ds(row, rows), :]
                    if not last:
                        self.oa[step - 1, pl.ds(row, rows), :] = total
                if last:
                    done_a(p, total)
                else:
                    self.go(self.outer_a(step, p))
            if step >= 1:
                for j in range(r.inner):
                    self.outer_b(j, step - 1).wait_recv()
                    total = self.ob[j, step - 1] + self.part(r.shard(step + 1, j), r.rows_a, r.rows_b)[...]
                    self.ob[j, step - 1] = total
                    if not last:
                        self.go(self.outer_b(j, step))
                    elif j > 0:
                        self.go(self.inner_b(j))
        total = self.ob[0, r.outer - 2]
        for j in range(1, r.inner):
            self.inner_b(j).wait_recv()
            total = total + self.ib[j - 1]
        done_b(total)

    def finish(self):
        for copy in self.sent:
            copy.wait_send()


def params(cid, vmem):
    return pltpu.CompilerParams(collective_id=cid, has_side_effects=True, vmem_limit_bytes=vmem)


def gather_columns(x, n, cid):
    rows, lanes = x.shape
    ring = Ring(n, rows)
    flat = lanes % 128 == 0

    def kernel(x_ref, out, *sems):
        ring.place()
        ring.barrier()

        def view(shard, row, count):
            if flat:
                return out.at[pl.ds(row, count), pl.ds(pl.multiple_of(shard * lanes, 128), lanes)]
            return out.at[shard, pl.ds(row, count), :]

        gather = Gather(ring, view, lambda row, count: x_ref.at[pl.ds(row, count), :], sems[:8])
        keep = pltpu.make_async_copy(x_ref, view(ring.shard(0), 0, rows), sems[8])
        gather.start_b()
        for p in range(ring.count):
            gather.start_a(p)
        keep.start()
        gather.middle()
        gather.finish()
        keep.wait()

    shape = (rows, n * lanes) if flat else (n, rows, lanes)
    out = pl.pallas_call(
        kernel,
        out_shape=jax.ShapeDtypeStruct(shape, F32),
        in_specs=[pl.BlockSpec(memory_space=pltpu.VMEM)],
        out_specs=pl.BlockSpec(memory_space=pl.ANY),
        scratch_shapes=ring.gather_semaphores() + [pltpu.SemaphoreType.DMA],
        compiler_params=params(cid, 16 << 20),
        name="gather_columns",
    )(x)
    return out if flat else out.transpose(1, 0, 2).reshape(rows, n * lanes)


def reduce_rows(x, n, cid):
    total, width = x.shape
    rows = total // n
    ring = Ring(n, rows)

    def kernel(x_ref, out, *scratch):
        ring.place()
        ring.barrier()
        reduce = Reduce(ring, x_ref, scratch)
        reduce.start()

        def done_a(p, value):
            row, count = ring.pieces[p]
            out[pl.ds(row, count), :] = value

        def done_b(value):
            out[pl.ds(ring.rows_a, ring.rows_b), :] = value

        reduce.run(done_a, done_b)
        reduce.finish()

    return pl.pallas_call(
        kernel,
        out_shape=jax.ShapeDtypeStruct((rows, width), F32),
        in_specs=[pl.BlockSpec(memory_space=pltpu.VMEM)],
        out_specs=pl.BlockSpec(memory_space=pltpu.VMEM),
        scratch_shapes=ring.reduce_scratch(width),
        compiler_params=params(cid, 40 << 20),
        name="reduce_rows",
    )(x)


def reduce_norm_gather(part, values, upper, gain, n, cid):
    total, width = part.shape
    rows = total // n
    ring = Ring(n, rows)
    n_red = len(ring.reduce_scratch(width))

    def kernel(part_ref, val_ref, up_ref, gain_ref, out, gain_out, piece, keep_sem, *scratch):
        ring.place()
        ring.barrier()
        reduce = Reduce(ring, part_ref, scratch[:n_red])
        gather = Gather(ring, lambda shard, row, count: out.at[pl.ds(pl.multiple_of(shard * rows + row, 8), count), :],
                        lambda row, count: piece.at[pl.ds(row, count), :], scratch[n_red:])
        gain_out[...] = jnp.zeros_like(gain_out)
        reduce.start()

        def back(row, count, grad):
            x = val_ref[pl.ds(row, count), :]
            rr = lax.rsqrt(jnp.mean(x * x, axis=1, keepdims=True) + EPSILON)
            scaled = gain_ref[...] * grad
            inner = jnp.mean(scaled * x, axis=1, keepdims=True)
            piece[pl.ds(row, count), :] = up_ref[pl.ds(row, count), :] + rr * scaled - x * (rr * rr * rr * inner)
            gain_out[...] += jnp.sum(grad * x * rr, axis=0, keepdims=True)

        def done_a(p, value):
            row, count = ring.pieces[p]
            back(row, count, value)
            gather.start_a(p)

        def done_b(value):
            back(ring.rows_a, ring.rows_b, value)
            gather.start_b()

        reduce.run(done_a, done_b)
        keep = pltpu.make_async_copy(piece, out.at[pl.ds(pl.multiple_of(ring.shard(0) * rows, 8), rows), :], keep_sem)
        keep.start()
        gather.middle()
        gather.finish()
        reduce.finish()
        keep.wait()

    vm = pl.BlockSpec(memory_space=pltpu.VMEM)
    out, gain_part = pl.pallas_call(
        kernel,
        out_shape=(jax.ShapeDtypeStruct((total, width), F32), jax.ShapeDtypeStruct((1, width), F32)),
        in_specs=[vm] * 4,
        out_specs=(pl.BlockSpec(memory_space=pl.ANY), vm),
        scratch_shapes=[pltpu.VMEM((rows, width), F32), pltpu.SemaphoreType.DMA]
        + ring.reduce_scratch(width) + ring.gather_semaphores(),
        compiler_params=params(cid, 48 << 20),
        name="reduce_norm_gather",
    )(part, values, upper, gain.reshape(1, width))
    return out, gain_part[0]


EPSILON = 1e-06
PRECISE = lax.Precision.HIGHEST


def rms_norm(values, gain):
    return values * lax.rsqrt(jnp.mean(values * values, axis=-1, keepdims=True) + EPSILON) * gain


def rms_back(values, gain, grad):
    rr = lax.rsqrt(jnp.mean(values * values, axis=-1, keepdims=True) + EPSILON)
    scaled = gain * grad
    back = rr * scaled - values * (rr * rr * rr) * jnp.mean(scaled * values, axis=-1, keepdims=True)
    return back, jnp.sum(grad * values * rr, axis=0)


def make_shards(mesh):
    n_tensor = mesh.shape["tensor"]
    n_dp = mesh.shape["dp"]

    def shards(tokens, cotangent, gain_attn, gain_moe, w_qkv, w_out, rel_bias, w_router, w_in, w_down,
               segment_ids, routes, order):
        tok, width = tokens.shape
        lanes = w_qkv.shape[2]
        share_rows = tok // n_tensor
        row0 = lax.axis_index("tensor") * share_rows

        def halve(a):
            bit = 1
            while bit < n_dp:
                pairs = a.reshape((a.shape[0] // 2, 2) + a.shape[1:])
                side = lax.axis_index("dp") // bit % 2
                keep = lax.dynamic_index_in_dim(pairs, side, 1, keepdims=False)
                give = lax.dynamic_index_in_dim(pairs, 1 - side, 1, keepdims=False)
                a = keep + lax.ppermute(give, "dp", [(d, d ^ bit) for d in range(n_dp)])
                bit *= 2
            return a[0]

        def own(a):
            return lax.dynamic_slice_in_dim(a, row0, share_rows, 0)

        one = (order[0, 0] >= 0).astype(F32)
        w_out_all = lax.all_gather(w_out.astype(F32), "tensor", axis=0, tiled=True) * one
        x = tokens.astype(F32)
        attn_input = rms_norm(x, gain_attn).astype(BF16)
        qkv = jnp.dot(attn_input, w_qkv.reshape(width, 3 * lanes), preferred_element_type=F32).astype(BF16)
        q, k, v = (qkv[:, i * lanes:(i + 1) * lanes] for i in range(3))
        rb = rel_bias.astype(F32).reshape(-1)
        attended = attention_fwd(q, k, v.T, segment_ids, rb)
        tgt = slot_targets(routes, order[0])
        y = dispatch(tgt, cotangent)

        attended_all = gather_columns(attended, n_tensor, 0)
        hidden_one = x + jnp.dot(attended_all, w_out_all, preferred_element_type=F32)
        moe_input = rms_norm(hidden_one, gain_moe).astype(BF16)
        logits = jnp.dot(moe_input, w_router, preferred_element_type=F32)
        picked = (routes[:, :, None] == jnp.arange(EXPERTS, dtype=jnp.int32)[None, None, :]).astype(F32)

        def route(logit_rows, picked_rows):
            soft = jax.nn.softmax(logit_rows, axis=-1)
            chosen = jnp.sum(soft[:, None, :] * picked_rows, axis=-1)
            return soft, chosen, jnp.sum(chosen, axis=-1, keepdims=True)

        soft, chosen, both = route(logits, picked)
        pair_share = chosen / both
        xs, slot_share = dispatch(tgt, moe_input, jnp.broadcast_to(pair_share.T.reshape(-1, 1), (2 * tok, LN)))
        act, gate_up_grad, moe_in_part, share_part = k1(tgt, xs, y, slot_share, w_in, w_down, tok)
        w_in_local, w_down_local, moe_part = k2(tgt, xs, y, slot_share, act, gate_up_grad, w_down, tok, n_dp)

        share_grad = lax.psum_scatter(share_part[:, :, 0].T, "tensor", scatter_dimension=0, tiled=True)
        moe_in_sum = reduce_rows(moe_in_part, n_tensor, 1)
        result = hidden_one + lax.psum(moe_part, "tensor")

        soft_s, chosen_s, both_s, picked_s = own(soft), own(chosen), own(both), own(picked)
        chosen_grad = share_grad / both_s - jnp.sum(share_grad * chosen_s, axis=-1, keepdims=True) / (both_s * both_s)
        prob_grad = jnp.sum(chosen_grad[:, :, None] * picked_s, axis=1)
        logits_grad = soft_s * (prob_grad - jnp.sum(soft_s * prob_grad, axis=-1, keepdims=True))
        moe_input_s = own(moe_input)
        router_part = jnp.dot(moe_input_s.astype(F32).T, logits_grad, precision=PRECISE)
        moe_input_grad = moe_in_sum + jnp.dot(logits_grad, w_router.astype(F32).T, precision=PRECISE)
        norm_grad, gain_moe_part = rms_back(own(hidden_one), gain_moe, moe_input_grad)
        hidden_grad = own(cotangent).astype(F32) + norm_grad
        proj_grad = hidden_grad.astype(BF16)
        att_grad_s = lax.dot_general(proj_grad, w_out_all.astype(BF16), (((1,), (1,)), ((), ())), preferred_element_type=F32)
        att_grad_s = att_grad_s.astype(BF16).astype(F32)
        pieces = att_grad_s.reshape(share_rows, n_tensor, lanes).transpose(1, 0, 2)
        attended_grad = lax.all_to_all(pieces, "tensor", 0, 0, tiled=False).reshape(tok, lanes)
        w_out_part = lax.dot_general(own(attended_all).astype(BF16), proj_grad, (((0,), (0,)), ((), ())), preferred_element_type=F32)

        dq, dk, dv, bias_part = attention_bwd(q, k, v, k.T, attended_grad, segment_ids, rb)
        qkv_grad = jnp.concatenate([dq, dk, dv], axis=1)
        attn_in_part = lax.dot_general(qkv_grad, w_qkv.reshape(width, 3 * lanes), (((1,), (1,)), ((), ())), preferred_element_type=F32)
        w_qkv_part = lax.dot_general(attn_input, qkv_grad, (((0,), (0,)), ((), ())), preferred_element_type=F32)

        input_grad, gain_attn_part = reduce_norm_gather(attn_in_part, own(x), hidden_grad, gain_attn, n_tensor, 2)

        def over_dp(a, dim):
            return lax.psum_scatter(a, "dp", scatter_dimension=dim, tiled=True)

        w_in_grad = halve(w_in_local)
        w_down_grad = halve(w_down_local)
        w_qkv_grad = over_dp(w_qkv_part, 0).reshape(width // n_dp, 3, lanes)
        w_out_grad = lax.psum_scatter(over_dp(w_out_part, 1), "tensor", scatter_dimension=0, tiled=True)
        small = jnp.concatenate([gain_attn_part[:, None], gain_moe_part[:, None], router_part], axis=1)
        small = over_dp(lax.psum(small, "tensor"), 0)
        rel_bias_grad = over_dp(bias_part[:, :, 0].T, 0)
        return (result, input_grad, small[:, 0], small[:, 1], w_qkv_grad, w_out_grad, rel_bias_grad,
                small[:, 2:], w_in_grad, w_down_grad)

    return shards


def solution(mesh):
    return jax.shard_map(
        make_shards(mesh),
        mesh=mesh,
        in_specs=(
            P("dp", None),
            P("dp", None),
            P(),
            P(),
            P(None, None, "tensor"),
            P("tensor", None),
            P(None, "tensor"),
            P(),
            P(None, None, None, "tensor"),
            P(None, "tensor", None),
            P("dp", None),
            P("dp", None),
            P("dp", None),
        ),
        out_specs=(
            P("dp", None),
            P("dp", None),
            P("dp"),
            P("dp"),
            P("dp", None, "tensor"),
            P("tensor", "dp"),
            P("dp", "tensor"),
            P("dp", None),
            P(None, None, "dp", "tensor"),
            P(None, "tensor", "dp"),
        ),
        check_vma=False,
    )
```

```python
import functools
import math

import jax
import jax.numpy as jnp
import numpy as np
from jax import lax
from jax.experimental import pallas as pl
from jax.experimental.pallas import tpu as pltpu
from jax.sharding import PartitionSpec as P


F32 = jnp.float32
BF16 = jnp.bfloat16


def dot(a, b, ca, cb):
    return lax.dot_general(a, b, (((ca,), (cb,)), ((), ())), preferred_element_type=F32)


NB=32; MAXDIST=128; HD=64; NEG=-1000000000.0


def thresholds(bucket_count, reach):
    half_count = bucket_count // 2
    exact_count = half_count // 2
    listing = []
    for bucket_level in range(1, half_count):
        if bucket_level <= exact_count:
            listing.append(bucket_level)
        else:
            distance = exact_count
            while (exact_count + int(np.floor(np.log(distance / exact_count) / np.log(reach / exact_count) * (half_count - exact_count))) < bucket_level):
                distance += 1
            listing.append(distance)
    return listing


THRESH = thresholds(NB, MAXDIST)
HALF = NB // 2
CH = 128


def distance(row0, rows, cols, origin):
    r = lax.broadcasted_iota(jnp.int32, (rows, cols), 0)
    c = lax.broadcasted_iota(jnp.int32, (rows, cols), 1)
    return r + (row0 - origin) - c


def build_bias(rb_ref, bias, heads, length, block):
    total = 2 * length - block
    origin = length - block
    low_end = (origin - THRESH[-1] + 1) // CH * CH
    high_start = -(-(origin + block - 1 + THRESH[-1]) // CH) * CH
    for h in range(heads):
        bias[h, 0:low_end, :] = jnp.full((low_end, block), rb_ref[(HALF - 1) * heads + h], F32)
        bias[h, high_start:total, :] = jnp.full((total - high_start, block), rb_ref[(NB - 1) * heads + h], F32)

        def chunk(i, carry):
            row0 = pl.multiple_of(low_end + i * CH, CH)
            d = distance(row0, CH, block, origin)
            mag = jnp.abs(d)
            back = jnp.full((CH, block), rb_ref[h], F32)
            ahead = jnp.full((CH, block), rb_ref[HALF * heads + h], F32)
            for level, t in enumerate(THRESH):
                far = mag >= t
                back = jnp.where(far, rb_ref[(level + 1) * heads + h], back)
                ahead = jnp.where(far, rb_ref[(HALF + level + 1) * heads + h], ahead)
            bias[h, pl.ds(row0, CH), :] = jnp.where(d > 0, ahead, back)
            return carry

        lax.fori_loop(0, (high_start - low_end) // CH, chunk, 0)


def fwd_kernel(heads, length, block, rb_ref, q_ref, k_ref, vt_ref, segr_ref, segc_ref, o_ref, bias):
    @pl.when(pl.program_id(0) == 0)
    def _():
        build_bias(rb_ref, bias, heads, length, block)

    lanes = heads * HD
    lane = lax.broadcasted_iota(jnp.int32, (block, lanes), 1) // HD

    def step(i, carry):
        q0 = pl.multiple_of(i * block, block)
        start = pl.multiple_of(length - block - q0, block)
        qb = q_ref[pl.ds(q0, block), :] * 0.125
        same = segc_ref[...] == segr_ref[0, :, pl.ds(q0, block)]
        pieces = []
        for h in range(heads):
            qm = jnp.where(lane == h, qb, jnp.zeros_like(qb)) if heads > 1 else qb
            s = dot(k_ref[...], qm, 1, 1) + bias[h, pl.ds(start, length), :]
            s = jnp.where(same, s, NEG)
            p = jnp.exp(s - jnp.max(s, axis=0, keepdims=True))
            total = jnp.sum(p, axis=0, keepdims=True)
            p = (p * (1.0 / total)).astype(BF16)
            pieces.append(dot(vt_ref[h * HD:(h + 1) * HD, :], p, 1, 0))
        o = jnp.concatenate(pieces, axis=0) if heads > 1 else pieces[0]
        o_ref[pl.ds(q0, block), :] = o.T.astype(BF16).astype(F32)
        return carry

    lax.fori_loop(0, length // block, step, 0)


def bwd_kernel(heads, length, block, rb_ref, q_ref, k_ref, v_ref, kt_ref, do_ref, segr_ref, segc_ref,
               dq_ref, dk_ref, dv_ref, db_ref, bias, dbias, dk, dv):
    step_id = pl.program_id(0)
    total_rows = 2 * length - block

    @pl.when(step_id == 0)
    def _():
        build_bias(rb_ref, bias, heads, length, block)
        dbias[...] = jnp.zeros_like(dbias)

    dk[...] = jnp.zeros_like(dk)
    dv[...] = jnp.zeros_like(dv)
    lanes = heads * HD
    lane = lax.broadcasted_iota(jnp.int32, (block, lanes), 1) // HD

    def step(i, carry):
        q0 = pl.multiple_of(i * block, block)
        start = pl.multiple_of(length - block - q0, block)
        qb = q_ref[pl.ds(q0, block), :] * 0.125
        dob = do_ref[pl.ds(q0, block), :].astype(BF16)
        same = segc_ref[...] == segr_ref[0, :, pl.ds(q0, block)]
        pieces = []
        for h in range(heads):
            qm = jnp.where(lane == h, qb, jnp.zeros_like(qb)) if heads > 1 else qb
            dom = jnp.where(lane == h, dob, jnp.zeros_like(dob)) if heads > 1 else dob
            s = dot(k_ref[...], qm, 1, 1) + bias[h, pl.ds(start, length), :]
            s = jnp.where(same, s, NEG)
            p = jnp.exp(s - jnp.max(s, axis=0, keepdims=True))
            p = p * (1.0 / jnp.sum(p, axis=0, keepdims=True))
            dp = dot(v_ref[...], dom, 1, 1)
            ds = (p * (dp - jnp.sum(p * dp, axis=0, keepdims=True))).astype(BF16)
            dbias[h, pl.ds(start, length), :] += ds.astype(F32)
            dk[...] += dot(ds, qm, 1, 0)
            dv[...] += dot(p.astype(BF16), dom, 1, 0)
            pieces.append(dot(kt_ref[h * HD:(h + 1) * HD, :], ds, 1, 0))
        dq = jnp.concatenate(pieces, axis=0) if heads > 1 else pieces[0]
        dq_ref[pl.ds(q0, block), :] = (dq * 0.125).T.astype(BF16)
        return carry

    lax.fori_loop(0, length // block, step, 0)
    dk_ref[...] = dk[...].astype(BF16)
    dv_ref[...] = dv[...].astype(BF16)

    @pl.when(step_id == pl.num_programs(0) - 1)
    def _():
        origin = length - block
        low_end = (origin - THRESH[-1] + 1) // CH * CH
        high_start = -(-(origin + block - 1 + THRESH[-1]) // CH) * CH

        def fold(x):
            return jnp.sum(x, axis=0, keepdims=True)

        for h in range(heads):
            def rows(lo, hi):
                def body(i, acc):
                    r0 = pl.multiple_of(lo + i * CH, CH)
                    return acc + fold(dbias[h, pl.ds(r0, CH), :])

                return lax.fori_loop(0, (hi - lo) // CH, body, jnp.zeros((1, block), F32))

            def chunk(i, sums):
                r0 = pl.multiple_of(low_end + i * CH, CH)
                g = dbias[h, pl.ds(r0, CH), :]
                d = distance(r0, CH, block, origin)
                mag = jnp.abs(d)
                gb = jnp.where(d > 0, 0.0, g)
                ga = jnp.where(d > 0, g, 0.0)
                out = [sums[0] + fold(gb), sums[HALF] + fold(ga)]
                tb, ta = [], []
                for t in THRESH:
                    far = mag >= t
                    tb.append(fold(jnp.where(far, gb, 0.0)))
                    ta.append(fold(jnp.where(far, ga, 0.0)))
                new = [out[0]] + [sums[1 + n] + tb[n] for n in range(HALF - 1)]
                new += [out[1]] + [sums[HALF + 1 + n] + ta[n] for n in range(HALF - 1)]
                return tuple(new)

            sums = lax.fori_loop(0, (high_start - low_end) // CH, chunk,
                                 tuple(jnp.zeros((1, block), F32) for _ in range(NB)))
            left, right = rows(0, low_end), rows(high_start, total_rows)
            for b in range(NB):
                val = sums[b]
                if b not in (HALF - 1, NB - 1):
                    val = val - sums[b + 1]
                else:
                    val = val + (left if b == HALF - 1 else right)
                db_ref[h, b:b + 1, :] = jnp.broadcast_to(jnp.sum(val, axis=1, keepdims=True), (1, 128))


def attention_fwd(q, k, vt, seg, rb, block=256):
    tok, lanes = q.shape
    seqs, length = seg.shape
    heads = lanes // HD
    full = pl.BlockSpec((length, lanes), lambda s: (s, 0))
    return pl.pallas_call(
        functools.partial(fwd_kernel, heads, length, block),
        grid=(seqs,),
        out_shape=jax.ShapeDtypeStruct((tok, lanes), F32),
        in_specs=[pl.BlockSpec(memory_space=pltpu.SMEM), full, full,
                  pl.BlockSpec((lanes, length), lambda s: (0, s)),
                  pl.BlockSpec((1, 1, length), lambda s: (s, 0, 0)),
                  pl.BlockSpec((length, 1), lambda s: (s, 0))],
        out_specs=full,
        scratch_shapes=[pltpu.VMEM((heads, 2 * length - block, block), F32)],
        compiler_params=pltpu.CompilerParams(vmem_limit_bytes=56 << 20),
        cost_estimate=pl.CostEstimate(flops=4 * tok * length * lanes, bytes_accessed=tok * lanes * 10, transcendentals=tok * length * heads),
        name="attn_fwd",
    )(rb, q, k, vt, seg.reshape(seqs, 1, length), seg.reshape(tok, 1))


def attention_bwd(q, k, v, kt, do, seg, rb, block=256):
    tok, lanes = q.shape
    seqs, length = seg.shape
    heads = lanes // HD
    full = pl.BlockSpec((length, lanes), lambda s: (s, 0))
    sh = jax.ShapeDtypeStruct((tok, lanes), BF16)
    return pl.pallas_call(
        functools.partial(bwd_kernel, heads, length, block),
        grid=(seqs,),
        out_shape=(sh, sh, sh, jax.ShapeDtypeStruct((heads, NB, 128), F32)),
        in_specs=[pl.BlockSpec(memory_space=pltpu.SMEM), full, full, full,
                  pl.BlockSpec((lanes, length), lambda s: (0, s)), full,
                  pl.BlockSpec((1, 1, length), lambda s: (s, 0, 0)),
                  pl.BlockSpec((length, 1), lambda s: (s, 0))],
        out_specs=(full, full, full, pl.BlockSpec((heads, NB, 128), lambda s: (0, 0, 0))),
        scratch_shapes=[pltpu.VMEM((heads, 2 * length - block, block), F32)] * 2
        + [pltpu.VMEM((length, lanes), F32)] * 2,
        compiler_params=pltpu.CompilerParams(vmem_limit_bytes=56 << 20),
        cost_estimate=pl.CostEstimate(flops=10 * tok * length * lanes, bytes_accessed=tok * lanes * 20, transcendentals=tok * length * heads),
        name="attn_bwd",
    )(rb, q, k, v, kt, do, seg.reshape(seqs, 1, length), seg.reshape(tok, 1))


MESH = pl.DeviceIdType.MESH


class Ring:
    def __init__(self, n, rows):
        self.n = n
        self.inner = 1
        while (self.inner * 2) ** 2 <= n:
            self.inner *= 2
        self.outer = n // self.inner
        self.rows = rows
        self.rows_b = max(rows // 8 // 8 * 8, 8)
        self.rows_a = rows - self.rows_b
        self.count = next(c for c in (4, 2, 1) if self.rows_a % (8 * c) == 0)
        self.piece = self.rows_a // self.count
        self.pieces = [(p * self.piece, self.piece) for p in range(self.count)]

    def place(self):
        self.me = me = lax.axis_index("tensor")
        self.o, self.i = lax.div(me, self.inner), lax.rem(me, self.inner)

    def shard(self, back, side=0):
        return (lax.rem(self.o - back + 2 * self.outer, self.outer) * self.inner
                + lax.rem(self.i - side + self.inner, self.inner))

    def barrier(self, everyone=False, others=()):
        if everyone:
            peers = [{"tensor": self.peer(j)} for j in range(1, self.n)]
        else:
            peers = [self.shard(-1)] + ([self.shard(1)] if self.outer > 2 else [])
            peers += [self.shard(0, j) for j in range(1, self.inner)]
            peers = [{"tensor": p} for p in peers]
        peers += list(others)
        sem = pltpu.get_barrier_semaphore()
        for peer in peers:
            pl.semaphore_signal(sem, inc=1, device_id=peer, device_id_type=MESH)
        pl.semaphore_wait(sem, len(peers))

    def peer(self, j):
        return lax.rem(self.me + j, self.n)

    def gather_semaphores(self):
        dma = pltpu.SemaphoreType.DMA
        one = [dma((self.outer - 1, self.count)), dma((self.inner - 1, self.outer, self.count)),
               dma((self.inner, self.outer - 1)), dma((self.inner - 1,))]
        return one + one

    def reduce_scratch(self, width):
        dma = pltpu.SemaphoreType.DMA
        one = [dma((self.inner - 1, self.outer, self.count)), dma((self.outer - 1, self.count)),
               dma((self.inner, self.outer - 1)), dma((self.inner - 1,))]
        return [pltpu.VMEM((self.inner - 1, self.outer, self.rows_a, width), F32),
                pltpu.VMEM((self.outer - 1, self.rows_a, width), F32),
                pltpu.VMEM((self.inner, self.outer - 1, self.rows_b, width), F32),
                pltpu.VMEM((self.inner - 1, self.rows_b, width), F32)] + one + one


def remote(src, dst, send, recv, peer):
    return pltpu.make_async_remote_copy(src_ref=src, dst_ref=dst, send_sem=send, recv_sem=recv,
                                        device_id={"tensor": peer}, device_id_type=MESH)


class Gather:
    def __init__(self, ring, view, own, sems):
        self.r, self.view, self.own = ring, view, own
        (self.s_oa, self.s_ia, self.s_ob, self.s_ib, self.r_oa, self.r_ia, self.r_ob, self.r_ib) = sems
        self.sent = []

    def outer_a(self, step, p):
        r = self.r
        row, rows = r.pieces[p]
        shard = r.shard(step)
        src = self.own(row, rows) if step == 0 else self.view(shard, row, rows)
        return remote(src, self.view(shard, row, rows), self.s_oa.at[step, p], self.r_oa.at[step, p], r.shard(-1))

    def inner_a(self, j, step, p):
        r = self.r
        row, rows = r.pieces[p]
        shard = r.shard(step)
        src = self.own(row, rows) if step == 0 else self.view(shard, row, rows)
        return remote(src, self.view(shard, row, rows), self.s_ia.at[j - 1, step, p], self.r_ia.at[j - 1, step, p],
                      r.shard(0, -j))

    def outer_b(self, j, step):
        r = self.r
        shard = r.shard(step, j)
        src = self.own(r.rows_a, r.rows_b) if step == 0 and j == 0 else self.view(shard, r.rows_a, r.rows_b)
        return remote(src, self.view(shard, r.rows_a, r.rows_b), self.s_ob.at[j, step], self.r_ob.at[j, step], r.shard(-1))

    def inner_b(self, j):
        r = self.r
        return remote(self.own(r.rows_a, r.rows_b), self.view(r.shard(0), r.rows_a, r.rows_b),
                      self.s_ib.at[j - 1], self.r_ib.at[j - 1], r.shard(0, -j))

    def go(self, copy):
        copy.start()
        self.sent.append(copy)

    def start_a(self, p):
        self.go(self.outer_a(0, p))
        for j in range(1, self.r.inner):
            self.go(self.inner_a(j, 0, p))

    def start_b(self):
        for j in range(1, self.r.inner):
            self.go(self.inner_b(j))
        self.go(self.outer_b(0, 0))

    def middle(self):
        r = self.r
        for j in range(1, r.inner):
            self.inner_b(j).wait_recv()
            self.go(self.outer_b(j, 0))
        for step in range(1, r.outer):
            for p in range(r.count):
                self.outer_a(step - 1, p).wait_recv()
                if step < r.outer - 1:
                    self.go(self.outer_a(step, p))
                for j in range(1, r.inner):
                    self.go(self.inner_a(j, step, p))
            for j in range(r.inner):
                self.outer_b(j, step - 1).wait_recv()
                if step < r.outer - 1:
                    self.go(self.outer_b(j, step))

    def finish(self):
        r = self.r
        for step in range(r.outer):
            for p in range(r.count):
                for j in range(1, r.inner):
                    self.inner_a(j, step, p).wait_recv()
        for copy in self.sent:
            copy.wait_send()


class Reduce:
    def __init__(self, ring, src, scratch):
        self.r, self.src = ring, src
        (self.ia, self.oa, self.ob, self.ib, self.s_ia, self.s_oa, self.s_ob, self.s_ib,
         self.r_ia, self.r_oa, self.r_ob, self.r_ib) = scratch
        self.sent = []

    def part(self, shard, row, rows):
        return self.src.at[pl.ds(pl.multiple_of(shard * self.r.rows + row, 8), rows), :]

    def inner_a(self, j, step, p):
        r = self.r
        row, rows = r.pieces[p]
        return remote(self.part(r.shard(step + 1, -j), row, rows), self.ia.at[j - 1, step, pl.ds(row, rows), :],
                      self.s_ia.at[j - 1, step, p], self.r_ia.at[j - 1, step, p], r.shard(0, -j))

    def outer_a(self, step, p):
        r = self.r
        row, rows = r.pieces[p]
        src = self.ia.at[0, 0, pl.ds(row, rows), :] if step == 0 else self.oa.at[step - 1, pl.ds(row, rows), :]
        return remote(src, self.oa.at[step, pl.ds(row, rows), :], self.s_oa.at[step, p], self.r_oa.at[step, p], r.shard(-1))

    def outer_b(self, j, step):
        r = self.r
        src = self.part(r.shard(1, j), r.rows_a, r.rows_b) if step == 0 else self.ob.at[j, step - 1]
        return remote(src, self.ob.at[j, step], self.s_ob.at[j, step], self.r_ob.at[j, step], r.shard(-1))

    def inner_b(self, j):
        r = self.r
        return remote(self.ob.at[j, r.outer - 2], self.ib.at[j - 1], self.s_ib.at[j - 1], self.r_ib.at[j - 1], r.shard(0, j))

    def go(self, make, *at):
        make(*at).start()
        self.sent.append((make, at))

    def start(self):
        r = self.r
        for j in range(r.inner):
            self.go(self.outer_b, j, 0)
        for step in range(r.outer):
            for p in range(r.count):
                for j in range(1, r.inner):
                    self.go(self.inner_a, j, step, p)

    def event_a(self, step, p, done_a):
        r = self.r
        last = step == r.outer - 1
        row, rows = r.pieces[p]
        for j in range(1, r.inner):
            self.inner_a(j, step, p).wait_recv()
        total = self.part(r.shard(step + 1), row, rows)[...]
        for j in range(1, r.inner):
            total = total + self.ia[j - 1, step, pl.ds(row, rows), :]
        if step == 0:
            self.ia[0, 0, pl.ds(row, rows), :] = total
        else:
            self.outer_a(step - 1, p).wait_recv()
            total = total + self.oa[step - 1, pl.ds(row, rows), :]
            if not last:
                self.oa[step - 1, pl.ds(row, rows), :] = total
        if last:
            done_a(p, total)
        else:
            self.go(self.outer_a, step, p)

    def event_b(self, step):
        r = self.r
        for j in range(r.inner):
            self.outer_b(j, step - 1).wait_recv()
            total = self.ob[j, step - 1] + self.part(r.shard(step + 1, j), r.rows_a, r.rows_b)[...]
            self.ob[j, step - 1] = total
            if step < r.outer - 1:
                self.go(self.outer_b, j, step)
            elif j > 0:
                self.go(self.inner_b, j)

    def last_b(self, done_b):
        total = self.ob[0, self.r.outer - 2]
        for j in range(1, self.r.inner):
            self.inner_b(j).wait_recv()
            total = total + self.ib[j - 1]
        done_b(total)

    def events(self, done_a, done_b):
        r = self.r
        todo = []
        for step in range(r.outer):
            for p in range(r.count):
                todo.append(functools.partial(self.event_a, step, p, done_a))
            if step >= 1:
                todo.append(functools.partial(self.event_b, step))
        return todo + [functools.partial(self.last_b, done_b)]

    def finish(self):
        for make, at in self.sent:
            make(*at).wait_send()


def on_steps(step, events, share, last):
    done = 0
    for i in range(last):
        upto = min(int(share * (i + 1)), len(events))
        if upto > done:
            @pl.when(step == i)
            def _():
                for event in events[done:upto]:
                    event()

            done = upto

    @pl.when(step == last)
    def _():
        for event in events[done:]:
            event()


def wire(us):
    return pl.CostEstimate(flops=0, bytes_accessed=us * 3_000_000, transcendentals=0)


def params(cid, vmem):
    return pltpu.CompilerParams(collective_id=cid, has_side_effects=True, vmem_limit_bytes=vmem)


def gather_columns(x, n, cid):
    rows, lanes = x.shape
    ring = Ring(n, rows)
    flat = lanes % 128 == 0

    def kernel(x_ref, out, *sems):
        ring.place()
        ring.barrier()

        def view(shard, row, count):
            if flat:
                return out.at[pl.ds(row, count), pl.ds(pl.multiple_of(shard * lanes, 128), lanes)]
            return out.at[shard, pl.ds(row, count), :]

        gather = Gather(ring, view, lambda row, count: x_ref.at[pl.ds(row, count), :], sems[:8])
        keep = pltpu.make_async_copy(x_ref, view(ring.shard(0), 0, rows), sems[8])
        gather.start_b()
        for p in range(ring.count):
            gather.start_a(p)
        keep.start()
        gather.middle()
        gather.finish()
        keep.wait()

    shape = (rows, n * lanes) if flat else (n, rows, lanes)
    out = pl.pallas_call(
        kernel,
        out_shape=jax.ShapeDtypeStruct(shape, F32),
        in_specs=[pl.BlockSpec(memory_space=pltpu.VMEM)],
        out_specs=pl.BlockSpec(memory_space=pl.ANY),
        scratch_shapes=ring.gather_semaphores() + [pltpu.SemaphoreType.DMA],
        compiler_params=params(cid, 16 << 20),
        cost_estimate=wire(90),
        name="gather_columns",
    )(x)
    return out if flat else out.transpose(1, 0, 2).reshape(rows, n * lanes)


class Swap:
    def __init__(self, axis, n, block, got, send, recv):
        self.axis, self.n, self.block, self.got, self.send, self.recv = axis, n, block, got, send, recv

    def copy(self, j):
        me = lax.axis_index(self.axis)
        peer = lax.rem(me + j, self.n)
        return pltpu.make_async_remote_copy(
            src_ref=self.block(peer), dst_ref=self.got.at[j - 1],
            send_sem=self.send.at[j - 1], recv_sem=self.recv.at[j - 1], device_id={self.axis: peer}, device_id_type=MESH)

    def start(self):
        for j in range(1, self.n):
            self.copy(j).start()

    def total(self):
        for j in range(1, self.n):
            self.copy(j).wait()
        value = self.block(lax.axis_index(self.axis))[...]
        for j in range(1, self.n):
            value = value + self.got[j - 1]
        return value

    @staticmethod
    def scratch(n, shape):
        return [pltpu.VMEM((n - 1,) + shape, F32), pltpu.SemaphoreType.DMA((n - 1,)), pltpu.SemaphoreType.DMA((n - 1,))]


def reduce_norm_gather(part, values, upper, gain, small, keep_rows, inner_w, outer_w, n, n_dp, cid):
    total, width = part.shape
    rows = total // n
    ring = Ring(n, rows)
    n_red = len(ring.reduce_scratch(width))
    wide = width // n_dp
    s_rows = small.shape[1]
    in_rows = inner_w.shape[0] // n_dp
    height = outer_w.shape[0]
    out_rows = height // n
    columns = wide % 128 == 0
    if not columns:
        outer_w = outer_w.reshape(height, n_dp, wide).transpose(1, 0, 2)
    swaps = [(n_dp, (s_rows, wide)), (n, (s_rows, wide)), (n_dp, (in_rows, inner_w.shape[1])),
             (n_dp, (height, wide)), (n, (out_rows, wide))]

    def kernel(part_ref, val_ref, up_ref, gain_ref, small_ref, in_ref, ou_ref, out, small_out, in_out, ou_out,
               piece, sm, sm2, ou2, gain_acc, keep_sem, *scratch):
        dp = lax.axis_index("dp")
        ring.place()
        ring.barrier(everyone=True, others=[{"dp": lax.rem(dp + j, n_dp)} for j in range(1, n_dp)])
        one = Swap("dp", n_dp, lambda p: sm.at[p], *scratch[:3])
        two = Swap("tensor", n, lambda p: sm2, *scratch[3:6])
        inner_sum = Swap("dp", n_dp, lambda p: in_ref.at[pl.ds(pl.multiple_of(p * in_rows, 8), in_rows), :], *scratch[6:9])
        ou_one = Swap("dp", n_dp, (lambda p: ou_ref.at[:, pl.ds(pl.multiple_of(p * wide, 128), wide)]) if columns
                      else (lambda p: ou_ref.at[p]), *scratch[9:12])
        ou_two = Swap("tensor", n, lambda p: ou2.at[pl.ds(pl.multiple_of(p * out_rows, 8), out_rows), :], *scratch[12:15])
        reduce = Reduce(ring, part_ref, scratch[15:15 + n_red])
        gather = Gather(ring, lambda shard, row, count: out.at[pl.ds(pl.multiple_of(shard * rows + row, 8), count), :],
                        lambda row, count: piece.at[pl.ds(row, count), :], scratch[15 + n_red:])
        reduce.start()
        ou_one.start()
        inner_sum.start()
        gain_acc[...] = jnp.zeros_like(gain_acc)
        sm[...] = small_ref[...]

        def back(row, count, grad):
            x = val_ref[pl.ds(row, count), :]
            rr = lax.rsqrt(jnp.mean(x * x, axis=1, keepdims=True) + EPSILON)
            scaled = gain_ref[...] * grad
            inner = jnp.mean(scaled * x, axis=1, keepdims=True)
            piece[pl.ds(row, count), :] = up_ref[pl.ds(row, count), :] + rr * scaled - x * (rr * rr * rr * inner)
            gain_acc[...] += jnp.sum(grad * x * rr, axis=0, keepdims=True)

        def done_a(p, value):
            row, count = ring.pieces[p]
            back(row, count, value)
            gather.start_a(p)

        def done_b(value):
            back(ring.rows_a, ring.rows_b, value)
            gather.start_b()

        for event in reduce.events(done_a, done_b):
            event()
        keep = pltpu.make_async_copy(piece, out.at[pl.ds(pl.multiple_of(ring.shard(0) * rows, 8), rows), :], keep_sem)
        keep.start()
        for p in range(n_dp):
            sm[p, 0:1, :] = gain_acc[:, p * wide:(p + 1) * wide]
        one.start()
        ou2[...] = ou_one.total()
        ou_two.start()
        gather.middle()
        sm2[...] = one.total()
        two.start()
        in_out[...] = inner_sum.total()
        gather.finish()
        ou_out[...] = ou_two.total()
        both = two.total()
        last = lax.broadcasted_iota(jnp.int32, both.shape, 0) >= s_rows - keep_rows
        small_out[...] = jnp.where(last, sm2[...], both)
        reduce.finish()
        keep.wait()

    vm = pl.BlockSpec(memory_space=pltpu.VMEM)
    block = (s_rows, wide)
    return pl.pallas_call(
        kernel,
        out_shape=[jax.ShapeDtypeStruct(s, F32) for s in ((total, width), block, (in_rows, inner_w.shape[1]), (out_rows, wide))],
        in_specs=[vm] * 7,
        out_specs=[pl.BlockSpec(memory_space=pl.ANY), vm, vm, vm],
        scratch_shapes=[pltpu.VMEM((rows, width), F32), pltpu.VMEM((n_dp,) + block, F32), pltpu.VMEM(block, F32),
                        pltpu.VMEM((height, wide), F32), pltpu.VMEM((1, width), F32), pltpu.SemaphoreType.DMA]
        + [ref for swap in swaps for ref in Swap.scratch(*swap)]
        + ring.reduce_scratch(width) + ring.gather_semaphores(),
        compiler_params=params(cid, 48 << 20),
        cost_estimate=wire(180),
        name="reduce_norm_gather",
    )(part, values, upper, gain.reshape(1, width), small, inner_w, outer_w)


EXPERTS = 8
CAP = 576
SLOTS = EXPERTS * CAP
LN = 128
GC = math.sqrt(2.0 / math.pi)


def spread(dst, row0, sub, src, rows):
    for j in range(sub):
        dst[pl.ds(row0 * sub + j, rows, stride=sub), :] = src[:, j * LN:(j + 1) * LN].astype(F32)


def tile(ref, row, sub):
    return ref.at[pl.ds(pl.multiple_of(row * sub, sub), sub), :]


def dispatch_kernel(tok, sub, step_slots, with_share, tgt, src, *rest):
    if with_share:
        share, out, share_out, rows_in, rows_out, share_rows = rest
    else:
        out, rows_in, rows_out = rest
    step = pl.program_id(0)

    @pl.when(step == 0)
    def _():
        def load(i, c):
            t0 = pl.multiple_of(i * 64, 64)
            spread(rows_in, t0, sub, src.at[pl.ds(t0, 64), :], 64)
            return c

        lax.fori_loop(0, tok // 64, load, 0)

        def zero(i, c):
            r0 = pl.multiple_of(i * 8 * sub, 8 * sub)
            rows_out[pl.ds(r0, 8 * sub), :] = jnp.zeros((8 * sub, LN), F32)
            if with_share:
                share_rows[pl.ds(pl.multiple_of(i * 8, 8), 8), :] = jnp.zeros((8, LN), F32)
            return c

        lax.fori_loop(0, SLOTS // 8, zero, 0)

        def move(i, c):
            for u in range(8):
                t = i * 8 + u
                row = tile(rows_in, t, sub)[...]
                for choice in range(2):
                    slot = tgt[choice * tok + t]
                    tile(rows_out, slot, sub)[...] = row
                    if with_share:
                        share_rows[pl.ds(slot, 1), :] = share[pl.ds(choice * tok + t, 1), :]
            return c

        lax.fori_loop(0, tok // 8, move, 0)

    base = step * step_slots

    def emit(i, c):
        s0 = pl.multiple_of(i * 64, 64)
        for j in range(sub):
            out[pl.ds(s0, 64), j * LN:(j + 1) * LN] = rows_out[pl.ds((base + s0) * sub + j, 64, stride=sub), :].astype(BF16)
        return c

    lax.fori_loop(0, step_slots // 64, emit, 0)
    if with_share:
        share_out[...] = share_rows[pl.ds(pl.multiple_of(base, step_slots), step_slots), :]


def dispatch(tgt, src, share=None, step_slots=512):
    tok, width = src.shape
    sub = width // LN
    ws = share is not None

    def whole(shape):
        return pl.BlockSpec(shape, lambda i, t: (0, 0), pipeline_mode=pl.Buffered(1))

    out_shape = [jax.ShapeDtypeStruct((SLOTS, width), BF16)]
    out_specs = [pl.BlockSpec((step_slots, width), lambda i, t: (i, 0))]
    scratch = [pltpu.VMEM((tok * sub, LN), F32), pltpu.VMEM(((SLOTS + 1) * sub, LN), F32)]
    in_specs = [whole((tok, width))]
    args = [src]
    if ws:
        in_specs.append(whole((2 * tok, LN)))
        args.append(share)
        out_shape.append(jax.ShapeDtypeStruct((SLOTS, LN), F32))
        out_specs.append(pl.BlockSpec((step_slots, LN), lambda i, t: (i, 0)))
        scratch.append(pltpu.VMEM((SLOTS + 8, LN), F32))
    r = pl.pallas_call(
        functools.partial(dispatch_kernel, tok, sub, step_slots, ws),
        grid_spec=pltpu.PrefetchScalarGridSpec(num_scalar_prefetch=1, grid=(SLOTS // step_slots,), in_specs=in_specs,
                                               out_specs=out_specs, scratch_shapes=scratch),
        out_shape=out_shape,
        compiler_params=pltpu.CompilerParams(vmem_limit_bytes=56 << 20),
        cost_estimate=pl.CostEstimate(flops=0, bytes_accessed=64 << 20, transcendentals=0),
        name="dispatch",
    )(tgt, *args)
    return r if ws else r[0]


def combine_rows(tgt, rows, mix, out, tok, sub, t0, count):
    def body(i, c):
        for u in range(8):
            r = i * 8 + u
            one = rows[pl.ds(pl.multiple_of(tgt[t0 + r] * sub, sub), sub), :]
            two = rows[pl.ds(pl.multiple_of(tgt[tok + t0 + r] * sub, sub), sub), :]
            mix[pl.ds(pl.multiple_of(r * sub, sub), sub), :] = one + two
        return c

    lax.fori_loop(0, count // 8, body, 0)
    for j in range(sub):
        out[:, j * LN:(j + 1) * LN] = mix[pl.ds(j, count, stride=sub), :]


def by_expert(shape):
    return pl.BlockSpec(shape, lambda i, *t: (jnp.minimum(i, EXPERTS - 1),) + (0,) * (len(shape) - 1))


def forward_kernel(tok, sub, count, tgt, x, sh, win, wdn, gate, up, act, mo, rows, mix):
    step = pl.program_id(0)

    @pl.when(step == 0)
    def _():
        rows[SLOTS * sub:, :] = jnp.zeros((sub, LN), F32)

    @pl.when(step < EXPERTS)
    def _():
        g = dot(x[...], win[0, 0], 1, 1)
        u = dot(x[...], win[0, 1], 1, 1)
        gate[0] = g
        up[0] = u
        a = (0.5 * g * (1.0 + jnp.tanh(GC * (g + 0.044715 * (g * g * g)))) * u).astype(BF16)
        act[0] = a
        spread(rows, step * CAP, sub, dot(a, wdn[0], 1, 0) * sh[:, 0:1], CAP)

    @pl.when(step >= EXPERTS)
    def _():
        combine_rows(tgt, rows, mix, mo, tok, sub, (step - EXPERTS) * count, count)


def experts_forward(tgt, x, sh, win, wdn, tok, count=256):
    width = x.shape[1]
    sub = width // LN
    ff = wdn.shape[1]
    mid = by_expert((1, CAP, ff))
    return pl.pallas_call(
        functools.partial(forward_kernel, tok, sub, count),
        grid_spec=pltpu.PrefetchScalarGridSpec(
            num_scalar_prefetch=1, grid=(EXPERTS + tok // count,),
            in_specs=[by_expert((CAP, width)), by_expert((CAP, LN)), by_expert((1, 2, ff, width)), by_expert((1, ff, width))],
            out_specs=[mid, mid, mid, pl.BlockSpec((count, width), lambda i, t: (jnp.maximum(i - EXPERTS, 0), 0))],
            scratch_shapes=[pltpu.VMEM(((SLOTS + 1) * sub, LN), F32), pltpu.VMEM((count * sub, LN), F32)]),
        out_shape=[jax.ShapeDtypeStruct((EXPERTS, CAP, ff), F32)] * 2
        + [jax.ShapeDtypeStruct((EXPERTS, CAP, ff), BF16), jax.ShapeDtypeStruct((tok, width), F32)],
        compiler_params=pltpu.CompilerParams(vmem_limit_bytes=60 << 20),
        cost_estimate=pl.CostEstimate(flops=6 * SLOTS * width * ff, bytes_accessed=100 << 20, transcendentals=SLOTS * ff),
        name="experts_forward",
    )(tgt, x, sh, win, wdn)


def backward_kernel(tok, chunk, ring, share, cot, tgt_row, tgt_col, sh, gate, up, act, win, wdn, part, hid,
                    y, dgu, mi, sg, res, acc, acc_sem, *scratch):
    step = pl.program_id(0)
    width = cot.shape[1]
    first = step * CAP
    ring.place()
    reduce = Reduce(ring, part, scratch)

    @pl.when(step == 0)
    def _():
        ring.barrier()
        reduce.start()
        acc[...] = jnp.zeros_like(acc)
        sg[...] = jnp.zeros_like(sg)

    slot = lax.broadcasted_iota(jnp.int32, (CAP, chunk), 0) + first

    def fetch(i, rows):
        t0 = pl.multiple_of(i * chunk, chunk)
        held = (tgt_row[0:1, pl.ds(t0, chunk)] == slot) | (tgt_row[1:2, pl.ds(t0, chunk)] == slot)
        return rows + dot(jnp.where(held, 1.0, 0.0).astype(BF16), cot[pl.ds(t0, chunk), :], 1, 0)

    rows = lax.fori_loop(0, tok // chunk, fetch, jnp.zeros((CAP, width), F32)).astype(BF16)
    y[...] = rows
    h = dot(rows, wdn[0], 1, 1)
    g, u = gate[0], up[0]
    g2 = g * g
    t = jnp.tanh(GC * (g + 0.044715 * g2 * g))
    half = 0.5 * (1.0 + t)
    sgrow = jnp.sum(act[0].astype(F32) * h, axis=1, keepdims=True)
    da = sh[:, 0:1] * h
    slope = half + (0.5 * GC) * g * (1.0 - t * t) * (1.0 + (3 * 0.044715) * g2)
    dg = (da * u * slope).astype(BF16)
    du = (da * (g * half)).astype(BF16)
    dgu[0, 0] = dg
    dgu[0, 1] = du
    dx = (dot(dg, win[0, 0], 1, 0) + dot(du, win[0, 1], 1, 0)).astype(BF16)
    lane = lax.broadcasted_iota(jnp.int32, (CAP, LN), 1)
    high = sgrow.astype(BF16).astype(F32)
    aux = jnp.where(lane == 0, high, jnp.where(lane == 1, sgrow - high, 0.0)).astype(BF16)
    slots = lax.broadcasted_iota(jnp.int32, (chunk, CAP), 1) + first
    lanes = lax.broadcasted_iota(jnp.int32, (chunk, LN), 1)

    def hand_back(i, c):
        t0 = pl.multiple_of(i * chunk, chunk)
        one, two = tgt_col[pl.ds(t0, chunk), 0:1], tgt_col[pl.ds(t0, chunk), 1:2]
        held = jnp.where((one == slots) | (two == slots), 1.0, 0.0).astype(BF16)
        acc[pl.ds(t0, chunk), :] += dot(held, dx, 1, 0)
        value = dot(held, aux, 1, 0)
        value = value[:, 0:1] + value[:, 1:2]
        pair = jnp.where(lanes == 0, one, jnp.where(lanes == 1, two, SLOTS))
        sg[pl.ds(t0, chunk), :] += jnp.where((pair >= first) & (pair < first + CAP), value, 0.0)
        return c

    lax.fori_loop(0, tok // chunk, hand_back, 0)

    def done_a(p, value):
        row, n = ring.pieces[p]
        res[pl.ds(row, n), :] = value + hid[pl.ds(row, n), :]

    def done_b(value):
        res[pl.ds(ring.rows_a, ring.rows_b), :] = value + hid[pl.ds(ring.rows_a, ring.rows_b), :]

    @pl.when(step == EXPERTS - 1)
    def _():
        pltpu.make_async_copy(acc, mi, acc_sem).start()

    on_steps(step, reduce.events(done_a, done_b), share, EXPERTS - 1)

    @pl.when(step == EXPERTS - 1)
    def _():
        pltpu.make_async_copy(acc, mi, acc_sem).wait()
        reduce.finish()


def whole(shape):
    return pl.BlockSpec(shape, lambda i, *t: (0,) * len(shape), pipeline_mode=pl.Buffered(1))


def experts_backward(tgt, cot, sh, gate, up, act, win, wdn, part, hid, n, cid, chunk=512, share=1.6):
    tok, width = part.shape
    ff = wdn.shape[1]
    ring = Ring(n, tok // n)
    mid = by_expert((1, CAP, ff))
    tgt_row = tgt.reshape(2, tok)
    return pl.pallas_call(
        functools.partial(backward_kernel, tok, chunk, ring, share),
        grid=(EXPERTS,),
        in_specs=[whole(cot.shape), whole((2, tok)), whole((tok, 2)), by_expert((CAP, LN)), mid, mid, mid,
                  by_expert((1, 2, ff, width)), by_expert((1, ff, width)), whole(part.shape), whole(hid.shape)],
        out_specs=[by_expert((CAP, width)), by_expert((1, 2, CAP, ff)), pl.BlockSpec(memory_space=pl.ANY),
                   pl.BlockSpec((tok, LN), lambda i: (0, 0)), pl.BlockSpec(hid.shape, lambda i: (0, 0))],
        scratch_shapes=[pltpu.VMEM((tok, width), F32), pltpu.SemaphoreType.DMA] + ring.reduce_scratch(width),
        out_shape=[jax.ShapeDtypeStruct((SLOTS, width), BF16), jax.ShapeDtypeStruct((EXPERTS, 2, CAP, ff), BF16),
                   jax.ShapeDtypeStruct((tok, width), F32), jax.ShapeDtypeStruct((tok, LN), F32),
                   jax.ShapeDtypeStruct(hid.shape, F32)],
        compiler_params=params(cid, 63 << 20),
        cost_estimate=wire(90),
        name="experts_backward",
    )(cot, tgt_row, tgt_row.T, sh, gate, up, act, win, wdn, part, hid)


def exclusive_or(a, b, bound):
    value, bit = 0, 1
    while bit < bound:
        value = value + lax.rem(lax.div(a, bit) + lax.div(b, bit), 2) * bit
        bit *= 2
    return value


def weights_kernel(parts, ring, n, share, x, y, sh, act, dgu, part, small, keep, give, out, small_out,
                   kept, gave, got, g_send, g_recv, sw_got, sw_send, sw_recv, *scratch):
    step = pl.program_id(0)
    dp = lax.axis_index("dp")
    mine = lax.rem(dp, 2)
    upper = lax.div(dp, 2)
    blocks = parts // 2
    half = blocks // 2
    ring.place()
    reduce = Reduce(ring, part, scratch)
    swap = Swap("tensor", n, lambda p: small.at[p], sw_got, sw_send, sw_recv)

    def to_partner(slot):
        return pltpu.make_async_remote_copy(
            src_ref=gave.at[slot], dst_ref=got.at[slot], send_sem=g_send.at[slot], recv_sem=g_recv.at[slot],
            device_id={"dp": dp + 1 - 2 * mine}, device_id_type=MESH)

    @pl.when(step == 0)
    def _():
        ring.barrier(everyone=True, others=[{"dp": dp + 1 - 2 * mine}])
        swap.start()
        reduce.start()

    @pl.when(step >= 1)
    def _():
        slot = lax.rem(step + 1, 2)
        to_partner(slot).wait()
        for q in range(blocks):
            to = exclusive_or(q, upper, blocks)

            @pl.when(to < half)
            def _():
                keep[to, 0] = kept[slot, q] + got[slot, q]

            @pl.when(to >= half)
            def _():
                give[to - half, 0] = kept[slot, q] + got[slot, q]

    @pl.when(step < EXPERTS)
    def _():
        slot = lax.rem(step, 2)
        og = (y[...].astype(F32) * sh[:, 0:1]).astype(BF16)
        wide = x.shape[1] // parts
        grads = [dot(dgu[0, 0], x[...], 0, 0), dot(dgu[0, 1], x[...], 0, 0), dot(act[0], og, 0, 0)]
        for bit in range(2):
            @pl.when(mine == bit)
            def _():
                for p in range(parts):
                    to = kept if p % 2 == bit else gave
                    for g in range(3):
                        to[slot, p // 2, g] = grads[g][:, p * wide:(p + 1) * wide]
        to_partner(slot).start()

    def done_a(p, value):
        row, count = ring.pieces[p]
        out[pl.ds(row, count), :] = value

    def done_b(value):
        out[pl.ds(ring.rows_a, ring.rows_b), :] = value

    on_steps(step, reduce.events(done_a, done_b), share, EXPERTS)

    @pl.when(step == EXPERTS)
    def _():
        small_out[...] = swap.total()
        reduce.finish()


def experts_weights(x, y, sh, act, dgu, part, small, n, parts, cid, share=1.3):
    tok, width = part.shape
    ff = act.shape[2]
    wide = width // parts
    ring = Ring(n, tok // n)
    half = parts // 4
    o_w = jax.ShapeDtypeStruct((half, EXPERTS, 3, ff, wide), F32)
    b_w = pl.BlockSpec((half, 1, 3, ff, wide), lambda i, *t: (0, jnp.maximum(i - 1, 0), 0, 0, 0))
    slots = pltpu.VMEM((2, parts // 2, 3, ff, wide), F32)
    dma = pltpu.SemaphoreType.DMA
    return pl.pallas_call(
        functools.partial(weights_kernel, parts, ring, n, share),
        grid=(EXPERTS + 1,),
        in_specs=[by_expert((CAP, width)), by_expert((CAP, width)), by_expert((CAP, LN)),
                  by_expert((1, CAP, ff)), by_expert((1, 2, CAP, ff)), whole(part.shape), whole(small.shape)],
        out_specs=[b_w, b_w, pl.BlockSpec((tok // n, width), lambda i: (0, 0)),
                   pl.BlockSpec(small.shape[1:], lambda i: (0, 0))],
        scratch_shapes=[slots, slots, slots, dma((2,)), dma((2,))]
        + Swap.scratch(n, small.shape[1:]) + ring.reduce_scratch(width),
        out_shape=[o_w, o_w, jax.ShapeDtypeStruct((tok // n, width), F32), jax.ShapeDtypeStruct(small.shape[1:], F32)],
        compiler_params=params(cid, 63 << 20),
        cost_estimate=wire(90),
        name="experts_weights",
    )(x, y, sh, act, dgu, part, small)


def slot_targets(routes, order):
    tok = routes.shape[0]
    pos = jnp.arange(tok, dtype=jnp.int32)
    rank = jnp.sum(jnp.where(order[:, None] == pos[None, :], pos[:, None], 0), axis=0)
    earlier = (rank[:, None] > rank[None, :]).astype(BF16)
    ex = jnp.arange(EXPERTS, dtype=jnp.int32)
    onehot = (routes[:, :, None] == ex[None, None, :]).astype(BF16)
    before = dot(earlier, onehot.reshape(tok, 2 * EXPERTS), 1, 0).reshape(tok, 2, EXPERTS)
    first = jnp.sum(onehot[:, 0].astype(F32), axis=0)
    before = before + jnp.stack([jnp.zeros((EXPERTS,), F32), first])[None]
    slot = jnp.sum(before * onehot.astype(F32), axis=2).astype(jnp.int32)
    return jnp.where(slot < CAP, routes * CAP + slot, SLOTS).T.reshape(-1)


EPSILON = 1e-06
PRECISE = lax.Precision.HIGHEST


def rms_norm(values, gain):
    return values * lax.rsqrt(jnp.mean(values * values, axis=-1, keepdims=True) + EPSILON) * gain


def rms_back(values, gain, grad):
    rr = lax.rsqrt(jnp.mean(values * values, axis=-1, keepdims=True) + EPSILON)
    scaled = gain * grad
    back = rr * scaled - values * (rr * rr * rr) * jnp.mean(scaled * values, axis=-1, keepdims=True)
    return back, jnp.sum(grad * values * rr, axis=0)


def make_shards(mesh):
    n_tensor = mesh.shape["tensor"]
    n_dp = mesh.shape["dp"]

    def layer(tokens, cotangent, gain_attn, gain_moe, w_qkv, w_out, rel_bias, w_router, w_in, w_down,
              segment_ids, routes, order):
        tok, width = tokens.shape
        lanes = w_qkv.shape[2]
        share_rows = tok // n_tensor
        row0 = lax.axis_index("tensor") * share_rows

        def halve(keep, give):
            while True:
                blocks = keep.shape[0]
                came = lax.ppermute(give, "dp", [(d, d ^ (2 * blocks)) for d in range(n_dp)])
                if blocks == 1:
                    return keep[0], came[0]
                a = keep + came
                keep, give = a[:blocks // 2], a[blocks // 2:]

        def own(a):
            return lax.dynamic_slice_in_dim(a, row0, share_rows, 0)

        one = (order[0, 0] >= 0).astype(F32)
        w_out_cols = lax.dynamic_slice_in_dim(w_out, lax.axis_index("dp") * (width // n_dp), width // n_dp, 1).astype(F32)
        w_out_rows = lax.all_gather(w_out_cols, "tensor", axis=0, tiled=True)
        x = tokens.astype(F32)
        attn_input = rms_norm(x, gain_attn).astype(BF16)
        qkv = jnp.dot(attn_input, w_qkv.reshape(width, 3 * lanes), preferred_element_type=F32).astype(BF16)
        q, k, v = (qkv[:, i * lanes:(i + 1) * lanes] for i in range(3))
        rb = rel_bias.astype(F32).reshape(-1)
        attended = attention_fwd(q, k, v.T, segment_ids, rb)
        tgt = slot_targets(routes, order[0])

        attended, w_out_rows = lax.optimization_barrier((attended, w_out_rows))
        w_out_all = lax.all_gather(w_out_rows, "dp", axis=1, tiled=True) * one
        attended_all = gather_columns(attended, n_tensor, 0)
        hidden_one = x + jnp.dot(attended_all, w_out_all, preferred_element_type=F32)
        moe_input = rms_norm(hidden_one, gain_moe).astype(BF16)
        logits = jnp.dot(moe_input, w_router, preferred_element_type=F32)
        picked = (routes[:, :, None] == jnp.arange(EXPERTS, dtype=jnp.int32)[None, None, :]).astype(F32)

        def route(logit_rows, picked_rows):
            soft = jax.nn.softmax(logit_rows, axis=-1)
            chosen = jnp.sum(soft[:, None, :] * picked_rows, axis=-1)
            return soft, chosen, jnp.sum(chosen, axis=-1, keepdims=True)

        soft, chosen, both = route(logits, picked)
        pair_share = chosen / both
        xs, slot_share = dispatch(tgt, moe_input, jnp.broadcast_to(pair_share.T.reshape(-1, 1), (2 * tok, LN)))
        w_in_t = jnp.swapaxes(w_in, 2, 3)
        gate, up, act, moe_part = experts_forward(tgt, xs, slot_share, w_in_t, w_down, tok)
        hidden_s = own(hidden_one)
        y, gate_up_grad, moe_in_part, share_part, result_s = experts_backward(
            tgt, cotangent, slot_share, gate, up, act, w_in_t, w_down, moe_part, hidden_s, n_tensor, 1)
        share_blocks = jnp.pad(share_part[:, :2].T.reshape(2, n_tensor, share_rows).transpose(1, 0, 2), ((0, 0), (0, 6), (0, 0)))
        keep, give, moe_in_sum, share_sum = experts_weights(
            xs, y, slot_share, act, gate_up_grad, moe_in_part, share_blocks, n_tensor, n_dp, 3)
        keep, came = halve(keep, give)
        share_grad = share_sum[0:2].T
        result_s, moe_in_sum = lax.optimization_barrier((result_s, moe_in_sum))
        result = lax.all_gather(result_s, "tensor", axis=0, tiled=True)

        soft_s, chosen_s, both_s, picked_s = own(soft), own(chosen), own(both), own(picked)
        chosen_grad = share_grad / both_s - jnp.sum(share_grad * chosen_s, axis=-1, keepdims=True) / (both_s * both_s)
        prob_grad = jnp.sum(chosen_grad[:, :, None] * picked_s, axis=1)
        logits_grad = soft_s * (prob_grad - jnp.sum(soft_s * prob_grad, axis=-1, keepdims=True))
        moe_input_s = own(moe_input)
        router_part = jnp.dot(moe_input_s.astype(F32).T, logits_grad, precision=PRECISE)
        moe_input_grad = moe_in_sum + jnp.dot(logits_grad, w_router.astype(F32).T, precision=PRECISE)
        norm_grad, gain_moe_part = rms_back(hidden_s, gain_moe, moe_input_grad)
        hidden_grad = own(cotangent).astype(F32) + norm_grad
        proj_grad = hidden_grad.astype(BF16)
        att_grad_s = lax.dot_general(proj_grad, w_out_all.astype(BF16), (((1,), (1,)), ((), ())), preferred_element_type=F32)
        att_grad_s = att_grad_s.astype(BF16).astype(F32)
        pieces = att_grad_s.reshape(share_rows, n_tensor, lanes).transpose(1, 0, 2)
        attended_grad = lax.all_to_all(pieces, "tensor", 0, 0, tiled=False).reshape(tok, lanes)
        w_out_part = lax.dot_general(own(attended_all).astype(BF16), proj_grad, (((0,), (0,)), ((), ())), preferred_element_type=F32)

        dq, dk, dv, bias_part = attention_bwd(q, k, v, k.T, attended_grad, segment_ids, rb)
        qkv_grad = jnp.concatenate([dq, dk, dv], axis=1)
        attn_in_part = lax.dot_general(qkv_grad, w_qkv.reshape(width, 3 * lanes), (((1,), (1,)), ((), ())), preferred_element_type=F32)
        w_qkv_part = lax.dot_general(attn_input, qkv_grad, (((0,), (0,)), ((), ())), preferred_element_type=F32)

        heads = lanes // HD
        wide = width // n_dp
        bias_rows = bias_part[:, :, 0].reshape(heads, n_dp, NB // n_dp).transpose(1, 0, 2)
        bias_rows = jnp.pad(bias_rows, ((0, 0), (0, 0), (0, wide - NB // n_dp)))
        sums = jnp.concatenate([jnp.zeros((1, width), F32), gain_moe_part[None], router_part.T], axis=0)
        sums = sums.reshape(sums.shape[0], n_dp, wide).transpose(1, 0, 2)
        small = jnp.concatenate([sums, jnp.zeros((n_dp, -(sums.shape[1] + heads) % 8, wide), F32), bias_rows], axis=1)
        input_grad, small, w_qkv_grad, w_out_grad = reduce_norm_gather(
            attn_in_part, own(tokens).astype(F32), hidden_grad, gain_attn, small, heads, w_qkv_part, w_out_part, n_tensor, n_dp, 2)

        small, keep = lax.optimization_barrier((small, keep))
        w_in_grad = jnp.swapaxes(keep[:, :2] + came[:, :2], 2, 3)
        w_down_grad = keep[:, 2] + came[:, 2]
        w_qkv_grad = w_qkv_grad.reshape(width // n_dp, 3, lanes)
        rel_bias_grad = small[small.shape[0] - heads:, :NB // n_dp].T
        return (result, input_grad, small[0], small[1], w_qkv_grad, w_out_grad, rel_bias_grad,
                small[2:2 + EXPERTS].T, w_in_grad, w_down_grad)

    return layer


def solution(mesh):
    return jax.shard_map(
        make_shards(mesh),
        mesh=mesh,
        in_specs=(
            P("dp", None),
            P("dp", None),
            P(),
            P(),
            P(None, None, "tensor"),
            P("tensor", None),
            P(None, "tensor"),
            P(),
            P(None, None, None, "tensor"),
            P(None, "tensor", None),
            P("dp", None),
            P("dp", None),
            P("dp", None),
        ),
        out_specs=(
            P("dp", None),
            P("dp", None),
            P("dp"),
            P("dp"),
            P("dp", None, "tensor"),
            P("tensor", "dp"),
            P("dp", "tensor"),
            P("dp", None),
            P(None, None, "dp", "tensor"),
            P(None, "tensor", "dp"),
        ),
        check_vma=False,
    )
```

```python
import functools
import math

import jax
import jax.numpy as jnp
import numpy as np
from jax import lax
from jax.experimental import pallas as pl
from jax.experimental.pallas import tpu as pltpu
from jax.sharding import PartitionSpec as P


F32 = jnp.float32
BF16 = jnp.bfloat16


def dot(a, b, ca, cb):
    return lax.dot_general(a, b, (((ca,), (cb,)), ((), ())), preferred_element_type=F32)


NB=32; MAXDIST=128; HD=64; NEG=-1000000000.0


def thresholds(bucket_count, reach):
    half_count = bucket_count // 2
    exact_count = half_count // 2
    listing = []
    for bucket_level in range(1, half_count):
        if bucket_level <= exact_count:
            listing.append(bucket_level)
        else:
            distance = exact_count
            while (exact_count + int(np.floor(np.log(distance / exact_count) / np.log(reach / exact_count) * (half_count - exact_count))) < bucket_level):
                distance += 1
            listing.append(distance)
    return listing


THRESH = thresholds(NB, MAXDIST)
HALF = NB // 2
CH = 128


def distance(row0, rows, cols, origin):
    r = lax.broadcasted_iota(jnp.int32, (rows, cols), 0)
    c = lax.broadcasted_iota(jnp.int32, (rows, cols), 1)
    return r + (row0 - origin) - c


def build_bias(rb_ref, bias, heads, length, block):
    total = 2 * length - block
    origin = length - block
    low_end = (origin - THRESH[-1] + 1) // CH * CH
    high_start = -(-(origin + block - 1 + THRESH[-1]) // CH) * CH
    for h in range(heads):
        bias[h, 0:low_end, :] = jnp.full((low_end, block), rb_ref[(HALF - 1) * heads + h], F32)
        bias[h, high_start:total, :] = jnp.full((total - high_start, block), rb_ref[(NB - 1) * heads + h], F32)

        def chunk(i, carry):
            row0 = pl.multiple_of(low_end + i * CH, CH)
            d = distance(row0, CH, block, origin)
            mag = jnp.abs(d)
            back = jnp.full((CH, block), rb_ref[h], F32)
            ahead = jnp.full((CH, block), rb_ref[HALF * heads + h], F32)
            for level, t in enumerate(THRESH):
                far = mag >= t
                back = jnp.where(far, rb_ref[(level + 1) * heads + h], back)
                ahead = jnp.where(far, rb_ref[(HALF + level + 1) * heads + h], ahead)
            bias[h, pl.ds(row0, CH), :] = jnp.where(d > 0, ahead, back)
            return carry

        lax.fori_loop(0, (high_start - low_end) // CH, chunk, 0)


def fwd_kernel(heads, length, block, rb_ref, q_ref, k_ref, vt_ref, segr_ref, segc_ref, o_ref, bias):
    @pl.when(pl.program_id(0) == 0)
    def _():
        build_bias(rb_ref, bias, heads, length, block)

    lanes = heads * HD
    lane = lax.broadcasted_iota(jnp.int32, (block, lanes), 1) // HD

    def step(i, carry):
        q0 = pl.multiple_of(i * block, block)
        start = pl.multiple_of(length - block - q0, block)
        qb = q_ref[pl.ds(q0, block), :] * 0.125
        same = segc_ref[...] == segr_ref[0, :, pl.ds(q0, block)]
        pieces = []
        for h in range(heads):
            qm = jnp.where(lane == h, qb, jnp.zeros_like(qb)) if heads > 1 else qb
            s = dot(k_ref[...], qm, 1, 1) + bias[h, pl.ds(start, length), :]
            s = jnp.where(same, s, NEG)
            p = jnp.exp(s - jnp.max(s, axis=0, keepdims=True))
            total = jnp.sum(p, axis=0, keepdims=True)
            p = (p * (1.0 / total)).astype(BF16)
            pieces.append(dot(vt_ref[h * HD:(h + 1) * HD, :], p, 1, 0))
        o = jnp.concatenate(pieces, axis=0) if heads > 1 else pieces[0]
        o_ref[pl.ds(q0, block), :] = o.T.astype(BF16).astype(F32)
        return carry

    lax.fori_loop(0, length // block, step, 0)


def bwd_kernel(heads, length, block, rb_ref, q_ref, k_ref, v_ref, kt_ref, do_ref, segr_ref, segc_ref,
               dq_ref, dk_ref, dv_ref, db_ref, bias, dbias, dk, dv):
    step_id = pl.program_id(0)
    total_rows = 2 * length - block

    @pl.when(step_id == 0)
    def _():
        build_bias(rb_ref, bias, heads, length, block)
        dbias[...] = jnp.zeros_like(dbias)

    dk[...] = jnp.zeros_like(dk)
    dv[...] = jnp.zeros_like(dv)
    lanes = heads * HD
    lane = lax.broadcasted_iota(jnp.int32, (block, lanes), 1) // HD

    def step(i, carry):
        q0 = pl.multiple_of(i * block, block)
        start = pl.multiple_of(length - block - q0, block)
        qb = q_ref[pl.ds(q0, block), :] * 0.125
        dob = do_ref[pl.ds(q0, block), :].astype(BF16)
        same = segc_ref[...] == segr_ref[0, :, pl.ds(q0, block)]
        pieces = []
        for h in range(heads):
            qm = jnp.where(lane == h, qb, jnp.zeros_like(qb)) if heads > 1 else qb
            dom = jnp.where(lane == h, dob, jnp.zeros_like(dob)) if heads > 1 else dob
            s = dot(k_ref[...], qm, 1, 1) + bias[h, pl.ds(start, length), :]
            s = jnp.where(same, s, NEG)
            p = jnp.exp(s - jnp.max(s, axis=0, keepdims=True))
            p = p * (1.0 / jnp.sum(p, axis=0, keepdims=True))
            dp = dot(v_ref[...], dom, 1, 1)
            ds = (p * (dp - jnp.sum(p * dp, axis=0, keepdims=True))).astype(BF16)
            dbias[h, pl.ds(start, length), :] += ds.astype(F32)
            dk[...] += dot(ds, qm, 1, 0)
            dv[...] += dot(p.astype(BF16), dom, 1, 0)
            pieces.append(dot(kt_ref[h * HD:(h + 1) * HD, :], ds, 1, 0))
        dq = jnp.concatenate(pieces, axis=0) if heads > 1 else pieces[0]
        dq_ref[pl.ds(q0, block), :] = (dq * 0.125).T.astype(BF16)
        return carry

    lax.fori_loop(0, length // block, step, 0)
    dk_ref[...] = dk[...].astype(BF16)
    dv_ref[...] = dv[...].astype(BF16)

    @pl.when(step_id == pl.num_programs(0) - 1)
    def _():
        origin = length - block
        low_end = (origin - THRESH[-1] + 1) // CH * CH
        high_start = -(-(origin + block - 1 + THRESH[-1]) // CH) * CH

        def fold(x):
            return jnp.sum(x, axis=0, keepdims=True)

        for h in range(heads):
            def rows(lo, hi):
                def body(i, acc):
                    r0 = pl.multiple_of(lo + i * CH, CH)
                    return acc + fold(dbias[h, pl.ds(r0, CH), :])

                return lax.fori_loop(0, (hi - lo) // CH, body, jnp.zeros((1, block), F32))

            def chunk(i, sums):
                r0 = pl.multiple_of(low_end + i * CH, CH)
                g = dbias[h, pl.ds(r0, CH), :]
                d = distance(r0, CH, block, origin)
                mag = jnp.abs(d)
                gb = jnp.where(d > 0, 0.0, g)
                ga = jnp.where(d > 0, g, 0.0)
                out = [sums[0] + fold(gb), sums[HALF] + fold(ga)]
                tb, ta = [], []
                for t in THRESH:
                    far = mag >= t
                    tb.append(fold(jnp.where(far, gb, 0.0)))
                    ta.append(fold(jnp.where(far, ga, 0.0)))
                new = [out[0]] + [sums[1 + n] + tb[n] for n in range(HALF - 1)]
                new += [out[1]] + [sums[HALF + 1 + n] + ta[n] for n in range(HALF - 1)]
                return tuple(new)

            sums = lax.fori_loop(0, (high_start - low_end) // CH, chunk,
                                 tuple(jnp.zeros((1, block), F32) for _ in range(NB)))
            left, right = rows(0, low_end), rows(high_start, total_rows)
            for b in range(NB):
                val = sums[b]
                if b not in (HALF - 1, NB - 1):
                    val = val - sums[b + 1]
                else:
                    val = val + (left if b == HALF - 1 else right)
                db_ref[h, b:b + 1, :] = jnp.broadcast_to(jnp.sum(val, axis=1, keepdims=True), (1, 128))


def attention_fwd(q, k, vt, seg, rb, block=256):
    tok, lanes = q.shape
    seqs, length = seg.shape
    heads = lanes // HD
    full = pl.BlockSpec((length, lanes), lambda s: (s, 0))
    return pl.pallas_call(
        functools.partial(fwd_kernel, heads, length, block),
        grid=(seqs,),
        out_shape=jax.ShapeDtypeStruct((tok, lanes), F32),
        in_specs=[pl.BlockSpec(memory_space=pltpu.SMEM), full, full,
                  pl.BlockSpec((lanes, length), lambda s: (0, s)),
                  pl.BlockSpec((1, 1, length), lambda s: (s, 0, 0)),
                  pl.BlockSpec((length, 1), lambda s: (s, 0))],
        out_specs=full,
        scratch_shapes=[pltpu.VMEM((heads, 2 * length - block, block), F32)],
        compiler_params=pltpu.CompilerParams(vmem_limit_bytes=56 << 20),
        cost_estimate=pl.CostEstimate(flops=4 * tok * length * lanes, bytes_accessed=tok * lanes * 10, transcendentals=tok * length * heads),
        name="attn_fwd",
    )(rb, q, k, vt, seg.reshape(seqs, 1, length), seg.reshape(tok, 1))


def attention_bwd(q, k, v, kt, do, seg, rb, block=256):
    tok, lanes = q.shape
    seqs, length = seg.shape
    heads = lanes // HD
    full = pl.BlockSpec((length, lanes), lambda s: (s, 0))
    sh = jax.ShapeDtypeStruct((tok, lanes), BF16)
    return pl.pallas_call(
        functools.partial(bwd_kernel, heads, length, block),
        grid=(seqs,),
        out_shape=(sh, sh, sh, jax.ShapeDtypeStruct((heads, NB, 128), F32)),
        in_specs=[pl.BlockSpec(memory_space=pltpu.SMEM), full, full, full,
                  pl.BlockSpec((lanes, length), lambda s: (0, s)), full,
                  pl.BlockSpec((1, 1, length), lambda s: (s, 0, 0)),
                  pl.BlockSpec((length, 1), lambda s: (s, 0))],
        out_specs=(full, full, full, pl.BlockSpec((heads, NB, 128), lambda s: (0, 0, 0))),
        scratch_shapes=[pltpu.VMEM((heads, 2 * length - block, block), F32)] * 2
        + [pltpu.VMEM((length, lanes), F32)] * 2,
        compiler_params=pltpu.CompilerParams(vmem_limit_bytes=56 << 20),
        cost_estimate=pl.CostEstimate(flops=10 * tok * length * lanes, bytes_accessed=tok * lanes * 20, transcendentals=tok * length * heads),
        name="attn_bwd",
    )(rb, q, k, v, kt, do, seg.reshape(seqs, 1, length), seg.reshape(tok, 1))


MESH = pl.DeviceIdType.MESH


class Ring:
    def __init__(self, n, rows):
        self.n = n
        self.inner = 1
        while (self.inner * 2) ** 2 <= n:
            self.inner *= 2
        self.outer = n // self.inner
        self.rows = rows
        self.rows_b = max(rows // 8 // 8 * 8, 8)
        self.rows_a = rows - self.rows_b
        self.count = next(c for c in (4, 2, 1) if self.rows_a % (8 * c) == 0)
        self.piece = self.rows_a // self.count
        self.pieces = [(p * self.piece, self.piece) for p in range(self.count)]

    def place(self):
        self.me = me = lax.axis_index("tensor")
        self.o, self.i = lax.div(me, self.inner), lax.rem(me, self.inner)

    def shard(self, back, side=0):
        return (lax.rem(self.o - back + 2 * self.outer, self.outer) * self.inner
                + lax.rem(self.i - side + self.inner, self.inner))

    def barrier(self, everyone=False, others=()):
        if everyone:
            peers = [{"tensor": self.peer(j)} for j in range(1, self.n)]
        else:
            peers = [self.shard(-1)] + ([self.shard(1)] if self.outer > 2 else [])
            peers += [self.shard(0, j) for j in range(1, self.inner)]
            peers = [{"tensor": p} for p in peers]
        peers += list(others)
        sem = pltpu.get_barrier_semaphore()
        for peer in peers:
            pl.semaphore_signal(sem, inc=1, device_id=peer, device_id_type=MESH)
        pl.semaphore_wait(sem, len(peers))

    def peer(self, j):
        return lax.rem(self.me + j, self.n)

    def gather_semaphores(self):
        dma = pltpu.SemaphoreType.DMA
        one = [dma((self.outer - 1, self.count)), dma((self.inner - 1, self.outer, self.count)),
               dma((self.inner, self.outer - 1)), dma((self.inner - 1,))]
        return one + one

    def reduce_scratch(self, width):
        dma = pltpu.SemaphoreType.DMA
        one = [dma((self.inner - 1, self.outer, self.count)), dma((self.outer - 1, self.count)),
               dma((self.inner, self.outer - 1)), dma((self.inner - 1,))]
        return [pltpu.VMEM((self.inner - 1, self.outer, self.rows_a, width), F32),
                pltpu.VMEM((self.outer - 1, self.rows_a, width), F32),
                pltpu.VMEM((self.inner, self.outer - 1, self.rows_b, width), F32),
                pltpu.VMEM((self.inner - 1, self.rows_b, width), F32)] + one + one


def remote(src, dst, send, recv, peer):
    return pltpu.make_async_remote_copy(src_ref=src, dst_ref=dst, send_sem=send, recv_sem=recv,
                                        device_id={"tensor": peer}, device_id_type=MESH)


class Gather:
    def __init__(self, ring, view, own, sems):
        self.r, self.view, self.own = ring, view, own
        (self.s_oa, self.s_ia, self.s_ob, self.s_ib, self.r_oa, self.r_ia, self.r_ob, self.r_ib) = sems
        self.sent = []

    def outer_a(self, step, p):
        r = self.r
        row, rows = r.pieces[p]
        shard = r.shard(step)
        src = self.own(row, rows) if step == 0 else self.view(shard, row, rows)
        return remote(src, self.view(shard, row, rows), self.s_oa.at[step, p], self.r_oa.at[step, p], r.shard(-1))

    def inner_a(self, j, step, p):
        r = self.r
        row, rows = r.pieces[p]
        shard = r.shard(step)
        src = self.own(row, rows) if step == 0 else self.view(shard, row, rows)
        return remote(src, self.view(shard, row, rows), self.s_ia.at[j - 1, step, p], self.r_ia.at[j - 1, step, p],
                      r.shard(0, -j))

    def outer_b(self, j, step):
        r = self.r
        shard = r.shard(step, j)
        src = self.own(r.rows_a, r.rows_b) if step == 0 and j == 0 else self.view(shard, r.rows_a, r.rows_b)
        return remote(src, self.view(shard, r.rows_a, r.rows_b), self.s_ob.at[j, step], self.r_ob.at[j, step], r.shard(-1))

    def inner_b(self, j):
        r = self.r
        return remote(self.own(r.rows_a, r.rows_b), self.view(r.shard(0), r.rows_a, r.rows_b),
                      self.s_ib.at[j - 1], self.r_ib.at[j - 1], r.shard(0, -j))

    def go(self, copy):
        copy.start()
        self.sent.append(copy)

    def start_a(self, p):
        self.go(self.outer_a(0, p))
        for j in range(1, self.r.inner):
            self.go(self.inner_a(j, 0, p))

    def start_b(self):
        for j in range(1, self.r.inner):
            self.go(self.inner_b(j))
        self.go(self.outer_b(0, 0))

    def middle(self):
        r = self.r
        for j in range(1, r.inner):
            self.inner_b(j).wait_recv()
            self.go(self.outer_b(j, 0))
        for step in range(1, r.outer):
            for p in range(r.count):
                self.outer_a(step - 1, p).wait_recv()
                if step < r.outer - 1:
                    self.go(self.outer_a(step, p))
                for j in range(1, r.inner):
                    self.go(self.inner_a(j, step, p))
            for j in range(r.inner):
                self.outer_b(j, step - 1).wait_recv()
                if step < r.outer - 1:
                    self.go(self.outer_b(j, step))

    def finish(self):
        r = self.r
        for step in range(r.outer):
            for p in range(r.count):
                for j in range(1, r.inner):
                    self.inner_a(j, step, p).wait_recv()
        for copy in self.sent:
            copy.wait_send()


class Reduce:
    def __init__(self, ring, src, scratch):
        self.r, self.src = ring, src
        (self.ia, self.oa, self.ob, self.ib, self.s_ia, self.s_oa, self.s_ob, self.s_ib,
         self.r_ia, self.r_oa, self.r_ob, self.r_ib) = scratch
        self.sent = []

    def part(self, shard, row, rows):
        return self.src.at[pl.ds(pl.multiple_of(shard * self.r.rows + row, 8), rows), :]

    def inner_a(self, j, step, p):
        r = self.r
        row, rows = r.pieces[p]
        return remote(self.part(r.shard(step + 1, -j), row, rows), self.ia.at[j - 1, step, pl.ds(row, rows), :],
                      self.s_ia.at[j - 1, step, p], self.r_ia.at[j - 1, step, p], r.shard(0, -j))

    def outer_a(self, step, p):
        r = self.r
        row, rows = r.pieces[p]
        src = self.ia.at[0, 0, pl.ds(row, rows), :] if step == 0 else self.oa.at[step - 1, pl.ds(row, rows), :]
        return remote(src, self.oa.at[step, pl.ds(row, rows), :], self.s_oa.at[step, p], self.r_oa.at[step, p], r.shard(-1))

    def outer_b(self, j, step):
        r = self.r
        src = self.part(r.shard(1, j), r.rows_a, r.rows_b) if step == 0 else self.ob.at[j, step - 1]
        return remote(src, self.ob.at[j, step], self.s_ob.at[j, step], self.r_ob.at[j, step], r.shard(-1))

    def inner_b(self, j):
        r = self.r
        return remote(self.ob.at[j, r.outer - 2], self.ib.at[j - 1], self.s_ib.at[j - 1], self.r_ib.at[j - 1], r.shard(0, j))

    def go(self, make, *at):
        make(*at).start()
        self.sent.append((make, at))

    def start(self):
        r = self.r
        for j in range(r.inner):
            self.go(self.outer_b, j, 0)
        for step in range(r.outer):
            for p in range(r.count):
                for j in range(1, r.inner):
                    self.go(self.inner_a, j, step, p)

    def event_a(self, step, p, done_a):
        r = self.r
        last = step == r.outer - 1
        row, rows = r.pieces[p]
        for j in range(1, r.inner):
            self.inner_a(j, step, p).wait_recv()
        total = self.part(r.shard(step + 1), row, rows)[...]
        for j in range(1, r.inner):
            total = total + self.ia[j - 1, step, pl.ds(row, rows), :]
        if step == 0:
            self.ia[0, 0, pl.ds(row, rows), :] = total
        else:
            self.outer_a(step - 1, p).wait_recv()
            total = total + self.oa[step - 1, pl.ds(row, rows), :]
            if not last:
                self.oa[step - 1, pl.ds(row, rows), :] = total
        if last:
            done_a(p, total)
        else:
            self.go(self.outer_a, step, p)

    def event_b(self, step):
        r = self.r
        for j in range(r.inner):
            self.outer_b(j, step - 1).wait_recv()
            total = self.ob[j, step - 1] + self.part(r.shard(step + 1, j), r.rows_a, r.rows_b)[...]
            self.ob[j, step - 1] = total
            if step < r.outer - 1:
                self.go(self.outer_b, j, step)
            elif j > 0:
                self.go(self.inner_b, j)

    def last_b(self, done_b):
        total = self.ob[0, self.r.outer - 2]
        for j in range(1, self.r.inner):
            self.inner_b(j).wait_recv()
            total = total + self.ib[j - 1]
        done_b(total)

    def events(self, done_a, done_b):
        r = self.r
        todo = []
        for step in range(r.outer):
            for p in range(r.count):
                todo.append(functools.partial(self.event_a, step, p, done_a))
            if step >= 1:
                todo.append(functools.partial(self.event_b, step))
        return todo + [functools.partial(self.last_b, done_b)]

    def finish(self):
        for make, at in self.sent:
            make(*at).wait_send()


def on_steps(step, events, share, last):
    due, done, total = [], 0, 0.0
    for i in range(last):
        total += share[0] if i < 8 else share[1]
        due.append(min(int(total), len(events)))
    for i, upto in enumerate(due):
        if upto > done:
            @pl.when(step == i)
            def _():
                for event in events[done:upto]:
                    event()

            done = upto

    @pl.when(step == last)
    def _():
        for event in events[done:]:
            event()


def wire(us):
    return pl.CostEstimate(flops=0, bytes_accessed=us * 3_000_000, transcendentals=0)


def params(cid, vmem):
    return pltpu.CompilerParams(collective_id=cid, has_side_effects=True, vmem_limit_bytes=vmem)


def gather_columns(x, n, cid):
    rows, lanes = x.shape
    ring = Ring(n, rows)
    flat = lanes % 128 == 0

    def kernel(x_ref, out, *sems):
        ring.place()
        ring.barrier()

        def view(shard, row, count):
            if flat:
                return out.at[pl.ds(row, count), pl.ds(pl.multiple_of(shard * lanes, 128), lanes)]
            return out.at[shard, pl.ds(row, count), :]

        gather = Gather(ring, view, lambda row, count: x_ref.at[pl.ds(row, count), :], sems[:8])
        keep = pltpu.make_async_copy(x_ref, view(ring.shard(0), 0, rows), sems[8])
        gather.start_b()
        for p in range(ring.count):
            gather.start_a(p)
        keep.start()
        gather.middle()
        gather.finish()
        keep.wait()

    shape = (rows, n * lanes) if flat else (n, rows, lanes)
    out = pl.pallas_call(
        kernel,
        out_shape=jax.ShapeDtypeStruct(shape, F32),
        in_specs=[pl.BlockSpec(memory_space=pltpu.VMEM)],
        out_specs=pl.BlockSpec(memory_space=pl.ANY),
        scratch_shapes=ring.gather_semaphores() + [pltpu.SemaphoreType.DMA],
        compiler_params=params(cid, 16 << 20),
        cost_estimate=wire(90),
        name="gather_columns",
    )(x)
    return out if flat else out.transpose(1, 0, 2).reshape(rows, n * lanes)


class Swap:
    def __init__(self, axis, n, block, got, send, recv):
        self.axis, self.n, self.block, self.got, self.send, self.recv = axis, n, block, got, send, recv

    def copy(self, j):
        me = lax.axis_index(self.axis)
        peer = lax.rem(me + j, self.n)
        return pltpu.make_async_remote_copy(
            src_ref=self.block(peer), dst_ref=self.got.at[j - 1],
            send_sem=self.send.at[j - 1], recv_sem=self.recv.at[j - 1], device_id={self.axis: peer}, device_id_type=MESH)

    def start(self):
        for j in range(1, self.n):
            self.copy(j).start()

    def total(self):
        for j in range(1, self.n):
            self.copy(j).wait()
        value = self.block(lax.axis_index(self.axis))[...]
        for j in range(1, self.n):
            value = value + self.got[j - 1]
        return value

    @staticmethod
    def scratch(n, shape):
        return [pltpu.VMEM((n - 1,) + shape, F32), pltpu.SemaphoreType.DMA((n - 1,)), pltpu.SemaphoreType.DMA((n - 1,))]


def reduce_norm_gather(part, values, upper, gain, small, keep_rows, inner_w, outer_w, n, n_dp, cid):
    total, width = part.shape
    rows = total // n
    ring = Ring(n, rows)
    n_red = len(ring.reduce_scratch(width))
    wide = width // n_dp
    s_rows = small.shape[1]
    in_rows = inner_w.shape[0] // n_dp
    height = outer_w.shape[0]
    out_rows = height // n
    columns = wide % 128 == 0
    if not columns:
        outer_w = outer_w.reshape(height, n_dp, wide).transpose(1, 0, 2)
    swaps = [(n_dp, (s_rows, wide)), (n, (s_rows, wide)), (n_dp, (in_rows, inner_w.shape[1])),
             (n_dp, (height, wide)), (n, (out_rows, wide))]

    def kernel(part_ref, val_ref, up_ref, gain_ref, small_ref, in_ref, ou_ref, out, small_out, in_out, ou_out,
               piece, sm, sm2, ou2, gain_acc, keep_sem, *scratch):
        dp = lax.axis_index("dp")
        ring.place()
        ring.barrier(everyone=True, others=[{"dp": lax.rem(dp + j, n_dp)} for j in range(1, n_dp)])
        one = Swap("dp", n_dp, lambda p: sm.at[p], *scratch[:3])
        two = Swap("tensor", n, lambda p: sm2, *scratch[3:6])
        inner_sum = Swap("dp", n_dp, lambda p: in_ref.at[pl.ds(pl.multiple_of(p * in_rows, 8), in_rows), :], *scratch[6:9])
        ou_one = Swap("dp", n_dp, (lambda p: ou_ref.at[:, pl.ds(pl.multiple_of(p * wide, 128), wide)]) if columns
                      else (lambda p: ou_ref.at[p]), *scratch[9:12])
        ou_two = Swap("tensor", n, lambda p: ou2.at[pl.ds(pl.multiple_of(p * out_rows, 8), out_rows), :], *scratch[12:15])
        reduce = Reduce(ring, part_ref, scratch[15:15 + n_red])
        gather = Gather(ring, lambda shard, row, count: out.at[pl.ds(pl.multiple_of(shard * rows + row, 8), count), :],
                        lambda row, count: piece.at[pl.ds(row, count), :], scratch[15 + n_red:])
        reduce.start()
        ou_one.start()
        inner_sum.start()
        gain_acc[...] = jnp.zeros_like(gain_acc)
        sm[...] = small_ref[...]

        def back(row, count, grad):
            x = val_ref[pl.ds(row, count), :]
            rr = lax.rsqrt(jnp.mean(x * x, axis=1, keepdims=True) + EPSILON)
            scaled = gain_ref[...] * grad
            inner = jnp.mean(scaled * x, axis=1, keepdims=True)
            piece[pl.ds(row, count), :] = up_ref[pl.ds(row, count), :] + rr * scaled - x * (rr * rr * rr * inner)
            gain_acc[...] += jnp.sum(grad * x * rr, axis=0, keepdims=True)

        def done_a(p, value):
            row, count = ring.pieces[p]
            back(row, count, value)
            gather.start_a(p)

        def done_b(value):
            back(ring.rows_a, ring.rows_b, value)
            gather.start_b()

        for event in reduce.events(done_a, done_b):
            event()
        keep = pltpu.make_async_copy(piece, out.at[pl.ds(pl.multiple_of(ring.shard(0) * rows, 8), rows), :], keep_sem)
        keep.start()
        for p in range(n_dp):
            sm[p, 0:1, :] = gain_acc[:, p * wide:(p + 1) * wide]
        one.start()
        ou2[...] = ou_one.total()
        ou_two.start()
        gather.middle()
        sm2[...] = one.total()
        two.start()
        in_out[...] = inner_sum.total()
        gather.finish()
        ou_out[...] = ou_two.total()
        both = two.total()
        last = lax.broadcasted_iota(jnp.int32, both.shape, 0) >= s_rows - keep_rows
        small_out[...] = jnp.where(last, sm2[...], both)
        reduce.finish()
        keep.wait()

    vm = pl.BlockSpec(memory_space=pltpu.VMEM)
    block = (s_rows, wide)
    return pl.pallas_call(
        kernel,
        out_shape=[jax.ShapeDtypeStruct(s, F32) for s in ((total, width), block, (in_rows, inner_w.shape[1]), (out_rows, wide))],
        in_specs=[vm] * 7,
        out_specs=[pl.BlockSpec(memory_space=pl.ANY), vm, vm, vm],
        scratch_shapes=[pltpu.VMEM((rows, width), F32), pltpu.VMEM((n_dp,) + block, F32), pltpu.VMEM(block, F32),
                        pltpu.VMEM((height, wide), F32), pltpu.VMEM((1, width), F32), pltpu.SemaphoreType.DMA]
        + [ref for swap in swaps for ref in Swap.scratch(*swap)]
        + ring.reduce_scratch(width) + ring.gather_semaphores(),
        compiler_params=params(cid, 48 << 20),
        cost_estimate=wire(180),
        name="reduce_norm_gather",
    )(part, values, upper, gain.reshape(1, width), small, inner_w, outer_w)


EXPERTS = 8
CAP = 576
SLOTS = EXPERTS * CAP
LN = 128
GC = math.sqrt(2.0 / math.pi)


def spread(dst, row0, sub, src, rows):
    for j in range(sub):
        dst[pl.ds(row0 * sub + j, rows, stride=sub), :] = src[:, j * LN:(j + 1) * LN].astype(F32)


def tile(ref, row, sub):
    return ref.at[pl.ds(pl.multiple_of(row * sub, sub), sub), :]


def combine_rows(tgt, rows, mix, out, tok, sub, t0, count):
    def body(i, c):
        for u in range(8):
            r = i * 8 + u
            one = rows[pl.ds(pl.multiple_of(tgt[t0 + r] * sub, sub), sub), :]
            two = rows[pl.ds(pl.multiple_of(tgt[tok + t0 + r] * sub, sub), sub), :]
            mix[pl.ds(pl.multiple_of(r * sub, sub), sub), :] = one + two
        return c

    lax.fori_loop(0, count // 8, body, 0)
    for j in range(sub):
        out[:, j * LN:(j + 1) * LN] = mix[pl.ds(j, count, stride=sub), :]


def by_expert(shape):
    return pl.BlockSpec(shape, lambda i, *t: (jnp.minimum(i, EXPERTS - 1),) + (0,) * (len(shape) - 1))


def whole(shape):
    return pl.BlockSpec(shape, lambda i, *t: (0,) * len(shape), pipeline_mode=pl.Buffered(1))


def forward_kernel(tok, sub, count, tgt, held, src, share, win, wdn, x, sh, gate, up, act, mo, rows_in, rows, shares, mix):
    step = pl.program_id(0)
    row0 = pl.multiple_of(step * CAP, 8)

    @pl.when(step == 0)
    def _():
        rows[SLOTS * sub:, :] = jnp.zeros((sub, LN), F32)

        def load(i, c):
            t0 = pl.multiple_of(i * 64, 64)
            spread(rows_in, t0, sub, src.at[pl.ds(t0, 64), :], 64)
            return c

        lax.fori_loop(0, tok // 64, load, 0)

        def move(i, c):
            for u in range(8):
                t = i * 8 + u
                row = tile(rows_in, t, sub)[...]
                for choice in range(2):
                    slot = tgt[choice * tok + t]
                    tile(rows, slot, sub)[...] = row
                    shares[pl.ds(slot, 1), :] = share[pl.ds(choice * tok + t, 1), :]
            return c

        lax.fori_loop(0, tok // 8, move, 0)
        rows[SLOTS * sub:, :] = jnp.zeros((sub, LN), F32)

        for e in range(EXPERTS):
            def clear(s, c):
                tile(rows, e * CAP + s, sub)[...] = jnp.zeros((sub, LN), F32)
                shares[pl.ds(e * CAP + s, 1), :] = jnp.zeros((1, LN), F32)
                return c

            lax.fori_loop(held[e], CAP, clear, 0)

    @pl.when(step < EXPERTS)
    def _():
        for j in range(sub):
            x[:, j * LN:(j + 1) * LN] = rows[pl.ds(row0 * sub + j, CAP, stride=sub), :].astype(BF16)
        sh[...] = shares[pl.ds(row0, CAP), :]
        g = dot(x[...], win[0, 0], 1, 1)
        u = dot(x[...], win[0, 1], 1, 1)
        gate[0] = g
        up[0] = u
        a = (0.5 * g * (1.0 + jnp.tanh(GC * (g + 0.044715 * (g * g * g)))) * u).astype(BF16)
        act[0] = a
        spread(rows, row0, sub, dot(a, wdn[0], 1, 0) * sh[:, 0:1], CAP)

    @pl.when(step >= EXPERTS)
    def _():
        combine_rows(tgt, rows, mix, mo, tok, sub, (step - EXPERTS) * count, count)


def experts_forward(tgt, held, src, share, win, wdn, count=256):
    tok, width = src.shape
    sub = width // LN
    ff = wdn.shape[1]
    mid = by_expert((1, CAP, ff))
    return pl.pallas_call(
        functools.partial(forward_kernel, tok, sub, count),
        grid_spec=pltpu.PrefetchScalarGridSpec(
            num_scalar_prefetch=2, grid=(EXPERTS + tok // count,),
            in_specs=[whole(src.shape), whole(share.shape), by_expert((1, 2, ff, width)), by_expert((1, ff, width))],
            out_specs=[by_expert((CAP, width)), by_expert((CAP, LN)), mid, mid, mid,
                       pl.BlockSpec((count, width), lambda i, *t: (jnp.maximum(i - EXPERTS, 0), 0))],
            scratch_shapes=[pltpu.VMEM((tok * sub, LN), F32), pltpu.VMEM(((SLOTS + 1) * sub, LN), F32),
                            pltpu.VMEM((SLOTS + 8, LN), F32), pltpu.VMEM((count * sub, LN), F32)]),
        out_shape=[jax.ShapeDtypeStruct((SLOTS, width), BF16), jax.ShapeDtypeStruct((SLOTS, LN), F32)]
        + [jax.ShapeDtypeStruct((EXPERTS, CAP, ff), F32)] * 2
        + [jax.ShapeDtypeStruct((EXPERTS, CAP, ff), BF16), jax.ShapeDtypeStruct((tok, width), F32)],
        compiler_params=pltpu.CompilerParams(vmem_limit_bytes=62 << 20),
        cost_estimate=pl.CostEstimate(flops=6 * SLOTS * width * ff, bytes_accessed=120 << 20, transcendentals=SLOTS * ff),
        name="experts_forward",
    )(tgt, held, src, share, win, wdn)


def backward_kernel(tok, chunk, ring, share, cot, tgt_row, tgt_col, sh, gate, up, act, win, wdn, part, hid,
                    y, dgu, mi, sg, res, dxs, aux, mask, *scratch):
    step = pl.program_id(0)
    last = EXPERTS + tok // chunk - 1
    ring.place()
    reduce = Reduce(ring, part, scratch)

    @pl.when(step == 0)
    def _():
        ring.barrier()
        reduce.start()

    @pl.when(step < EXPERTS)
    def _():
        first = pl.multiple_of(step * CAP, 8)
        slot = lax.broadcasted_iota(jnp.int32, (CAP, LN), 0) + first

        def fill(i, c):
            t0 = pl.multiple_of(i * LN, LN)
            held = (tgt_row[0:1, pl.ds(t0, LN)] == slot) | (tgt_row[1:2, pl.ds(t0, LN)] == slot)
            mask[:, pl.ds(t0, LN)] = jnp.where(held, 1.0, 0.0).astype(BF16)
            return c

        lax.fori_loop(0, tok // LN, fill, 0)
        rows = dot(mask[...], cot[...], 1, 0).astype(BF16)
        y[...] = rows
        h = dot(rows, wdn[0], 1, 1)
        g, u = gate[0], up[0]
        g2 = g * g
        t = jnp.tanh(GC * (g + 0.044715 * g2 * g))
        half = 0.5 * (1.0 + t)
        sgrow = jnp.sum(act[0].astype(F32) * h, axis=1, keepdims=True)
        da = sh[:, 0:1] * h
        slope = half + (0.5 * GC) * g * (1.0 - t * t) * (1.0 + (3 * 0.044715) * g2)
        dg = (da * u * slope).astype(BF16)
        du = (da * (g * half)).astype(BF16)
        dgu[0, 0] = dg
        dgu[0, 1] = du
        dxs[pl.ds(first, CAP), :] = (dot(dg, win[0, 0], 1, 0) + dot(du, win[0, 1], 1, 0)).astype(BF16)
        lane = lax.broadcasted_iota(jnp.int32, (CAP, LN), 1)
        high = sgrow.astype(BF16).astype(F32)
        low = jnp.where(lane == 2 * step + 1, sgrow - high, 0.0)
        aux[pl.ds(first, CAP), :] = jnp.where(lane == 2 * step, high, low).astype(BF16)

    @pl.when(step >= EXPERTS)
    def _():
        t0 = pl.multiple_of((step - EXPERTS) * chunk, chunk)
        span = 4 * CAP
        slots = lax.broadcasted_iota(jnp.int32, (chunk, span), 1)
        one, two = tgt_col[pl.ds(t0, chunk), 0:1], tgt_col[pl.ds(t0, chunk), 1:2]
        rows = jnp.zeros((chunk, cot.shape[1]), F32)
        value = jnp.zeros((chunk, LN), F32)
        for s0 in range(0, SLOTS, span):
            held = (one - s0 == slots) | (two - s0 == slots)
            both = jnp.where(held, 1.0, 0.0).astype(BF16)
            rows = rows + dot(both, dxs[s0:s0 + span, :], 1, 0)
            value = value + dot(both, aux[s0:s0 + span, :], 1, 0)
        mi[...] = rows
        lane = lax.broadcasted_iota(jnp.int32, (chunk, LN), 1)
        low = lax.div(lane, 2) * CAP
        sums = [jnp.sum(jnp.where((c >= low) & (c < low + CAP), value, 0.0), axis=1, keepdims=True) for c in (one, two)]
        sg[...] = jnp.where(lane == 0, sums[0], sums[1])

    def done_a(p, value):
        row, n = ring.pieces[p]
        res[pl.ds(row, n), :] = value + hid[pl.ds(row, n), :]

    def done_b(value):
        res[pl.ds(ring.rows_a, ring.rows_b), :] = value + hid[pl.ds(ring.rows_a, ring.rows_b), :]

    on_steps(step, reduce.events(done_a, done_b), share, last)

    @pl.when(step == last)
    def _():
        reduce.finish()


def experts_backward(tgt, cot, sh, gate, up, act, win, wdn, part, hid, n, cid, chunk=256, share=(1.4, 0.65)):
    tok, width = part.shape
    ff = wdn.shape[1]
    ring = Ring(n, tok // n)
    mid = by_expert((1, CAP, ff))
    tgt_row = tgt.reshape(2, tok)

    def by_chunk(lanes):
        return pl.BlockSpec((chunk, lanes), lambda i: (jnp.maximum(i - EXPERTS, 0), 0))

    return pl.pallas_call(
        functools.partial(backward_kernel, tok, chunk, ring, share),
        grid=(EXPERTS + tok // chunk,),
        in_specs=[whole(cot.shape), whole((2, tok)), whole((tok, 2)), by_expert((CAP, LN)), mid, mid, mid,
                  by_expert((1, 2, ff, width)), by_expert((1, ff, width)), whole(part.shape), whole(hid.shape)],
        out_specs=[by_expert((CAP, width)), by_expert((1, 2, CAP, ff)), by_chunk(width), by_chunk(LN),
                   pl.BlockSpec(hid.shape, lambda i: (0, 0))],
        scratch_shapes=[pltpu.VMEM((SLOTS, width), BF16), pltpu.VMEM((SLOTS, LN), BF16), pltpu.VMEM((CAP, tok), BF16)]
        + ring.reduce_scratch(width),
        out_shape=[jax.ShapeDtypeStruct((SLOTS, width), BF16), jax.ShapeDtypeStruct((EXPERTS, 2, CAP, ff), BF16),
                   jax.ShapeDtypeStruct((tok, width), F32), jax.ShapeDtypeStruct((tok, LN), F32),
                   jax.ShapeDtypeStruct(hid.shape, F32)],
        compiler_params=params(cid, 63 << 20),
        cost_estimate=wire(90),
        name="experts_backward",
    )(cot, tgt_row, tgt_row.T, sh, gate, up, act, win, wdn, part, hid)


def exclusive_or(a, b, bound):
    value, bit = 0, 1
    while bit < bound:
        value = value + lax.rem(lax.div(a, bit) + lax.div(b, bit), 2) * bit
        bit *= 2
    return value


def weights_kernel(parts, ring, n, share, x, y, sh, act, dgu, part, small, keep, give, out, small_out,
                   kept, gave, got, g_send, g_recv, sw_got, sw_send, sw_recv, *scratch):
    step = pl.program_id(0)
    dp = lax.axis_index("dp")
    mine = lax.rem(dp, 2)
    upper = lax.div(dp, 2)
    blocks = parts // 2
    half = blocks // 2
    ring.place()
    reduce = Reduce(ring, part, scratch)
    swap = Swap("tensor", n, lambda p: small.at[p], sw_got, sw_send, sw_recv)

    def to_partner(slot):
        return pltpu.make_async_remote_copy(
            src_ref=gave.at[slot], dst_ref=got.at[slot], send_sem=g_send.at[slot], recv_sem=g_recv.at[slot],
            device_id={"dp": dp + 1 - 2 * mine}, device_id_type=MESH)

    @pl.when(step == 0)
    def _():
        ring.barrier(everyone=True, others=[{"dp": dp + 1 - 2 * mine}])
        swap.start()
        reduce.start()

    @pl.when(step >= 1)
    def _():
        slot = lax.rem(step + 1, 2)
        to_partner(slot).wait()
        for q in range(blocks):
            to = exclusive_or(q, upper, blocks)

            @pl.when(to < half)
            def _():
                keep[to, 0] = kept[slot, q] + got[slot, q]

            @pl.when(to >= half)
            def _():
                give[to - half, 0] = kept[slot, q] + got[slot, q]

    @pl.when(step < EXPERTS)
    def _():
        slot = lax.rem(step, 2)
        og = (y[...].astype(F32) * sh[:, 0:1]).astype(BF16)
        wide = x.shape[1] // parts
        grads = [dot(dgu[0, 0], x[...], 0, 0), dot(dgu[0, 1], x[...], 0, 0), dot(act[0], og, 0, 0)]
        for bit in range(2):
            @pl.when(mine == bit)
            def _():
                for p in range(parts):
                    to = kept if p % 2 == bit else gave
                    for g in range(3):
                        to[slot, p // 2, g] = grads[g][:, p * wide:(p + 1) * wide]
        to_partner(slot).start()

    def done_a(p, value):
        row, count = ring.pieces[p]
        out[pl.ds(row, count), :] = value

    def done_b(value):
        out[pl.ds(ring.rows_a, ring.rows_b), :] = value

    on_steps(step, reduce.events(done_a, done_b), share, EXPERTS)

    @pl.when(step == EXPERTS)
    def _():
        small_out[...] = swap.total()
        reduce.finish()


def experts_weights(x, y, sh, act, dgu, part, small, n, parts, cid, share=(1.3, 0)):
    tok, width = part.shape
    ff = act.shape[2]
    wide = width // parts
    ring = Ring(n, tok // n)
    half = parts // 4
    o_w = jax.ShapeDtypeStruct((half, EXPERTS, 3, ff, wide), F32)
    b_w = pl.BlockSpec((half, 1, 3, ff, wide), lambda i, *t: (0, jnp.maximum(i - 1, 0), 0, 0, 0))
    slots = pltpu.VMEM((2, parts // 2, 3, ff, wide), F32)
    dma = pltpu.SemaphoreType.DMA
    return pl.pallas_call(
        functools.partial(weights_kernel, parts, ring, n, share),
        grid=(EXPERTS + 1,),
        in_specs=[by_expert((CAP, width)), by_expert((CAP, width)), by_expert((CAP, LN)),
                  by_expert((1, CAP, ff)), by_expert((1, 2, CAP, ff)), whole(part.shape), whole(small.shape)],
        out_specs=[b_w, b_w, pl.BlockSpec((tok // n, width), lambda i: (0, 0)),
                   pl.BlockSpec(small.shape[1:], lambda i: (0, 0))],
        scratch_shapes=[slots, slots, slots, dma((2,)), dma((2,))]
        + Swap.scratch(n, small.shape[1:]) + ring.reduce_scratch(width),
        out_shape=[o_w, o_w, jax.ShapeDtypeStruct((tok // n, width), F32), jax.ShapeDtypeStruct(small.shape[1:], F32)],
        compiler_params=params(cid, 63 << 20),
        cost_estimate=wire(90),
        name="experts_weights",
    )(x, y, sh, act, dgu, part, small)


def slot_targets(routes, order):
    tok = routes.shape[0]
    pos = jnp.arange(tok, dtype=jnp.int32)
    rank = jnp.sum(jnp.where(order[:, None] == pos[None, :], pos[:, None], 0), axis=0)
    earlier = (rank[:, None] > rank[None, :]).astype(BF16)
    ex = jnp.arange(EXPERTS, dtype=jnp.int32)
    onehot = (routes[:, :, None] == ex[None, None, :]).astype(BF16)
    before = dot(earlier, onehot.reshape(tok, 2 * EXPERTS), 1, 0).reshape(tok, 2, EXPERTS)
    first = jnp.sum(onehot[:, 0].astype(F32), axis=0)
    before = before + jnp.stack([jnp.zeros((EXPERTS,), F32), first])[None]
    slot = jnp.sum(before * onehot.astype(F32), axis=2).astype(jnp.int32)
    held = jnp.minimum(jnp.sum(onehot.astype(F32), axis=(0, 1)), CAP).astype(jnp.int32)
    return jnp.where(slot < CAP, routes * CAP + slot, SLOTS).T.reshape(-1), held


EPSILON = 1e-06
PRECISE = lax.Precision.HIGHEST


def rms_norm(values, gain):
    return values * lax.rsqrt(jnp.mean(values * values, axis=-1, keepdims=True) + EPSILON) * gain


def rms_back(values, gain, grad):
    rr = lax.rsqrt(jnp.mean(values * values, axis=-1, keepdims=True) + EPSILON)
    scaled = gain * grad
    back = rr * scaled - values * (rr * rr * rr) * jnp.mean(scaled * values, axis=-1, keepdims=True)
    return back, jnp.sum(grad * values * rr, axis=0)


def make_shards(mesh):
    n_tensor = mesh.shape["tensor"]
    n_dp = mesh.shape["dp"]

    def layer(tokens, cotangent, gain_attn, gain_moe, w_qkv, w_out, rel_bias, w_router, w_in, w_down,
              segment_ids, routes, order):
        tok, width = tokens.shape
        lanes = w_qkv.shape[2]
        share_rows = tok // n_tensor
        row0 = lax.axis_index("tensor") * share_rows

        def halve(keep, give):
            while True:
                blocks = keep.shape[0]
                came = lax.ppermute(give, "dp", [(d, d ^ (2 * blocks)) for d in range(n_dp)])
                if blocks == 1:
                    return keep[0], came[0]
                a = keep + came
                keep, give = a[:blocks // 2], a[blocks // 2:]

        def own(a):
            return lax.dynamic_slice_in_dim(a, row0, share_rows, 0)

        one = (order[0, 0] >= 0).astype(F32)
        w_out_cols = lax.dynamic_slice_in_dim(w_out, lax.axis_index("dp") * (width // n_dp), width // n_dp, 1).astype(F32)
        w_out_rows = lax.all_gather(w_out_cols, "tensor", axis=0, tiled=True)
        x = tokens.astype(F32)
        attn_input = rms_norm(x, gain_attn).astype(BF16)
        qkv = jnp.dot(attn_input, w_qkv.reshape(width, 3 * lanes), preferred_element_type=F32).astype(BF16)
        q, k, v = (qkv[:, i * lanes:(i + 1) * lanes] for i in range(3))
        rb = rel_bias.astype(F32).reshape(-1)
        attended = attention_fwd(q, k, v.T, segment_ids, rb)
        tgt, held = slot_targets(routes, order[0])

        attended, w_out_rows, tgt, held = lax.optimization_barrier((attended, w_out_rows, tgt, held))
        w_out_all = lax.all_gather(w_out_rows, "dp", axis=1, tiled=True) * one
        attended_all = gather_columns(attended, n_tensor, 0)
        hidden_one = x + jnp.dot(attended_all, w_out_all, preferred_element_type=F32)
        moe_input = rms_norm(hidden_one, gain_moe).astype(BF16)
        logits = jnp.dot(moe_input, w_router, preferred_element_type=F32)
        picked = (routes[:, :, None] == jnp.arange(EXPERTS, dtype=jnp.int32)[None, None, :]).astype(F32)

        def route(logit_rows, picked_rows):
            soft = jax.nn.softmax(logit_rows, axis=-1)
            chosen = jnp.sum(soft[:, None, :] * picked_rows, axis=-1)
            return soft, chosen, jnp.sum(chosen, axis=-1, keepdims=True)

        soft, chosen, both = route(logits, picked)
        pair_share = chosen / both
        w_in_t = jnp.swapaxes(w_in, 2, 3)
        share_rep = jnp.broadcast_to(pair_share.T.reshape(-1, 1), (2 * tok, LN))
        xs, slot_share, gate, up, act, moe_part = experts_forward(tgt, held, moe_input, share_rep, w_in_t, w_down)
        hidden_s = own(hidden_one)
        y, gate_up_grad, moe_in_part, share_part, result_s = experts_backward(
            tgt, cotangent, slot_share, gate, up, act, w_in_t, w_down, moe_part, hidden_s, n_tensor, 1)
        share_blocks = jnp.pad(share_part[:, :2].T.reshape(2, n_tensor, share_rows).transpose(1, 0, 2), ((0, 0), (0, 6), (0, 0)))
        keep, give, moe_in_sum, share_sum = experts_weights(
            xs, y, slot_share, act, gate_up_grad, moe_in_part, share_blocks, n_tensor, n_dp, 3)
        keep, came = halve(keep, give)
        share_grad = share_sum[0:2].T
        result_s, moe_in_sum = lax.optimization_barrier((result_s, moe_in_sum))
        result = lax.all_gather(result_s, "tensor", axis=0, tiled=True)

        soft_s, chosen_s, both_s, picked_s = own(soft), own(chosen), own(both), own(picked)
        chosen_grad = share_grad / both_s - jnp.sum(share_grad * chosen_s, axis=-1, keepdims=True) / (both_s * both_s)
        prob_grad = jnp.sum(chosen_grad[:, :, None] * picked_s, axis=1)
        logits_grad = soft_s * (prob_grad - jnp.sum(soft_s * prob_grad, axis=-1, keepdims=True))
        moe_input_s = own(moe_input)
        router_part = jnp.dot(moe_input_s.astype(F32).T, logits_grad, precision=PRECISE)
        moe_input_grad = moe_in_sum + jnp.dot(logits_grad, w_router.astype(F32).T, precision=PRECISE)
        norm_grad, gain_moe_part = rms_back(hidden_s, gain_moe, moe_input_grad)
        hidden_grad = own(cotangent).astype(F32) + norm_grad
        proj_grad = hidden_grad.astype(BF16)
        att_grad_s = lax.dot_general(proj_grad, w_out_all.astype(BF16), (((1,), (1,)), ((), ())), preferred_element_type=F32)
        att_grad_s = att_grad_s.astype(BF16).astype(F32)
        pieces = att_grad_s.reshape(share_rows, n_tensor, lanes).transpose(1, 0, 2)
        attended_grad = lax.all_to_all(pieces, "tensor", 0, 0, tiled=False).reshape(tok, lanes)
        w_out_part = lax.dot_general(own(attended_all).astype(BF16), proj_grad, (((0,), (0,)), ((), ())), preferred_element_type=F32)

        dq, dk, dv, bias_part = attention_bwd(q, k, v, k.T, attended_grad, segment_ids, rb)
        qkv_grad = jnp.concatenate([dq, dk, dv], axis=1)
        attn_in_part = lax.dot_general(qkv_grad, w_qkv.reshape(width, 3 * lanes), (((1,), (1,)), ((), ())), preferred_element_type=F32)
        w_qkv_part = lax.dot_general(attn_input, qkv_grad, (((0,), (0,)), ((), ())), preferred_element_type=F32)

        heads = lanes // HD
        wide = width // n_dp
        bias_rows = bias_part[:, :, 0].reshape(heads, n_dp, NB // n_dp).transpose(1, 0, 2)
        bias_rows = jnp.pad(bias_rows, ((0, 0), (0, 0), (0, wide - NB // n_dp)))
        sums = jnp.concatenate([jnp.zeros((1, width), F32), gain_moe_part[None], router_part.T], axis=0)
        sums = sums.reshape(sums.shape[0], n_dp, wide).transpose(1, 0, 2)
        small = jnp.concatenate([sums, jnp.zeros((n_dp, -(sums.shape[1] + heads) % 8, wide), F32), bias_rows], axis=1)
        input_grad, small, w_qkv_grad, w_out_grad = reduce_norm_gather(
            attn_in_part, own(tokens).astype(F32), hidden_grad, gain_attn, small, heads, w_qkv_part, w_out_part, n_tensor, n_dp, 2)

        small, keep = lax.optimization_barrier((small, keep))
        w_in_grad = jnp.swapaxes(keep[:, :2] + came[:, :2], 2, 3)
        w_down_grad = keep[:, 2] + came[:, 2]
        w_qkv_grad = w_qkv_grad.reshape(width // n_dp, 3, lanes)
        rel_bias_grad = small[small.shape[0] - heads:, :NB // n_dp].T
        return (result, input_grad, small[0], small[1], w_qkv_grad, w_out_grad, rel_bias_grad,
                small[2:2 + EXPERTS].T, w_in_grad, w_down_grad)

    return layer


def solution(mesh):
    return jax.shard_map(
        make_shards(mesh),
        mesh=mesh,
        in_specs=(
            P("dp", None),
            P("dp", None),
            P(),
            P(),
            P(None, None, "tensor"),
            P("tensor", None),
            P(None, "tensor"),
            P(),
            P(None, None, None, "tensor"),
            P(None, "tensor", None),
            P("dp", None),
            P("dp", None),
            P("dp", None),
        ),
        out_specs=(
            P("dp", None),
            P("dp", None),
            P("dp"),
            P("dp"),
            P("dp", None, "tensor"),
            P("tensor", "dp"),
            P("dp", "tensor"),
            P("dp", None),
            P(None, None, "dp", "tensor"),
            P(None, "tensor", "dp"),
        ),
        check_vma=False,
    )
```

```python
import functools
import math

import jax
import jax.numpy as jnp
import numpy as np
from jax import lax
from jax.experimental import pallas as pl
from jax.experimental.pallas import tpu as pltpu
from jax.sharding import PartitionSpec as P


F32 = jnp.float32
BF16 = jnp.bfloat16


def dot(a, b, ca, cb):
    return lax.dot_general(a, b, (((ca,), (cb,)), ((), ())), preferred_element_type=F32)


NB=32; MAXDIST=128; HD=64; NEG=-1000000000.0


def thresholds(bucket_count, reach):
    half_count = bucket_count // 2
    exact_count = half_count // 2
    listing = []
    for bucket_level in range(1, half_count):
        if bucket_level <= exact_count:
            listing.append(bucket_level)
        else:
            distance = exact_count
            while (exact_count + int(np.floor(np.log(distance / exact_count) / np.log(reach / exact_count) * (half_count - exact_count))) < bucket_level):
                distance += 1
            listing.append(distance)
    return listing


THRESH = thresholds(NB, MAXDIST)
HALF = NB // 2
CH = 128


def distance(row0, rows, cols, origin):
    r = lax.broadcasted_iota(jnp.int32, (rows, cols), 0)
    c = lax.broadcasted_iota(jnp.int32, (rows, cols), 1)
    return r + (row0 - origin) - c


def build_bias(rb_ref, bias, heads, length, block):
    total = 2 * length - block
    origin = length - block
    low_end = (origin - THRESH[-1] + 1) // CH * CH
    high_start = -(-(origin + block - 1 + THRESH[-1]) // CH) * CH
    for h in range(heads):
        bias[h, 0:low_end, :] = jnp.full((low_end, block), rb_ref[(HALF - 1) * heads + h], F32)
        bias[h, high_start:total, :] = jnp.full((total - high_start, block), rb_ref[(NB - 1) * heads + h], F32)

        def chunk(i, carry):
            row0 = pl.multiple_of(low_end + i * CH, CH)
            d = distance(row0, CH, block, origin)
            mag = jnp.abs(d)
            back = jnp.full((CH, block), rb_ref[h], F32)
            ahead = jnp.full((CH, block), rb_ref[HALF * heads + h], F32)
            for level, t in enumerate(THRESH):
                far = mag >= t
                back = jnp.where(far, rb_ref[(level + 1) * heads + h], back)
                ahead = jnp.where(far, rb_ref[(HALF + level + 1) * heads + h], ahead)
            bias[h, pl.ds(row0, CH), :] = jnp.where(d > 0, ahead, back)
            return carry

        lax.fori_loop(0, (high_start - low_end) // CH, chunk, 0)


def fwd_kernel(heads, length, block, rb_ref, q_ref, k_ref, vt_ref, segr_ref, segc_ref, o_ref, bias):
    @pl.when(pl.program_id(0) == 0)
    def _():
        build_bias(rb_ref, bias, heads, length, block)

    lanes = heads * HD
    lane = lax.broadcasted_iota(jnp.int32, (block, lanes), 1) // HD

    def step(i, carry):
        q0 = pl.multiple_of(i * block, block)
        start = pl.multiple_of(length - block - q0, block)
        qb = q_ref[pl.ds(q0, block), :] * 0.125
        same = segc_ref[...] == segr_ref[0, :, pl.ds(q0, block)]
        pieces = []
        for h in range(heads):
            qm = jnp.where(lane == h, qb, jnp.zeros_like(qb)) if heads > 1 else qb
            s = dot(k_ref[...], qm, 1, 1) + bias[h, pl.ds(start, length), :]
            s = jnp.where(same, s, NEG)
            p = jnp.exp(s - jnp.max(s, axis=0, keepdims=True))
            total = jnp.sum(p, axis=0, keepdims=True)
            p = (p * (1.0 / total)).astype(BF16)
            pieces.append(dot(vt_ref[h * HD:(h + 1) * HD, :], p, 1, 0))
        o = jnp.concatenate(pieces, axis=0) if heads > 1 else pieces[0]
        o_ref[pl.ds(q0, block), :] = o.T.astype(BF16).astype(F32)
        return carry

    lax.fori_loop(0, length // block, step, 0)


def bwd_kernel(heads, length, block, rb_ref, q_ref, k_ref, v_ref, kt_ref, do_ref, segr_ref, segc_ref,
               out_ref, db_ref, bias, dbias, dk, dv):
    step_id = pl.program_id(0)
    total_rows = 2 * length - block

    @pl.when(step_id == 0)
    def _():
        build_bias(rb_ref, bias, heads, length, block)
        dbias[...] = jnp.zeros_like(dbias)

    dk[...] = jnp.zeros_like(dk)
    dv[...] = jnp.zeros_like(dv)
    lanes = heads * HD
    lane = lax.broadcasted_iota(jnp.int32, (block, lanes), 1) // HD

    def step(i, carry):
        q0 = pl.multiple_of(i * block, block)
        start = pl.multiple_of(length - block - q0, block)
        qb = q_ref[pl.ds(q0, block), :] * 0.125
        dob = do_ref[pl.ds(q0, block), :].astype(BF16)
        same = segc_ref[...] == segr_ref[0, :, pl.ds(q0, block)]
        pieces = []
        for h in range(heads):
            qm = jnp.where(lane == h, qb, jnp.zeros_like(qb)) if heads > 1 else qb
            dom = jnp.where(lane == h, dob, jnp.zeros_like(dob)) if heads > 1 else dob
            s = dot(k_ref[...], qm, 1, 1) + bias[h, pl.ds(start, length), :]
            s = jnp.where(same, s, NEG)
            p = jnp.exp(s - jnp.max(s, axis=0, keepdims=True))
            p = p * (1.0 / jnp.sum(p, axis=0, keepdims=True))
            dp = dot(v_ref[...], dom, 1, 1)
            ds = (p * (dp - jnp.sum(p * dp, axis=0, keepdims=True))).astype(BF16)
            dbias[h, pl.ds(start, length), :] += ds.astype(F32)
            dk[...] += dot(ds, qm, 1, 0)
            dv[...] += dot(p.astype(BF16), dom, 1, 0)
            pieces.append(dot(kt_ref[h * HD:(h + 1) * HD, :], ds, 1, 0))
        dq = jnp.concatenate(pieces, axis=0) if heads > 1 else pieces[0]
        out_ref[pl.ds(q0, block), 0:lanes] = (dq * 0.125).T.astype(BF16)
        return carry

    lax.fori_loop(0, length // block, step, 0)
    out_ref[:, lanes:2 * lanes] = dk[...].astype(BF16)
    out_ref[:, 2 * lanes:] = dv[...].astype(BF16)

    @pl.when(step_id == pl.num_programs(0) - 1)
    def _():
        origin = length - block
        low_end = (origin - THRESH[-1] + 1) // CH * CH
        high_start = -(-(origin + block - 1 + THRESH[-1]) // CH) * CH

        def fold(x):
            return jnp.sum(x, axis=0, keepdims=True)

        for h in range(heads):
            def rows(lo, hi):
                def body(i, acc):
                    r0 = pl.multiple_of(lo + i * CH, CH)
                    return acc + fold(dbias[h, pl.ds(r0, CH), :])

                return lax.fori_loop(0, (hi - lo) // CH, body, jnp.zeros((1, block), F32))

            def chunk(i, sums):
                r0 = pl.multiple_of(low_end + i * CH, CH)
                g = dbias[h, pl.ds(r0, CH), :]
                d = distance(r0, CH, block, origin)
                mag = jnp.abs(d)
                gb = jnp.where(d > 0, 0.0, g)
                ga = jnp.where(d > 0, g, 0.0)
                out = [sums[0] + fold(gb), sums[HALF] + fold(ga)]
                tb, ta = [], []
                for t in THRESH:
                    far = mag >= t
                    tb.append(fold(jnp.where(far, gb, 0.0)))
                    ta.append(fold(jnp.where(far, ga, 0.0)))
                new = [out[0]] + [sums[1 + n] + tb[n] for n in range(HALF - 1)]
                new += [out[1]] + [sums[HALF + 1 + n] + ta[n] for n in range(HALF - 1)]
                return tuple(new)

            sums = lax.fori_loop(0, (high_start - low_end) // CH, chunk,
                                 tuple(jnp.zeros((1, block), F32) for _ in range(NB)))
            left, right = rows(0, low_end), rows(high_start, total_rows)
            for b in range(NB):
                val = sums[b]
                if b not in (HALF - 1, NB - 1):
                    val = val - sums[b + 1]
                else:
                    val = val + (left if b == HALF - 1 else right)
                db_ref[h, b:b + 1, :] = jnp.broadcast_to(jnp.sum(val, axis=1, keepdims=True), (1, 128))


def attention_fwd(q, k, vt, seg, rb, block=256):
    tok, lanes = q.shape
    seqs, length = seg.shape
    heads = lanes // HD
    full = pl.BlockSpec((length, lanes), lambda s: (s, 0))
    return pl.pallas_call(
        functools.partial(fwd_kernel, heads, length, block),
        grid=(seqs,),
        out_shape=jax.ShapeDtypeStruct((tok, lanes), F32),
        in_specs=[pl.BlockSpec(memory_space=pltpu.SMEM), full, full,
                  pl.BlockSpec((lanes, length), lambda s: (0, s)),
                  pl.BlockSpec((1, 1, length), lambda s: (s, 0, 0)),
                  pl.BlockSpec((length, 1), lambda s: (s, 0))],
        out_specs=full,
        scratch_shapes=[pltpu.VMEM((heads, 2 * length - block, block), F32)],
        compiler_params=pltpu.CompilerParams(vmem_limit_bytes=56 << 20),
        cost_estimate=pl.CostEstimate(flops=4 * tok * length * lanes, bytes_accessed=tok * lanes * 10, transcendentals=tok * length * heads),
        name="attn_fwd",
    )(rb, q, k, vt, seg.reshape(seqs, 1, length), seg.reshape(tok, 1))


def attention_bwd(q, k, v, kt, do, seg, rb, block=256):
    tok, lanes = q.shape
    seqs, length = seg.shape
    heads = lanes // HD
    full = pl.BlockSpec((length, lanes), lambda s: (s, 0))
    return pl.pallas_call(
        functools.partial(bwd_kernel, heads, length, block),
        grid=(seqs,),
        out_shape=(jax.ShapeDtypeStruct((tok, 3 * lanes), BF16), jax.ShapeDtypeStruct((heads, NB, 128), F32)),
        in_specs=[pl.BlockSpec(memory_space=pltpu.SMEM), full, full, full,
                  pl.BlockSpec((lanes, length), lambda s: (0, s)), full,
                  pl.BlockSpec((1, 1, length), lambda s: (s, 0, 0)),
                  pl.BlockSpec((length, 1), lambda s: (s, 0))],
        out_specs=(pl.BlockSpec((length, 3 * lanes), lambda s: (s, 0)), pl.BlockSpec((heads, NB, 128), lambda s: (0, 0, 0))),
        scratch_shapes=[pltpu.VMEM((heads, 2 * length - block, block), F32)] * 2
        + [pltpu.VMEM((length, lanes), F32)] * 2,
        compiler_params=pltpu.CompilerParams(vmem_limit_bytes=56 << 20),
        cost_estimate=pl.CostEstimate(flops=10 * tok * length * lanes, bytes_accessed=tok * lanes * 20, transcendentals=tok * length * heads),
        name="attn_bwd",
    )(rb, q, k, v, kt, do, seg.reshape(seqs, 1, length), seg.reshape(tok, 1))


MESH = pl.DeviceIdType.MESH


class Ring:
    def __init__(self, n, rows):
        self.n = n
        self.inner = 1
        while (self.inner * 2) ** 2 <= n:
            self.inner *= 2
        self.outer = n // self.inner
        self.rows = rows
        self.rows_b = max(rows // 8 // 8 * 8, 8)
        self.rows_a = rows - self.rows_b
        self.count = next(c for c in (4, 2, 1) if self.rows_a % (8 * c) == 0)
        self.piece = self.rows_a // self.count
        self.pieces = [(p * self.piece, self.piece) for p in range(self.count)]

    def place(self):
        self.me = me = lax.axis_index("tensor")
        self.o, self.i = lax.div(me, self.inner), lax.rem(me, self.inner)

    def shard(self, back, side=0):
        return (lax.rem(self.o - back + 2 * self.outer, self.outer) * self.inner
                + lax.rem(self.i - side + self.inner, self.inner))

    def barrier(self, everyone=False, others=()):
        if everyone:
            peers = [{"tensor": self.peer(j)} for j in range(1, self.n)]
        else:
            peers = [self.shard(-1)] + ([self.shard(1)] if self.outer > 2 else [])
            peers += [self.shard(0, j) for j in range(1, self.inner)]
            peers = [{"tensor": p} for p in peers]
        peers += list(others)
        sem = pltpu.get_barrier_semaphore()
        for peer in peers:
            pl.semaphore_signal(sem, inc=1, device_id=peer, device_id_type=MESH)
        pl.semaphore_wait(sem, len(peers))

    def peer(self, j):
        return lax.rem(self.me + j, self.n)

    def gather_semaphores(self):
        dma = pltpu.SemaphoreType.DMA
        one = [dma((self.outer - 1, self.count)), dma((self.inner - 1, self.outer, self.count)),
               dma((self.inner, self.outer - 1)), dma((self.inner - 1,))]
        return one + one

    def reduce_scratch(self, width):
        dma = pltpu.SemaphoreType.DMA
        one = [dma((self.inner - 1, self.outer, self.count)), dma((self.outer - 1, self.count)),
               dma((self.inner, self.outer - 1)), dma((self.inner - 1,))]
        return [pltpu.VMEM((self.inner - 1, self.outer, self.rows_a, width), F32),
                pltpu.VMEM((self.outer - 1, self.rows_a, width), F32),
                pltpu.VMEM((self.inner, self.outer - 1, self.rows_b, width), F32),
                pltpu.VMEM((self.inner - 1, self.rows_b, width), F32)] + one + one


def remote(src, dst, send, recv, peer):
    return pltpu.make_async_remote_copy(src_ref=src, dst_ref=dst, send_sem=send, recv_sem=recv,
                                        device_id={"tensor": peer}, device_id_type=MESH)


class Gather:
    def __init__(self, ring, view, own, sems):
        self.r, self.view, self.own = ring, view, own
        (self.s_oa, self.s_ia, self.s_ob, self.s_ib, self.r_oa, self.r_ia, self.r_ob, self.r_ib) = sems
        self.sent = []

    def outer_a(self, step, p):
        r = self.r
        row, rows = r.pieces[p]
        shard = r.shard(step)
        src = self.own(row, rows) if step == 0 else self.view(shard, row, rows)
        return remote(src, self.view(shard, row, rows), self.s_oa.at[step, p], self.r_oa.at[step, p], r.shard(-1))

    def inner_a(self, j, step, p):
        r = self.r
        row, rows = r.pieces[p]
        shard = r.shard(step)
        src = self.own(row, rows) if step == 0 else self.view(shard, row, rows)
        return remote(src, self.view(shard, row, rows), self.s_ia.at[j - 1, step, p], self.r_ia.at[j - 1, step, p],
                      r.shard(0, -j))

    def outer_b(self, j, step):
        r = self.r
        shard = r.shard(step, j)
        src = self.own(r.rows_a, r.rows_b) if step == 0 and j == 0 else self.view(shard, r.rows_a, r.rows_b)
        return remote(src, self.view(shard, r.rows_a, r.rows_b), self.s_ob.at[j, step], self.r_ob.at[j, step], r.shard(-1))

    def inner_b(self, j):
        r = self.r
        return remote(self.own(r.rows_a, r.rows_b), self.view(r.shard(0), r.rows_a, r.rows_b),
                      self.s_ib.at[j - 1], self.r_ib.at[j - 1], r.shard(0, -j))

    def go(self, copy):
        copy.start()
        self.sent.append(copy)

    def start_a(self, p):
        self.go(self.outer_a(0, p))
        for j in range(1, self.r.inner):
            self.go(self.inner_a(j, 0, p))

    def start_b(self):
        for j in range(1, self.r.inner):
            self.go(self.inner_b(j))
        self.go(self.outer_b(0, 0))

    def middle(self):
        r = self.r
        for j in range(1, r.inner):
            self.inner_b(j).wait_recv()
            self.go(self.outer_b(j, 0))
        for step in range(1, r.outer):
            for p in range(r.count):
                self.outer_a(step - 1, p).wait_recv()
                if step < r.outer - 1:
                    self.go(self.outer_a(step, p))
                for j in range(1, r.inner):
                    self.go(self.inner_a(j, step, p))
            for j in range(r.inner):
                self.outer_b(j, step - 1).wait_recv()
                if step < r.outer - 1:
                    self.go(self.outer_b(j, step))

    def finish(self):
        r = self.r
        for step in range(r.outer):
            for p in range(r.count):
                for j in range(1, r.inner):
                    self.inner_a(j, step, p).wait_recv()
        for copy in self.sent:
            copy.wait_send()


class Reduce:
    def __init__(self, ring, src, scratch):
        self.r, self.src = ring, src
        (self.ia, self.oa, self.ob, self.ib, self.s_ia, self.s_oa, self.s_ob, self.s_ib,
         self.r_ia, self.r_oa, self.r_ob, self.r_ib) = scratch
        self.sent = []

    def part(self, shard, row, rows):
        return self.src.at[pl.ds(pl.multiple_of(shard * self.r.rows + row, 8), rows), :]

    def inner_a(self, j, step, p):
        r = self.r
        row, rows = r.pieces[p]
        return remote(self.part(r.shard(step + 1, -j), row, rows), self.ia.at[j - 1, step, pl.ds(row, rows), :],
                      self.s_ia.at[j - 1, step, p], self.r_ia.at[j - 1, step, p], r.shard(0, -j))

    def outer_a(self, step, p):
        r = self.r
        row, rows = r.pieces[p]
        src = self.ia.at[0, 0, pl.ds(row, rows), :] if step == 0 else self.oa.at[step - 1, pl.ds(row, rows), :]
        return remote(src, self.oa.at[step, pl.ds(row, rows), :], self.s_oa.at[step, p], self.r_oa.at[step, p], r.shard(-1))

    def outer_b(self, j, step):
        r = self.r
        src = self.part(r.shard(1, j), r.rows_a, r.rows_b) if step == 0 else self.ob.at[j, step - 1]
        return remote(src, self.ob.at[j, step], self.s_ob.at[j, step], self.r_ob.at[j, step], r.shard(-1))

    def inner_b(self, j):
        r = self.r
        return remote(self.ob.at[j, r.outer - 2], self.ib.at[j - 1], self.s_ib.at[j - 1], self.r_ib.at[j - 1], r.shard(0, j))

    def go(self, make, *at):
        make(*at).start()
        self.sent.append((make, at))

    def start(self):
        r = self.r
        for j in range(r.inner):
            self.go(self.outer_b, j, 0)
        for step in range(r.outer):
            for p in range(r.count):
                for j in range(1, r.inner):
                    self.go(self.inner_a, j, step, p)

    def event_a(self, step, p, done_a):
        r = self.r
        last = step == r.outer - 1
        row, rows = r.pieces[p]
        for j in range(1, r.inner):
            self.inner_a(j, step, p).wait_recv()
        total = self.part(r.shard(step + 1), row, rows)[...]
        for j in range(1, r.inner):
            total = total + self.ia[j - 1, step, pl.ds(row, rows), :]
        if step == 0:
            self.ia[0, 0, pl.ds(row, rows), :] = total
        else:
            self.outer_a(step - 1, p).wait_recv()
            total = total + self.oa[step - 1, pl.ds(row, rows), :]
            if not last:
                self.oa[step - 1, pl.ds(row, rows), :] = total
        if last:
            done_a(p, total)
        else:
            self.go(self.outer_a, step, p)

    def event_b(self, step):
        r = self.r
        for j in range(r.inner):
            self.outer_b(j, step - 1).wait_recv()
            total = self.ob[j, step - 1] + self.part(r.shard(step + 1, j), r.rows_a, r.rows_b)[...]
            self.ob[j, step - 1] = total
            if step < r.outer - 1:
                self.go(self.outer_b, j, step)
            elif j > 0:
                self.go(self.inner_b, j)

    def last_b(self, done_b):
        total = self.ob[0, self.r.outer - 2]
        for j in range(1, self.r.inner):
            self.inner_b(j).wait_recv()
            total = total + self.ib[j - 1]
        done_b(total)

    def events(self, done_a, done_b):
        r = self.r
        todo = []
        for step in range(r.outer):
            for p in range(r.count):
                todo.append(functools.partial(self.event_a, step, p, done_a))
            if step >= 1:
                todo.append(functools.partial(self.event_b, step))
        return todo + [functools.partial(self.last_b, done_b)]

    def finish(self):
        for make, at in self.sent:
            make(*at).wait_send()


def on_steps(step, events, share, last):
    due, done, total = [], 0, 0.0
    for i in range(last):
        total += share[0] if i < 8 else share[1]
        due.append(min(int(total), len(events)))
    for i, upto in enumerate(due):
        if upto > done:
            @pl.when(step == i)
            def _():
                for event in events[done:upto]:
                    event()

            done = upto

    @pl.when(step == last)
    def _():
        for event in events[done:]:
            event()


def wire(us):
    return pl.CostEstimate(flops=0, bytes_accessed=us * 3_000_000, transcendentals=0)


def params(cid, vmem):
    return pltpu.CompilerParams(collective_id=cid, has_side_effects=True, vmem_limit_bytes=vmem)


def gather_columns(x, n, cid):
    rows, lanes = x.shape
    ring = Ring(n, rows)
    flat = lanes % 128 == 0

    def kernel(x_ref, out, *sems):
        ring.place()
        ring.barrier()

        def view(shard, row, count):
            if flat:
                return out.at[pl.ds(row, count), pl.ds(pl.multiple_of(shard * lanes, 128), lanes)]
            return out.at[shard, pl.ds(row, count), :]

        gather = Gather(ring, view, lambda row, count: x_ref.at[pl.ds(row, count), :], sems[:8])
        keep = pltpu.make_async_copy(x_ref, view(ring.shard(0), 0, rows), sems[8])
        gather.start_b()
        for p in range(ring.count):
            gather.start_a(p)
        keep.start()
        gather.middle()
        gather.finish()
        keep.wait()

    shape = (rows, n * lanes) if flat else (n, rows, lanes)
    out = pl.pallas_call(
        kernel,
        out_shape=jax.ShapeDtypeStruct(shape, F32),
        in_specs=[pl.BlockSpec(memory_space=pltpu.VMEM)],
        out_specs=pl.BlockSpec(memory_space=pl.ANY),
        scratch_shapes=ring.gather_semaphores() + [pltpu.SemaphoreType.DMA],
        compiler_params=params(cid, 60 << 20),
        cost_estimate=wire(90),
        name="gather_columns",
    )(x)
    return out if flat else out.transpose(1, 0, 2).reshape(rows, n * lanes)


class Swap:
    def __init__(self, axis, n, block, got, send, recv):
        self.axis, self.n, self.block, self.got, self.send, self.recv = axis, n, block, got, send, recv

    def copy(self, j):
        me = lax.axis_index(self.axis)
        peer = lax.rem(me + j, self.n)
        return pltpu.make_async_remote_copy(
            src_ref=self.block(peer), dst_ref=self.got.at[j - 1],
            send_sem=self.send.at[j - 1], recv_sem=self.recv.at[j - 1], device_id={self.axis: peer}, device_id_type=MESH)

    def start(self):
        for j in range(1, self.n):
            self.copy(j).start()

    def total(self):
        for j in range(1, self.n):
            self.copy(j).wait()
        value = self.block(lax.axis_index(self.axis))[...]
        for j in range(1, self.n):
            value = value + self.got[j - 1]
        return value

    @staticmethod
    def scratch(n, shape):
        return [pltpu.VMEM((n - 1,) + shape, F32), pltpu.SemaphoreType.DMA((n - 1,)), pltpu.SemaphoreType.DMA((n - 1,))]


def reduce_norm_gather(part, values, upper, gain, small, keep_rows, inner_w, outer_w, n, n_dp, cid):
    total, width = part.shape
    rows = total // n
    ring = Ring(n, rows)
    n_red = len(ring.reduce_scratch(width))
    wide = width // n_dp
    s_rows = small.shape[1]
    in_rows = inner_w.shape[0] // n_dp
    height = outer_w.shape[0]
    out_rows = height // n
    columns = wide % 128 == 0
    if not columns:
        outer_w = outer_w.reshape(height, n_dp, wide).transpose(1, 0, 2)
    swaps = [(n_dp, (s_rows, wide)), (n, (s_rows, wide)), (n_dp, (in_rows, inner_w.shape[1])),
             (n_dp, (height, wide)), (n, (out_rows, wide))]

    def kernel(part_ref, val_ref, up_ref, gain_ref, small_ref, in_ref, ou_ref, out, small_out, in_out, ou_out,
               piece, sm, sm2, ou2, gain_acc, keep_sem, *scratch):
        dp = lax.axis_index("dp")
        ring.place()
        ring.barrier(everyone=True, others=[{"dp": lax.rem(dp + j, n_dp)} for j in range(1, n_dp)])
        one = Swap("dp", n_dp, lambda p: sm.at[p], *scratch[:3])
        two = Swap("tensor", n, lambda p: sm2, *scratch[3:6])
        inner_sum = Swap("dp", n_dp, lambda p: in_ref.at[pl.ds(pl.multiple_of(p * in_rows, 8), in_rows), :], *scratch[6:9])
        ou_one = Swap("dp", n_dp, (lambda p: ou_ref.at[:, pl.ds(pl.multiple_of(p * wide, 128), wide)]) if columns
                      else (lambda p: ou_ref.at[p]), *scratch[9:12])
        ou_two = Swap("tensor", n, lambda p: ou2.at[pl.ds(pl.multiple_of(p * out_rows, 8), out_rows), :], *scratch[12:15])
        reduce = Reduce(ring, part_ref, scratch[15:15 + n_red])
        gather = Gather(ring, lambda shard, row, count: out.at[pl.ds(pl.multiple_of(shard * rows + row, 8), count), :],
                        lambda row, count: piece.at[pl.ds(row, count), :], scratch[15 + n_red:])
        reduce.start()
        ou_one.start()
        inner_sum.start()
        gain_acc[...] = jnp.zeros_like(gain_acc)
        sm[...] = small_ref[...]

        def back(row, count, grad):
            x = val_ref[pl.ds(row, count), :]
            rr = lax.rsqrt(jnp.mean(x * x, axis=1, keepdims=True) + EPSILON)
            scaled = gain_ref[...] * grad
            inner = jnp.mean(scaled * x, axis=1, keepdims=True)
            piece[pl.ds(row, count), :] = up_ref[pl.ds(row, count), :] + rr * scaled - x * (rr * rr * rr * inner)
            gain_acc[...] += jnp.sum(grad * x * rr, axis=0, keepdims=True)

        def done_a(p, value):
            row, count = ring.pieces[p]
            back(row, count, value)
            gather.start_a(p)

        def done_b(value):
            back(ring.rows_a, ring.rows_b, value)
            gather.start_b()

        for event in reduce.events(done_a, done_b):
            event()
        keep = pltpu.make_async_copy(piece, out.at[pl.ds(pl.multiple_of(ring.shard(0) * rows, 8), rows), :], keep_sem)
        keep.start()
        for p in range(n_dp):
            sm[p, 0:1, :] = gain_acc[:, p * wide:(p + 1) * wide]
        one.start()
        ou2[...] = ou_one.total()
        ou_two.start()
        gather.middle()
        sm2[...] = one.total()
        two.start()
        in_out[...] = inner_sum.total()
        gather.finish()
        ou_out[...] = ou_two.total()
        both = two.total()
        last = lax.broadcasted_iota(jnp.int32, both.shape, 0) >= s_rows - keep_rows
        small_out[...] = jnp.where(last, sm2[...], both)
        reduce.finish()
        keep.wait()

    vm = pl.BlockSpec(memory_space=pltpu.VMEM)
    block = (s_rows, wide)
    return pl.pallas_call(
        kernel,
        out_shape=[jax.ShapeDtypeStruct(s, F32) for s in ((total, width), block, (in_rows, inner_w.shape[1]), (out_rows, wide))],
        in_specs=[vm] * 7,
        out_specs=[pl.BlockSpec(memory_space=pl.ANY), vm, vm, vm],
        scratch_shapes=[pltpu.VMEM((rows, width), F32), pltpu.VMEM((n_dp,) + block, F32), pltpu.VMEM(block, F32),
                        pltpu.VMEM((height, wide), F32), pltpu.VMEM((1, width), F32), pltpu.SemaphoreType.DMA]
        + [ref for swap in swaps for ref in Swap.scratch(*swap)]
        + ring.reduce_scratch(width) + ring.gather_semaphores(),
        compiler_params=params(cid, 48 << 20),
        cost_estimate=wire(180),
        name="reduce_norm_gather",
    )(part, values, upper, gain.reshape(1, width), small, inner_w, outer_w)


EXPERTS = 8
CAP = 576
SLOTS = EXPERTS * CAP
LN = 128
GC = math.sqrt(2.0 / math.pi)


def spread(dst, row0, sub, src, rows):
    for j in range(sub):
        dst[pl.ds(row0 * sub + j, rows, stride=sub), :] = src[:, j * LN:(j + 1) * LN].astype(F32)


def tile(ref, row, sub):
    return ref.at[pl.ds(pl.multiple_of(row * sub, sub), sub), :]


def combine_rows(tgt, rows, mix, out, tok, sub, t0, count):
    def body(i, c):
        for u in range(8):
            r = i * 8 + u
            one = rows[pl.ds(pl.multiple_of(tgt[t0 + r] * sub, sub), sub), :]
            two = rows[pl.ds(pl.multiple_of(tgt[tok + t0 + r] * sub, sub), sub), :]
            mix[pl.ds(pl.multiple_of(r * sub, sub), sub), :] = one + two
        return c

    lax.fori_loop(0, count // 8, body, 0)
    for j in range(sub):
        out[:, j * LN:(j + 1) * LN] = mix[pl.ds(j, count, stride=sub), :]


def by_expert(shape):
    return pl.BlockSpec(shape, lambda i, *t: (jnp.minimum(i, EXPERTS - 1),) + (0,) * (len(shape) - 1))


def whole(shape):
    return pl.BlockSpec(shape, lambda i, *t: (0,) * len(shape), pipeline_mode=pl.Buffered(1))


def forward_kernel(tok, sub, count, tgt, held, src, share, win, wdn, x, sh, gate, up, act, mo, rows_in, rows, shares, mix):
    step = pl.program_id(0)
    row0 = pl.multiple_of(step * CAP, 8)

    @pl.when(step == 0)
    def _():
        rows[SLOTS * sub:, :] = jnp.zeros((sub, LN), F32)

        def load(i, c):
            t0 = pl.multiple_of(i * 64, 64)
            spread(rows_in, t0, sub, src.at[pl.ds(t0, 64), :], 64)
            return c

        lax.fori_loop(0, tok // 64, load, 0)

        def move(i, c):
            for u in range(8):
                t = i * 8 + u
                row = tile(rows_in, t, sub)[...]
                for choice in range(2):
                    slot = tgt[choice * tok + t]
                    tile(rows, slot, sub)[...] = row
                    shares[pl.ds(slot, 1), :] = share[pl.ds(choice * tok + t, 1), :]
            return c

        lax.fori_loop(0, tok // 8, move, 0)
        rows[SLOTS * sub:, :] = jnp.zeros((sub, LN), F32)

        for e in range(EXPERTS):
            def clear(s, c):
                tile(rows, e * CAP + s, sub)[...] = jnp.zeros((sub, LN), F32)
                shares[pl.ds(e * CAP + s, 1), :] = jnp.zeros((1, LN), F32)
                return c

            lax.fori_loop(held[e], CAP, clear, 0)

    @pl.when(step < EXPERTS)
    def _():
        for j in range(sub):
            x[:, j * LN:(j + 1) * LN] = rows[pl.ds(row0 * sub + j, CAP, stride=sub), :].astype(BF16)
        sh[...] = shares[pl.ds(row0, CAP), :]
        g = dot(x[...], win[0, 0], 1, 1)
        u = dot(x[...], win[0, 1], 1, 1)
        gate[0] = g
        up[0] = u
        a = (0.5 * g * (1.0 + jnp.tanh(GC * (g + 0.044715 * (g * g * g)))) * u).astype(BF16)
        act[0] = a
        spread(rows, row0, sub, dot(a, wdn[0], 1, 0) * sh[:, 0:1], CAP)

    @pl.when(step >= EXPERTS)
    def _():
        combine_rows(tgt, rows, mix, mo, tok, sub, (step - EXPERTS) * count, count)


def experts_forward(tgt, held, src, share, win, wdn, count=256):
    tok, width = src.shape
    sub = width // LN
    ff = wdn.shape[1]
    mid = by_expert((1, CAP, ff))
    return pl.pallas_call(
        functools.partial(forward_kernel, tok, sub, count),
        grid_spec=pltpu.PrefetchScalarGridSpec(
            num_scalar_prefetch=2, grid=(EXPERTS + tok // count,),
            in_specs=[whole(src.shape), whole(share.shape), by_expert((1, 2, ff, width)), by_expert((1, ff, width))],
            out_specs=[by_expert((CAP, width)), by_expert((CAP, LN)), mid, mid, mid,
                       pl.BlockSpec((count, width), lambda i, *t: (jnp.maximum(i - EXPERTS, 0), 0))],
            scratch_shapes=[pltpu.VMEM((tok * sub, LN), F32), pltpu.VMEM(((SLOTS + 1) * sub, LN), F32),
                            pltpu.VMEM((SLOTS + 8, LN), F32), pltpu.VMEM((count * sub, LN), F32)]),
        out_shape=[jax.ShapeDtypeStruct((SLOTS, width), BF16), jax.ShapeDtypeStruct((SLOTS, LN), F32)]
        + [jax.ShapeDtypeStruct((EXPERTS, CAP, ff), F32)] * 2
        + [jax.ShapeDtypeStruct((EXPERTS, CAP, ff), BF16), jax.ShapeDtypeStruct((tok, width), F32)],
        compiler_params=pltpu.CompilerParams(vmem_limit_bytes=62 << 20),
        cost_estimate=pl.CostEstimate(flops=6 * SLOTS * width * ff, bytes_accessed=120 << 20, transcendentals=SLOTS * ff),
        name="experts_forward",
    )(tgt, held, src, share, win, wdn)


def backward_kernel(tok, chunk, ring, share, cot, tgt_row, tgt_col, sh, gate, up, act, win, wdn, part, hid,
                    y, dgu, mi, sg, res, dxs, aux, mask, *scratch):
    step = pl.program_id(0)
    last = EXPERTS + tok // chunk - 1
    ring.place()
    reduce = Reduce(ring, part, scratch)

    @pl.when(step == 0)
    def _():
        ring.barrier()
        reduce.start()

    @pl.when(step < EXPERTS)
    def _():
        first = pl.multiple_of(step * CAP, 8)
        slot = lax.broadcasted_iota(jnp.int32, (CAP, LN), 0) + first

        def fill(i, c):
            t0 = pl.multiple_of(i * LN, LN)
            held = (tgt_row[0:1, pl.ds(t0, LN)] == slot) | (tgt_row[1:2, pl.ds(t0, LN)] == slot)
            mask[:, pl.ds(t0, LN)] = jnp.where(held, 1.0, 0.0).astype(BF16)
            return c

        lax.fori_loop(0, tok // LN, fill, 0)
        rows = dot(mask[...], cot[...], 1, 0).astype(BF16)
        y[...] = rows
        h = dot(rows, wdn[0], 1, 1)
        g, u = gate[0], up[0]
        g2 = g * g
        t = jnp.tanh(GC * (g + 0.044715 * g2 * g))
        half = 0.5 * (1.0 + t)
        sgrow = jnp.sum(act[0].astype(F32) * h, axis=1, keepdims=True)
        da = sh[:, 0:1] * h
        slope = half + (0.5 * GC) * g * (1.0 - t * t) * (1.0 + (3 * 0.044715) * g2)
        dg = (da * u * slope).astype(BF16)
        du = (da * (g * half)).astype(BF16)
        dgu[0, 0] = dg
        dgu[0, 1] = du
        dxs[pl.ds(first, CAP), :] = (dot(dg, win[0, 0], 1, 0) + dot(du, win[0, 1], 1, 0)).astype(BF16)
        lane = lax.broadcasted_iota(jnp.int32, (CAP, LN), 1)
        high = sgrow.astype(BF16).astype(F32)
        low = jnp.where(lane == 2 * step + 1, sgrow - high, 0.0)
        aux[pl.ds(first, CAP), :] = jnp.where(lane == 2 * step, high, low).astype(BF16)

    @pl.when(step >= EXPERTS)
    def _():
        t0 = pl.multiple_of((step - EXPERTS) * chunk, chunk)
        span = 4 * CAP
        slots = lax.broadcasted_iota(jnp.int32, (chunk, span), 1)
        one, two = tgt_col[pl.ds(t0, chunk), 0:1], tgt_col[pl.ds(t0, chunk), 1:2]
        rows = jnp.zeros((chunk, cot.shape[1]), F32)
        value = jnp.zeros((chunk, LN), F32)
        for s0 in range(0, SLOTS, span):
            held = (one - s0 == slots) | (two - s0 == slots)
            both = jnp.where(held, 1.0, 0.0).astype(BF16)
            rows = rows + dot(both, dxs[s0:s0 + span, :], 1, 0)
            value = value + dot(both, aux[s0:s0 + span, :], 1, 0)
        mi[...] = rows
        lane = lax.broadcasted_iota(jnp.int32, (chunk, LN), 1)
        low = lax.div(lane, 2) * CAP
        sums = [jnp.sum(jnp.where((c >= low) & (c < low + CAP), value, 0.0), axis=1, keepdims=True) for c in (one, two)]
        sg[...] = jnp.where(lane == 0, sums[0], sums[1])

    def done_a(p, value):
        row, n = ring.pieces[p]
        res[pl.ds(row, n), :] = value + hid[pl.ds(row, n), :]

    def done_b(value):
        res[pl.ds(ring.rows_a, ring.rows_b), :] = value + hid[pl.ds(ring.rows_a, ring.rows_b), :]

    on_steps(step, reduce.events(done_a, done_b), share, last)

    @pl.when(step == last)
    def _():
        reduce.finish()


def experts_backward(tgt, cot, sh, gate, up, act, win, wdn, part, hid, n, cid, chunk=256, share=(1.4, 0.65)):
    tok, width = part.shape
    ff = wdn.shape[1]
    ring = Ring(n, tok // n)
    mid = by_expert((1, CAP, ff))
    tgt_row = tgt.reshape(2, tok)

    def by_chunk(lanes):
        return pl.BlockSpec((chunk, lanes), lambda i: (jnp.maximum(i - EXPERTS, 0), 0))

    return pl.pallas_call(
        functools.partial(backward_kernel, tok, chunk, ring, share),
        grid=(EXPERTS + tok // chunk,),
        in_specs=[whole(cot.shape), whole((2, tok)), whole((tok, 2)), by_expert((CAP, LN)), mid, mid, mid,
                  by_expert((1, 2, ff, width)), by_expert((1, ff, width)), whole(part.shape), whole(hid.shape)],
        out_specs=[by_expert((CAP, width)), by_expert((1, 2, CAP, ff)), by_chunk(width), by_chunk(LN),
                   pl.BlockSpec(hid.shape, lambda i: (0, 0))],
        scratch_shapes=[pltpu.VMEM((SLOTS, width), BF16), pltpu.VMEM((SLOTS, LN), BF16), pltpu.VMEM((CAP, tok), BF16)]
        + ring.reduce_scratch(width),
        out_shape=[jax.ShapeDtypeStruct((SLOTS, width), BF16), jax.ShapeDtypeStruct((EXPERTS, 2, CAP, ff), BF16),
                   jax.ShapeDtypeStruct((tok, width), F32), jax.ShapeDtypeStruct((tok, LN), F32),
                   jax.ShapeDtypeStruct(hid.shape, F32)],
        compiler_params=params(cid, 63 << 20),
        cost_estimate=wire(90),
        name="experts_backward",
    )(cot, tgt_row, tgt_row.T, sh, gate, up, act, win, wdn, part, hid)


def exclusive_or(a, b, bound):
    value, bit = 0, 1
    while bit < bound:
        value = value + lax.rem(lax.div(a, bit) + lax.div(b, bit), 2) * bit
        bit *= 2
    return value


def weights_kernel(parts, ring, n, share, x, y, sh, act, dgu, part, small, keep, give, out, small_out,
                   kept, gave, got, g_send, g_recv, sw_got, sw_send, sw_recv, *scratch):
    step = pl.program_id(0)
    dp = lax.axis_index("dp")
    mine = lax.rem(dp, 2)
    upper = lax.div(dp, 2)
    blocks = parts // 2
    half = blocks // 2
    ring.place()
    reduce = Reduce(ring, part, scratch)
    swap = Swap("tensor", n, lambda p: small.at[p], sw_got, sw_send, sw_recv)

    def to_partner(slot):
        return pltpu.make_async_remote_copy(
            src_ref=gave.at[slot], dst_ref=got.at[slot], send_sem=g_send.at[slot], recv_sem=g_recv.at[slot],
            device_id={"dp": dp + 1 - 2 * mine}, device_id_type=MESH)

    @pl.when(step == 0)
    def _():
        ring.barrier(everyone=True, others=[{"dp": dp + 1 - 2 * mine}])
        swap.start()
        reduce.start()

    @pl.when(step >= 1)
    def _():
        slot = lax.rem(step + 1, 2)
        to_partner(slot).wait()
        for q in range(blocks):
            to = exclusive_or(q, upper, blocks)

            @pl.when(to < half)
            def _():
                keep[to, 0] = kept[slot, q] + got[slot, q]

            @pl.when(to >= half)
            def _():
                give[to - half, 0] = kept[slot, q] + got[slot, q]

    @pl.when(step < EXPERTS)
    def _():
        slot = lax.rem(step, 2)
        og = (y[...].astype(F32) * sh[:, 0:1]).astype(BF16)
        wide = x.shape[1] // parts
        grads = [dot(dgu[0, 0], x[...], 0, 0), dot(dgu[0, 1], x[...], 0, 0), dot(act[0], og, 0, 0)]
        for bit in range(2):
            @pl.when(mine == bit)
            def _():
                for p in range(parts):
                    to = kept if p % 2 == bit else gave
                    for g in range(3):
                        to[slot, p // 2, g] = grads[g][:, p * wide:(p + 1) * wide]
        to_partner(slot).start()

    def done_a(p, value):
        row, count = ring.pieces[p]
        out[pl.ds(row, count), :] = value

    def done_b(value):
        out[pl.ds(ring.rows_a, ring.rows_b), :] = value

    on_steps(step, reduce.events(done_a, done_b), share, EXPERTS)

    @pl.when(step == EXPERTS)
    def _():
        small_out[...] = swap.total()
        reduce.finish()


def experts_weights(x, y, sh, act, dgu, part, small, n, parts, cid, share=(1.3, 0)):
    tok, width = part.shape
    ff = act.shape[2]
    wide = width // parts
    ring = Ring(n, tok // n)
    half = parts // 4
    o_w = jax.ShapeDtypeStruct((half, EXPERTS, 3, ff, wide), F32)
    b_w = pl.BlockSpec((half, 1, 3, ff, wide), lambda i, *t: (0, jnp.maximum(i - 1, 0), 0, 0, 0))
    slots = pltpu.VMEM((2, parts // 2, 3, ff, wide), F32)
    dma = pltpu.SemaphoreType.DMA
    return pl.pallas_call(
        functools.partial(weights_kernel, parts, ring, n, share),
        grid=(EXPERTS + 1,),
        in_specs=[by_expert((CAP, width)), by_expert((CAP, width)), by_expert((CAP, LN)),
                  by_expert((1, CAP, ff)), by_expert((1, 2, CAP, ff)), whole(part.shape), whole(small.shape)],
        out_specs=[b_w, b_w, pl.BlockSpec((tok // n, width), lambda i: (0, 0)),
                   pl.BlockSpec(small.shape[1:], lambda i: (0, 0))],
        scratch_shapes=[slots, slots, slots, dma((2,)), dma((2,))]
        + Swap.scratch(n, small.shape[1:]) + ring.reduce_scratch(width),
        out_shape=[o_w, o_w, jax.ShapeDtypeStruct((tok // n, width), F32), jax.ShapeDtypeStruct(small.shape[1:], F32)],
        compiler_params=params(cid, 63 << 20),
        cost_estimate=wire(90),
        name="experts_weights",
    )(x, y, sh, act, dgu, part, small)


def slot_targets(routes, order):
    tok = routes.shape[0]
    pos = jnp.arange(tok, dtype=jnp.int32)
    rank = jnp.sum(jnp.where(order[:, None] == pos[None, :], pos[:, None], 0), axis=0)
    earlier = (rank[:, None] > rank[None, :]).astype(BF16)
    ex = jnp.arange(EXPERTS, dtype=jnp.int32)
    onehot = (routes[:, :, None] == ex[None, None, :]).astype(BF16)
    before = dot(earlier, onehot.reshape(tok, 2 * EXPERTS), 1, 0).reshape(tok, 2, EXPERTS)
    first = jnp.sum(onehot[:, 0].astype(F32), axis=0)
    before = before + jnp.stack([jnp.zeros((EXPERTS,), F32), first])[None]
    slot = jnp.sum(before * onehot.astype(F32), axis=2).astype(jnp.int32)
    held = jnp.minimum(jnp.sum(onehot.astype(F32), axis=(0, 1)), CAP).astype(jnp.int32)
    return jnp.where(slot < CAP, routes * CAP + slot, SLOTS).T.reshape(-1), held


EPSILON = 1e-06
PRECISE = lax.Precision.HIGHEST


def rms_norm(values, gain):
    return values * lax.rsqrt(jnp.mean(values * values, axis=-1, keepdims=True) + EPSILON) * gain


def rms_back(values, gain, grad):
    rr = lax.rsqrt(jnp.mean(values * values, axis=-1, keepdims=True) + EPSILON)
    scaled = gain * grad
    back = rr * scaled - values * (rr * rr * rr) * jnp.mean(scaled * values, axis=-1, keepdims=True)
    return back, jnp.sum(grad * values * rr, axis=0)


def make_shards(mesh):
    n_tensor = mesh.shape["tensor"]
    n_dp = mesh.shape["dp"]

    def layer(tokens, cotangent, gain_attn, gain_moe, w_qkv, w_out, rel_bias, w_router, w_in, w_down,
              segment_ids, routes, order):
        tok, width = tokens.shape
        lanes = w_qkv.shape[2]
        share_rows = tok // n_tensor
        row0 = lax.axis_index("tensor") * share_rows

        def halve(keep, give):
            while True:
                blocks = keep.shape[0]
                came = lax.ppermute(give, "dp", [(d, d ^ (2 * blocks)) for d in range(n_dp)])
                if blocks == 1:
                    return keep[0], came[0]
                a = keep + came
                keep, give = a[:blocks // 2], a[blocks // 2:]

        def own(a):
            return lax.dynamic_slice_in_dim(a, row0, share_rows, 0)

        one = (order[0, 0] >= 0).astype(F32)
        w_out_cols = lax.dynamic_slice_in_dim(w_out, lax.axis_index("dp") * (width // n_dp), width // n_dp, 1).astype(F32)
        w_out_rows = lax.all_gather(w_out_cols, "tensor", axis=0, tiled=True)
        x = tokens.astype(F32)
        attn_input = rms_norm(x, gain_attn).astype(BF16)
        qkv = jnp.dot(attn_input, w_qkv.reshape(width, 3 * lanes), preferred_element_type=F32).astype(BF16)
        q, k, v = (qkv[:, i * lanes:(i + 1) * lanes] for i in range(3))
        rb = rel_bias.astype(F32).reshape(-1)
        attended = attention_fwd(q, k, v.T, segment_ids, rb)
        tgt, held = slot_targets(routes, order[0])

        attended, w_out_rows, tgt, held = lax.optimization_barrier((attended, w_out_rows, tgt, held))
        w_out_all = lax.all_gather(w_out_rows, "dp", axis=1, tiled=True) * one
        attended_all = gather_columns(attended, n_tensor, 0)
        hidden_one = x + jnp.dot(attended_all, w_out_all, preferred_element_type=F32)
        moe_input = rms_norm(hidden_one, gain_moe).astype(BF16)
        logits = jnp.dot(moe_input, w_router, preferred_element_type=F32)
        picked = (routes[:, :, None] == jnp.arange(EXPERTS, dtype=jnp.int32)[None, None, :]).astype(F32)

        def route(logit_rows, picked_rows):
            soft = jax.nn.softmax(logit_rows, axis=-1)
            chosen = jnp.sum(soft[:, None, :] * picked_rows, axis=-1)
            return soft, chosen, jnp.sum(chosen, axis=-1, keepdims=True)

        soft, chosen, both = route(logits, picked)
        pair_share = chosen / both
        w_in_t = jnp.swapaxes(w_in, 2, 3)
        share_rep = jnp.broadcast_to(pair_share.T.reshape(-1, 1), (2 * tok, LN))
        xs, slot_share, gate, up, act, moe_part = experts_forward(tgt, held, moe_input, share_rep, w_in_t, w_down)
        hidden_s = own(hidden_one)
        y, gate_up_grad, moe_in_part, share_part, result_s = experts_backward(
            tgt, cotangent, slot_share, gate, up, act, w_in_t, w_down, moe_part, hidden_s, n_tensor, 1)
        share_blocks = jnp.pad(share_part[:, :2].T.reshape(2, n_tensor, share_rows).transpose(1, 0, 2), ((0, 0), (0, 6), (0, 0)))
        keep, give, moe_in_sum, share_sum = experts_weights(
            xs, y, slot_share, act, gate_up_grad, moe_in_part, share_blocks, n_tensor, n_dp, 3)
        keep, came = halve(keep, give)
        share_grad = share_sum[0:2].T
        result_s, moe_in_sum = lax.optimization_barrier((result_s, moe_in_sum))
        result = lax.all_gather(result_s, "tensor", axis=0, tiled=True)

        soft_s, chosen_s, both_s, picked_s = own(soft), own(chosen), own(both), own(picked)
        chosen_grad = share_grad / both_s - jnp.sum(share_grad * chosen_s, axis=-1, keepdims=True) / (both_s * both_s)
        prob_grad = jnp.sum(chosen_grad[:, :, None] * picked_s, axis=1)
        logits_grad = soft_s * (prob_grad - jnp.sum(soft_s * prob_grad, axis=-1, keepdims=True))
        moe_input_s = own(moe_input)
        router_part = jnp.dot(moe_input_s.astype(F32).T, logits_grad, precision=PRECISE)
        moe_input_grad = moe_in_sum + jnp.dot(logits_grad, w_router.astype(F32).T, precision=PRECISE)
        norm_grad, gain_moe_part = rms_back(hidden_s, gain_moe, moe_input_grad)
        hidden_grad = own(cotangent).astype(F32) + norm_grad
        proj_grad = hidden_grad.astype(BF16)
        att_grad_s = lax.dot_general(proj_grad, w_out_all.astype(BF16), (((1,), (1,)), ((), ())), preferred_element_type=F32)
        att_grad_s = att_grad_s.astype(BF16).astype(F32)
        pieces = att_grad_s.reshape(share_rows, n_tensor, lanes).transpose(1, 0, 2)
        attended_grad = lax.all_to_all(pieces, "tensor", 0, 0, tiled=False).reshape(tok, lanes)
        w_out_part = lax.dot_general(own(attended_all).astype(BF16), proj_grad, (((0,), (0,)), ((), ())), preferred_element_type=F32)

        qkv_grad, bias_part = attention_bwd(q, k, v, k.T, attended_grad, segment_ids, rb)
        attn_in_part = lax.dot_general(qkv_grad, w_qkv.reshape(width, 3 * lanes), (((1,), (1,)), ((), ())), preferred_element_type=F32)
        w_qkv_part = lax.dot_general(attn_input, qkv_grad, (((0,), (0,)), ((), ())), preferred_element_type=F32)

        heads = lanes // HD
        wide = width // n_dp
        bias_rows = bias_part[:, :, 0].reshape(heads, n_dp, NB // n_dp).transpose(1, 0, 2)
        bias_rows = jnp.pad(bias_rows, ((0, 0), (0, 0), (0, wide - NB // n_dp)))
        sums = jnp.concatenate([jnp.zeros((1, width), F32), gain_moe_part[None], router_part.T], axis=0)
        sums = sums.reshape(sums.shape[0], n_dp, wide).transpose(1, 0, 2)
        small = jnp.concatenate([sums, jnp.zeros((n_dp, -(sums.shape[1] + heads) % 8, wide), F32), bias_rows], axis=1)
        input_grad, small, w_qkv_grad, w_out_grad = reduce_norm_gather(
            attn_in_part, own(tokens).astype(F32), hidden_grad, gain_attn, small, heads, w_qkv_part, w_out_part, n_tensor, n_dp, 2)

        small, keep = lax.optimization_barrier((small, keep))
        w_in_grad = jnp.swapaxes(keep[:, :2] + came[:, :2], 2, 3)
        w_down_grad = keep[:, 2] + came[:, 2]
        w_qkv_grad = w_qkv_grad.reshape(width // n_dp, 3, lanes)
        rel_bias_grad = small[small.shape[0] - heads:, :NB // n_dp].T
        return (result, input_grad, small[0], small[1], w_qkv_grad, w_out_grad, rel_bias_grad,
                small[2:2 + EXPERTS].T, w_in_grad, w_down_grad)

    return layer


def solution(mesh):
    return jax.shard_map(
        make_shards(mesh),
        mesh=mesh,
        in_specs=(
            P("dp", None),
            P("dp", None),
            P(),
            P(),
            P(None, None, "tensor"),
            P("tensor", None),
            P(None, "tensor"),
            P(),
            P(None, None, None, "tensor"),
            P(None, "tensor", None),
            P("dp", None),
            P("dp", None),
            P("dp", None),
        ),
        out_specs=(
            P("dp", None),
            P("dp", None),
            P("dp"),
            P("dp"),
            P("dp", None, "tensor"),
            P("tensor", "dp"),
            P("dp", "tensor"),
            P("dp", None),
            P(None, None, "dp", "tensor"),
            P(None, "tensor", "dp"),
        ),
        check_vma=False,
    )
```

```python
import functools
import math

import jax
import jax.numpy as jnp
import numpy as np
from jax import lax
from jax.experimental import pallas as pl
from jax.experimental.pallas import tpu as pltpu
from jax.sharding import PartitionSpec as P


F32 = jnp.float32
BF16 = jnp.bfloat16


def dot(a, b, ca, cb):
    return lax.dot_general(a, b, (((ca,), (cb,)), ((), ())), preferred_element_type=F32)


NB=32; MAXDIST=128; HD=64; NEG=-1000000000.0


def thresholds(bucket_count, reach):
    half_count = bucket_count // 2
    exact_count = half_count // 2
    listing = []
    for bucket_level in range(1, half_count):
        if bucket_level <= exact_count:
            listing.append(bucket_level)
        else:
            distance = exact_count
            while (exact_count + int(np.floor(np.log(distance / exact_count) / np.log(reach / exact_count) * (half_count - exact_count))) < bucket_level):
                distance += 1
            listing.append(distance)
    return listing


THRESH = thresholds(NB, MAXDIST)
HALF = NB // 2
CH = 128


def distance(row0, rows, cols, origin):
    r = lax.broadcasted_iota(jnp.int32, (rows, cols), 0)
    c = lax.broadcasted_iota(jnp.int32, (rows, cols), 1)
    return r + (row0 - origin) - c


def build_bias(rb_ref, bias, heads, length, block):
    total = 2 * length - block
    origin = length - block
    low_end = (origin - THRESH[-1] + 1) // CH * CH
    high_start = -(-(origin + block - 1 + THRESH[-1]) // CH) * CH
    for h in range(heads):
        bias[h, 0:low_end, :] = jnp.full((low_end, block), rb_ref[(HALF - 1) * heads + h], F32)
        bias[h, high_start:total, :] = jnp.full((total - high_start, block), rb_ref[(NB - 1) * heads + h], F32)

        def chunk(i, carry):
            row0 = pl.multiple_of(low_end + i * CH, CH)
            d = distance(row0, CH, block, origin)
            mag = jnp.abs(d)
            back = jnp.full((CH, block), rb_ref[h], F32)
            ahead = jnp.full((CH, block), rb_ref[HALF * heads + h], F32)
            for level, t in enumerate(THRESH):
                far = mag >= t
                back = jnp.where(far, rb_ref[(level + 1) * heads + h], back)
                ahead = jnp.where(far, rb_ref[(HALF + level + 1) * heads + h], ahead)
            bias[h, pl.ds(row0, CH), :] = jnp.where(d > 0, ahead, back)
            return carry

        lax.fori_loop(0, (high_start - low_end) // CH, chunk, 0)


def fwd_kernel(heads, length, block, rb_ref, q_ref, k_ref, vt_ref, segr_ref, segc_ref, o_ref, bias):
    @pl.when(pl.program_id(0) == 0)
    def _():
        build_bias(rb_ref, bias, heads, length, block)

    lanes = heads * HD
    lane = lax.broadcasted_iota(jnp.int32, (block, lanes), 1) // HD

    def step(i, carry):
        q0 = pl.multiple_of(i * block, block)
        start = pl.multiple_of(length - block - q0, block)
        qb = q_ref[pl.ds(q0, block), :] * 0.125
        same = segc_ref[...] == segr_ref[0, :, pl.ds(q0, block)]
        pieces = []
        for h in range(heads):
            qm = jnp.where(lane == h, qb, jnp.zeros_like(qb)) if heads > 1 else qb
            s = dot(k_ref[...], qm, 1, 1) + bias[h, pl.ds(start, length), :]
            s = jnp.where(same, s, NEG)
            p = jnp.exp(s - jnp.max(s, axis=0, keepdims=True))
            total = jnp.sum(p, axis=0, keepdims=True)
            p = (p * (1.0 / total)).astype(BF16)
            pieces.append(dot(vt_ref[h * HD:(h + 1) * HD, :], p, 1, 0))
        o = jnp.concatenate(pieces, axis=0) if heads > 1 else pieces[0]
        o_ref[pl.ds(q0, block), :] = o.T.astype(BF16).astype(F32)
        return carry

    lax.fori_loop(0, length // block, step, 0)


def bwd_kernel(heads, length, block, rb_ref, q_ref, k_ref, v_ref, kt_ref, do_ref, segr_ref, segc_ref,
               out_ref, db_ref, bias, dbias, dk, dv):
    step_id = pl.program_id(0)
    total_rows = 2 * length - block

    @pl.when(step_id == 0)
    def _():
        build_bias(rb_ref, bias, heads, length, block)
        dbias[...] = jnp.zeros_like(dbias)

    dk[...] = jnp.zeros_like(dk)
    dv[...] = jnp.zeros_like(dv)
    lanes = heads * HD
    lane = lax.broadcasted_iota(jnp.int32, (block, lanes), 1) // HD

    def step(i, carry):
        q0 = pl.multiple_of(i * block, block)
        start = pl.multiple_of(length - block - q0, block)
        qb = q_ref[pl.ds(q0, block), :] * 0.125
        dob = do_ref[pl.ds(q0, block), :].astype(BF16)
        same = segc_ref[...] == segr_ref[0, :, pl.ds(q0, block)]
        pieces = []
        for h in range(heads):
            qm = jnp.where(lane == h, qb, jnp.zeros_like(qb)) if heads > 1 else qb
            dom = jnp.where(lane == h, dob, jnp.zeros_like(dob)) if heads > 1 else dob
            s = dot(k_ref[...], qm, 1, 1) + bias[h, pl.ds(start, length), :]
            s = jnp.where(same, s, NEG)
            p = jnp.exp(s - jnp.max(s, axis=0, keepdims=True))
            p = p * (1.0 / jnp.sum(p, axis=0, keepdims=True))
            dp = dot(v_ref[...], dom, 1, 1)
            ds = (p * (dp - jnp.sum(p * dp, axis=0, keepdims=True))).astype(BF16)
            dbias[h, pl.ds(start, length), :] += ds.astype(F32)
            dk[...] += dot(ds, qm, 1, 0)
            dv[...] += dot(p.astype(BF16), dom, 1, 0)
            pieces.append(dot(kt_ref[h * HD:(h + 1) * HD, :], ds, 1, 0))
        dq = jnp.concatenate(pieces, axis=0) if heads > 1 else pieces[0]
        out_ref[pl.ds(q0, block), 0:lanes] = (dq * 0.125).T.astype(BF16)
        return carry

    lax.fori_loop(0, length // block, step, 0)
    out_ref[:, lanes:2 * lanes] = dk[...].astype(BF16)
    out_ref[:, 2 * lanes:] = dv[...].astype(BF16)

    @pl.when(step_id == pl.num_programs(0) - 1)
    def _():
        origin = length - block
        low_end = (origin - THRESH[-1] + 1) // CH * CH
        high_start = -(-(origin + block - 1 + THRESH[-1]) // CH) * CH

        def fold(x):
            return jnp.sum(x, axis=0, keepdims=True)

        for h in range(heads):
            def rows(lo, hi):
                def body(i, acc):
                    r0 = pl.multiple_of(lo + i * CH, CH)
                    return acc + fold(dbias[h, pl.ds(r0, CH), :])

                return lax.fori_loop(0, (hi - lo) // CH, body, jnp.zeros((1, block), F32))

            def chunk(i, sums):
                r0 = pl.multiple_of(low_end + i * CH, CH)
                g = dbias[h, pl.ds(r0, CH), :]
                d = distance(r0, CH, block, origin)
                mag = jnp.abs(d)
                gb = jnp.where(d > 0, 0.0, g)
                ga = jnp.where(d > 0, g, 0.0)
                out = [sums[0] + fold(gb), sums[HALF] + fold(ga)]
                tb, ta = [], []
                for t in THRESH:
                    far = mag >= t
                    tb.append(fold(jnp.where(far, gb, 0.0)))
                    ta.append(fold(jnp.where(far, ga, 0.0)))
                new = [out[0]] + [sums[1 + n] + tb[n] for n in range(HALF - 1)]
                new += [out[1]] + [sums[HALF + 1 + n] + ta[n] for n in range(HALF - 1)]
                return tuple(new)

            sums = lax.fori_loop(0, (high_start - low_end) // CH, chunk,
                                 tuple(jnp.zeros((1, block), F32) for _ in range(NB)))
            left, right = rows(0, low_end), rows(high_start, total_rows)
            for b in range(NB):
                val = sums[b]
                if b not in (HALF - 1, NB - 1):
                    val = val - sums[b + 1]
                else:
                    val = val + (left if b == HALF - 1 else right)
                db_ref[h, b:b + 1, :] = jnp.broadcast_to(jnp.sum(val, axis=1, keepdims=True), (1, 128))


def attention_fwd(q, k, vt, seg, rb, block=256):
    tok, lanes = q.shape
    seqs, length = seg.shape
    heads = lanes // HD
    full = pl.BlockSpec((length, lanes), lambda s: (s, 0))
    return pl.pallas_call(
        functools.partial(fwd_kernel, heads, length, block),
        grid=(seqs,),
        out_shape=jax.ShapeDtypeStruct((tok, lanes), F32),
        in_specs=[pl.BlockSpec(memory_space=pltpu.SMEM), full, full,
                  pl.BlockSpec((lanes, length), lambda s: (0, s)),
                  pl.BlockSpec((1, 1, length), lambda s: (s, 0, 0)),
                  pl.BlockSpec((length, 1), lambda s: (s, 0))],
        out_specs=full,
        scratch_shapes=[pltpu.VMEM((heads, 2 * length - block, block), F32)],
        compiler_params=pltpu.CompilerParams(vmem_limit_bytes=56 << 20),
        cost_estimate=pl.CostEstimate(flops=4 * tok * length * lanes, bytes_accessed=tok * lanes * 10, transcendentals=tok * length * heads),
        name="attn_fwd",
    )(rb, q, k, vt, seg.reshape(seqs, 1, length), seg.reshape(tok, 1))


def attention_bwd(q, k, v, kt, do, seg, rb, block=256):
    tok, lanes = q.shape
    seqs, length = seg.shape
    heads = lanes // HD
    full = pl.BlockSpec((length, lanes), lambda s: (s, 0))
    return pl.pallas_call(
        functools.partial(bwd_kernel, heads, length, block),
        grid=(seqs,),
        out_shape=(jax.ShapeDtypeStruct((tok, 3 * lanes), BF16), jax.ShapeDtypeStruct((heads, NB, 128), F32)),
        in_specs=[pl.BlockSpec(memory_space=pltpu.SMEM), full, full, full,
                  pl.BlockSpec((lanes, length), lambda s: (0, s)), full,
                  pl.BlockSpec((1, 1, length), lambda s: (s, 0, 0)),
                  pl.BlockSpec((length, 1), lambda s: (s, 0))],
        out_specs=(pl.BlockSpec((length, 3 * lanes), lambda s: (s, 0)), pl.BlockSpec((heads, NB, 128), lambda s: (0, 0, 0))),
        scratch_shapes=[pltpu.VMEM((heads, 2 * length - block, block), F32)] * 2
        + [pltpu.VMEM((length, lanes), F32)] * 2,
        compiler_params=pltpu.CompilerParams(vmem_limit_bytes=56 << 20),
        cost_estimate=pl.CostEstimate(flops=10 * tok * length * lanes, bytes_accessed=tok * lanes * 20, transcendentals=tok * length * heads),
        name="attn_bwd",
    )(rb, q, k, v, kt, do, seg.reshape(seqs, 1, length), seg.reshape(tok, 1))


MESH = pl.DeviceIdType.MESH


class Ring:
    def __init__(self, n, rows):
        self.n = n
        self.inner = 1
        while (self.inner * 2) ** 2 <= n:
            self.inner *= 2
        self.outer = n // self.inner
        self.rows = rows
        self.rows_b = max(rows // 8 // 8 * 8, 8)
        self.rows_a = rows - self.rows_b
        self.count = next(c for c in (4, 2, 1) if self.rows_a % (8 * c) == 0)
        self.piece = self.rows_a // self.count
        self.pieces = [(p * self.piece, self.piece) for p in range(self.count)]

    def place(self):
        self.me = me = lax.axis_index("tensor")
        self.o, self.i = lax.div(me, self.inner), lax.rem(me, self.inner)

    def shard(self, back, side=0):
        return (lax.rem(self.o - back + 2 * self.outer, self.outer) * self.inner
                + lax.rem(self.i - side + self.inner, self.inner))

    def barrier(self, everyone=False, others=()):
        if everyone:
            peers = [{"tensor": self.peer(j)} for j in range(1, self.n)]
        else:
            peers = [self.shard(-1)] + ([self.shard(1)] if self.outer > 2 else [])
            peers += [self.shard(0, j) for j in range(1, self.inner)]
            peers = [{"tensor": p} for p in peers]
        peers += list(others)
        sem = pltpu.get_barrier_semaphore()
        for peer in peers:
            pl.semaphore_signal(sem, inc=1, device_id=peer, device_id_type=MESH)
        pl.semaphore_wait(sem, len(peers))

    def peer(self, j):
        return lax.rem(self.me + j, self.n)

    def gather_semaphores(self):
        dma = pltpu.SemaphoreType.DMA
        one = [dma((self.outer - 1, self.count)), dma((self.inner - 1, self.outer, self.count)),
               dma((self.inner, self.outer - 1)), dma((self.inner - 1,))]
        return one + one

    def reduce_scratch(self, width):
        dma = pltpu.SemaphoreType.DMA
        one = [dma((self.inner - 1, self.outer, self.count)), dma((self.outer - 1, self.count)),
               dma((self.inner, self.outer - 1)), dma((self.inner - 1,))]
        return [pltpu.VMEM((self.inner - 1, self.outer, self.rows_a, width), F32),
                pltpu.VMEM((self.outer - 1, self.rows_a, width), F32),
                pltpu.VMEM((self.inner, self.outer - 1, self.rows_b, width), F32),
                pltpu.VMEM((self.inner - 1, self.rows_b, width), F32)] + one + one


def remote(src, dst, send, recv, peer):
    return pltpu.make_async_remote_copy(src_ref=src, dst_ref=dst, send_sem=send, recv_sem=recv,
                                        device_id={"tensor": peer}, device_id_type=MESH)


class Gather:
    def __init__(self, ring, view, own, sems):
        self.r, self.view, self.own = ring, view, own
        (self.s_oa, self.s_ia, self.s_ob, self.s_ib, self.r_oa, self.r_ia, self.r_ob, self.r_ib) = sems
        self.sent = []

    def outer_a(self, step, p):
        r = self.r
        row, rows = r.pieces[p]
        shard = r.shard(step)
        src = self.own(row, rows) if step == 0 else self.view(shard, row, rows)
        return remote(src, self.view(shard, row, rows), self.s_oa.at[step, p], self.r_oa.at[step, p], r.shard(-1))

    def inner_a(self, j, step, p):
        r = self.r
        row, rows = r.pieces[p]
        shard = r.shard(step)
        src = self.own(row, rows) if step == 0 else self.view(shard, row, rows)
        return remote(src, self.view(shard, row, rows), self.s_ia.at[j - 1, step, p], self.r_ia.at[j - 1, step, p],
                      r.shard(0, -j))

    def outer_b(self, j, step):
        r = self.r
        shard = r.shard(step, j)
        src = self.own(r.rows_a, r.rows_b) if step == 0 and j == 0 else self.view(shard, r.rows_a, r.rows_b)
        return remote(src, self.view(shard, r.rows_a, r.rows_b), self.s_ob.at[j, step], self.r_ob.at[j, step], r.shard(-1))

    def inner_b(self, j):
        r = self.r
        return remote(self.own(r.rows_a, r.rows_b), self.view(r.shard(0), r.rows_a, r.rows_b),
                      self.s_ib.at[j - 1], self.r_ib.at[j - 1], r.shard(0, -j))

    def go(self, copy):
        copy.start()
        self.sent.append(copy)

    def start_a(self, p):
        self.go(self.outer_a(0, p))
        for j in range(1, self.r.inner):
            self.go(self.inner_a(j, 0, p))

    def start_b(self):
        for j in range(1, self.r.inner):
            self.go(self.inner_b(j))
        self.go(self.outer_b(0, 0))

    def middle(self):
        r = self.r
        for j in range(1, r.inner):
            self.inner_b(j).wait_recv()
            self.go(self.outer_b(j, 0))
        for step in range(1, r.outer):
            for p in range(r.count):
                self.outer_a(step - 1, p).wait_recv()
                if step < r.outer - 1:
                    self.go(self.outer_a(step, p))
                for j in range(1, r.inner):
                    self.go(self.inner_a(j, step, p))
            for j in range(r.inner):
                self.outer_b(j, step - 1).wait_recv()
                if step < r.outer - 1:
                    self.go(self.outer_b(j, step))

    def finish(self):
        r = self.r
        for step in range(r.outer):
            for p in range(r.count):
                for j in range(1, r.inner):
                    self.inner_a(j, step, p).wait_recv()
        for copy in self.sent:
            copy.wait_send()


class Reduce:
    def __init__(self, ring, src, scratch):
        self.r, self.src = ring, src
        (self.ia, self.oa, self.ob, self.ib, self.s_ia, self.s_oa, self.s_ob, self.s_ib,
         self.r_ia, self.r_oa, self.r_ob, self.r_ib) = scratch
        self.sent = []

    def part(self, shard, row, rows):
        return self.src.at[pl.ds(pl.multiple_of(shard * self.r.rows + row, 8), rows), :]

    def inner_a(self, j, step, p):
        r = self.r
        row, rows = r.pieces[p]
        return remote(self.part(r.shard(step + 1, -j), row, rows), self.ia.at[j - 1, step, pl.ds(row, rows), :],
                      self.s_ia.at[j - 1, step, p], self.r_ia.at[j - 1, step, p], r.shard(0, -j))

    def outer_a(self, step, p):
        r = self.r
        row, rows = r.pieces[p]
        src = self.ia.at[0, 0, pl.ds(row, rows), :] if step == 0 else self.oa.at[step - 1, pl.ds(row, rows), :]
        return remote(src, self.oa.at[step, pl.ds(row, rows), :], self.s_oa.at[step, p], self.r_oa.at[step, p], r.shard(-1))

    def outer_b(self, j, step):
        r = self.r
        src = self.part(r.shard(1, j), r.rows_a, r.rows_b) if step == 0 else self.ob.at[j, step - 1]
        return remote(src, self.ob.at[j, step], self.s_ob.at[j, step], self.r_ob.at[j, step], r.shard(-1))

    def inner_b(self, j):
        r = self.r
        return remote(self.ob.at[j, r.outer - 2], self.ib.at[j - 1], self.s_ib.at[j - 1], self.r_ib.at[j - 1], r.shard(0, j))

    def go(self, make, *at):
        make(*at).start()
        self.sent.append((make, at))

    def start(self):
        r = self.r
        for j in range(r.inner):
            self.go(self.outer_b, j, 0)
        for step in range(r.outer):
            for p in range(r.count):
                for j in range(1, r.inner):
                    self.go(self.inner_a, j, step, p)

    def event_a(self, step, p, done_a):
        r = self.r
        last = step == r.outer - 1
        row, rows = r.pieces[p]
        for j in range(1, r.inner):
            self.inner_a(j, step, p).wait_recv()
        total = self.part(r.shard(step + 1), row, rows)[...]
        for j in range(1, r.inner):
            total = total + self.ia[j - 1, step, pl.ds(row, rows), :]
        if step == 0:
            self.ia[0, 0, pl.ds(row, rows), :] = total
        else:
            self.outer_a(step - 1, p).wait_recv()
            total = total + self.oa[step - 1, pl.ds(row, rows), :]
            if not last:
                self.oa[step - 1, pl.ds(row, rows), :] = total
        if last:
            done_a(p, total)
        else:
            self.go(self.outer_a, step, p)

    def event_b(self, step):
        r = self.r
        for j in range(r.inner):
            self.outer_b(j, step - 1).wait_recv()
            total = self.ob[j, step - 1] + self.part(r.shard(step + 1, j), r.rows_a, r.rows_b)[...]
            self.ob[j, step - 1] = total
            if step < r.outer - 1:
                self.go(self.outer_b, j, step)
            elif j > 0:
                self.go(self.inner_b, j)

    def last_b(self, done_b):
        total = self.ob[0, self.r.outer - 2]
        for j in range(1, self.r.inner):
            self.inner_b(j).wait_recv()
            total = total + self.ib[j - 1]
        done_b(total)

    def events(self, done_a, done_b):
        r = self.r
        todo = []
        for step in range(r.outer):
            for p in range(r.count):
                todo.append(functools.partial(self.event_a, step, p, done_a))
            if step >= 1:
                todo.append(functools.partial(self.event_b, step))
        return todo + [functools.partial(self.last_b, done_b)]

    def finish(self):
        for make, at in self.sent:
            make(*at).wait_send()


def on_steps(step, events, share, last):
    due, done, total = [], 0, 0.0
    for i in range(last):
        total += share[0] if i < 8 else share[1]
        due.append(min(int(total), len(events)))
    for i, upto in enumerate(due):
        if upto > done:
            @pl.when(step == i)
            def _():
                for event in events[done:upto]:
                    event()

            done = upto

    @pl.when(step == last)
    def _():
        for event in events[done:]:
            event()


def wire(us):
    return pl.CostEstimate(flops=0, bytes_accessed=us * 3_000_000, transcendentals=0)


def params(cid, vmem):
    return pltpu.CompilerParams(collective_id=cid, has_side_effects=True, vmem_limit_bytes=vmem)


def gather_columns(x, n, cid):
    rows, lanes = x.shape
    ring = Ring(n, rows)
    flat = lanes % 128 == 0

    def kernel(x_ref, out, *sems):
        ring.place()
        ring.barrier()

        def view(shard, row, count):
            if flat:
                return out.at[pl.ds(row, count), pl.ds(pl.multiple_of(shard * lanes, 128), lanes)]
            return out.at[shard, pl.ds(row, count), :]

        gather = Gather(ring, view, lambda row, count: x_ref.at[pl.ds(row, count), :], sems[:8])
        keep = pltpu.make_async_copy(x_ref, view(ring.shard(0), 0, rows), sems[8])
        gather.start_b()
        for p in range(ring.count):
            gather.start_a(p)
        keep.start()
        gather.middle()
        gather.finish()
        keep.wait()

    shape = (rows, n * lanes) if flat else (n, rows, lanes)
    out = pl.pallas_call(
        kernel,
        out_shape=jax.ShapeDtypeStruct(shape, F32),
        in_specs=[pl.BlockSpec(memory_space=pltpu.VMEM)],
        out_specs=pl.BlockSpec(memory_space=pl.ANY),
        scratch_shapes=ring.gather_semaphores() + [pltpu.SemaphoreType.DMA],
        compiler_params=params(cid, 60 << 20),
        cost_estimate=wire(90),
        name="gather_columns",
    )(x)
    return out if flat else out.transpose(1, 0, 2).reshape(rows, n * lanes)


class Swap:
    def __init__(self, axis, n, block, got, send, recv):
        self.axis, self.n, self.block, self.got, self.send, self.recv = axis, n, block, got, send, recv

    def copy(self, j):
        me = lax.axis_index(self.axis)
        peer = lax.rem(me + j, self.n)
        return pltpu.make_async_remote_copy(
            src_ref=self.block(peer), dst_ref=self.got.at[j - 1],
            send_sem=self.send.at[j - 1], recv_sem=self.recv.at[j - 1], device_id={self.axis: peer}, device_id_type=MESH)

    def start(self):
        for j in range(1, self.n):
            self.copy(j).start()

    def total(self):
        for j in range(1, self.n):
            self.copy(j).wait()
        value = self.block(lax.axis_index(self.axis))[...]
        for j in range(1, self.n):
            value = value + self.got[j - 1]
        return value

    @staticmethod
    def scratch(n, shape):
        return [pltpu.VMEM((n - 1,) + shape, F32), pltpu.SemaphoreType.DMA((n - 1,)), pltpu.SemaphoreType.DMA((n - 1,))]


def reduce_norm_gather(part, values, upper, gain, small, keep_rows, inner_w, outer_w, n, n_dp, cid):
    total, width = part.shape
    rows = total // n
    ring = Ring(n, rows)
    n_red = len(ring.reduce_scratch(width))
    wide = width // n_dp
    s_rows = small.shape[1]
    in_rows = inner_w.shape[0] // n_dp
    height = outer_w.shape[0]
    out_rows = height // n
    columns = wide % 128 == 0
    if not columns:
        outer_w = outer_w.reshape(height, n_dp, wide).transpose(1, 0, 2)
    swaps = [(n_dp, (s_rows, wide)), (n, (s_rows, wide)), (n_dp, (in_rows, inner_w.shape[1])),
             (n_dp, (height, wide)), (n, (out_rows, wide))]

    def kernel(part_ref, val_ref, up_ref, gain_ref, small_ref, in_ref, ou_ref, out, small_out, in_out, ou_out,
               piece, sm, sm2, ou2, gain_acc, keep_sem, *scratch):
        dp = lax.axis_index("dp")
        ring.place()
        ring.barrier(everyone=True, others=[{"dp": lax.rem(dp + j, n_dp)} for j in range(1, n_dp)])
        one = Swap("dp", n_dp, lambda p: sm.at[p], *scratch[:3])
        two = Swap("tensor", n, lambda p: sm2, *scratch[3:6])
        inner_sum = Swap("dp", n_dp, lambda p: in_ref.at[pl.ds(pl.multiple_of(p * in_rows, 8), in_rows), :], *scratch[6:9])
        ou_one = Swap("dp", n_dp, (lambda p: ou_ref.at[:, pl.ds(pl.multiple_of(p * wide, 128), wide)]) if columns
                      else (lambda p: ou_ref.at[p]), *scratch[9:12])
        ou_two = Swap("tensor", n, lambda p: ou2.at[pl.ds(pl.multiple_of(p * out_rows, 8), out_rows), :], *scratch[12:15])
        reduce = Reduce(ring, part_ref, scratch[15:15 + n_red])
        gather = Gather(ring, lambda shard, row, count: out.at[pl.ds(pl.multiple_of(shard * rows + row, 8), count), :],
                        lambda row, count: piece.at[pl.ds(row, count), :], scratch[15 + n_red:])
        reduce.start()
        ou_one.start()
        inner_sum.start()
        gain_acc[...] = jnp.zeros_like(gain_acc)
        sm[...] = small_ref[...]

        def back(row, count, grad):
            x = val_ref[pl.ds(row, count), :]
            rr = lax.rsqrt(jnp.mean(x * x, axis=1, keepdims=True) + EPSILON)
            scaled = gain_ref[...] * grad
            inner = jnp.mean(scaled * x, axis=1, keepdims=True)
            piece[pl.ds(row, count), :] = up_ref[pl.ds(row, count), :] + rr * scaled - x * (rr * rr * rr * inner)
            gain_acc[...] += jnp.sum(grad * x * rr, axis=0, keepdims=True)

        def done_a(p, value):
            row, count = ring.pieces[p]
            back(row, count, value)
            gather.start_a(p)

        def done_b(value):
            back(ring.rows_a, ring.rows_b, value)
            gather.start_b()

        for event in reduce.events(done_a, done_b):
            event()
        keep = pltpu.make_async_copy(piece, out.at[pl.ds(pl.multiple_of(ring.shard(0) * rows, 8), rows), :], keep_sem)
        keep.start()
        for p in range(n_dp):
            sm[p, 0:1, :] = gain_acc[:, p * wide:(p + 1) * wide]
        one.start()
        ou2[...] = ou_one.total()
        ou_two.start()
        gather.middle()
        sm2[...] = one.total()
        two.start()
        in_out[...] = inner_sum.total()
        gather.finish()
        ou_out[...] = ou_two.total()
        both = two.total()
        last = lax.broadcasted_iota(jnp.int32, both.shape, 0) >= s_rows - keep_rows
        small_out[...] = jnp.where(last, sm2[...], both)
        reduce.finish()
        keep.wait()

    vm = pl.BlockSpec(memory_space=pltpu.VMEM)
    block = (s_rows, wide)
    return pl.pallas_call(
        kernel,
        out_shape=[jax.ShapeDtypeStruct(s, F32) for s in ((total, width), block, (in_rows, inner_w.shape[1]), (out_rows, wide))],
        in_specs=[vm] * 7,
        out_specs=[pl.BlockSpec(memory_space=pl.ANY), vm, vm, vm],
        scratch_shapes=[pltpu.VMEM((rows, width), F32), pltpu.VMEM((n_dp,) + block, F32), pltpu.VMEM(block, F32),
                        pltpu.VMEM((height, wide), F32), pltpu.VMEM((1, width), F32), pltpu.SemaphoreType.DMA]
        + [ref for swap in swaps for ref in Swap.scratch(*swap)]
        + ring.reduce_scratch(width) + ring.gather_semaphores(),
        compiler_params=params(cid, 48 << 20),
        cost_estimate=wire(180),
        name="reduce_norm_gather",
    )(part, values, upper, gain.reshape(1, width), small, inner_w, outer_w)


EXPERTS = 8
CAP = 576
SLOTS = EXPERTS * CAP
LN = 128
GC = math.sqrt(2.0 / math.pi)


def spread(dst, row0, sub, src, rows):
    for j in range(sub):
        dst[pl.ds(row0 * sub + j, rows, stride=sub), :] = src[:, j * LN:(j + 1) * LN].astype(F32)


def tile(ref, row, sub):
    return ref.at[pl.ds(pl.multiple_of(row * sub, sub), sub), :]


def combine_rows(tgt, rows, mix, out, tok, sub, t0, count):
    def body(i, c):
        for u in range(8):
            r = i * 8 + u
            one = rows[pl.ds(pl.multiple_of(tgt[t0 + r] * sub, sub), sub), :]
            two = rows[pl.ds(pl.multiple_of(tgt[tok + t0 + r] * sub, sub), sub), :]
            mix[pl.ds(pl.multiple_of(r * sub, sub), sub), :] = one + two
        return c

    lax.fori_loop(0, count // 8, body, 0)
    for j in range(sub):
        out[:, j * LN:(j + 1) * LN] = mix[pl.ds(j, count, stride=sub), :]


def by_expert(shape):
    return pl.BlockSpec(shape, lambda i, *t: (jnp.minimum(i, EXPERTS - 1),) + (0,) * (len(shape) - 1))


def whole(shape):
    return pl.BlockSpec(shape, lambda i, *t: (0,) * len(shape), pipeline_mode=pl.Buffered(1))


def forward_kernel(tok, sub, count, tgt, held, src, share, win, wdn, x, sh, gate, up, act, mo, rows_in, rows, shares, mix):
    step = pl.program_id(0)
    row0 = pl.multiple_of(step * CAP, 8)

    @pl.when(step == 0)
    def _():
        rows[SLOTS * sub:, :] = jnp.zeros((sub, LN), F32)

        def load(i, c):
            t0 = pl.multiple_of(i * 64, 64)
            spread(rows_in, t0, sub, src.at[pl.ds(t0, 64), :], 64)
            return c

        lax.fori_loop(0, tok // 64, load, 0)

        def move(i, c):
            for u in range(8):
                t = i * 8 + u
                row = tile(rows_in, t, sub)[...]
                for choice in range(2):
                    slot = tgt[choice * tok + t]
                    tile(rows, slot, sub)[...] = row
                    shares[pl.ds(slot, 1), :] = share[pl.ds(choice * tok + t, 1), :]
            return c

        lax.fori_loop(0, tok // 8, move, 0)
        rows[SLOTS * sub:, :] = jnp.zeros((sub, LN), F32)

        for e in range(EXPERTS):
            def clear(s, c):
                tile(rows, e * CAP + s, sub)[...] = jnp.zeros((sub, LN), F32)
                shares[pl.ds(e * CAP + s, 1), :] = jnp.zeros((1, LN), F32)
                return c

            lax.fori_loop(held[e], CAP, clear, 0)

    @pl.when(step < EXPERTS)
    def _():
        for j in range(sub):
            x[:, j * LN:(j + 1) * LN] = rows[pl.ds(row0 * sub + j, CAP, stride=sub), :].astype(BF16)
        sh[...] = shares[pl.ds(row0, CAP), :]
        g = dot(x[...], win[0, 0], 1, 1)
        u = dot(x[...], win[0, 1], 1, 1)
        gate[0] = g
        up[0] = u
        a = (0.5 * g * (1.0 + jnp.tanh(GC * (g + 0.044715 * (g * g * g)))) * u).astype(BF16)
        act[0] = a
        spread(rows, row0, sub, dot(a, wdn[0], 1, 0) * sh[:, 0:1], CAP)

    @pl.when(step >= EXPERTS)
    def _():
        combine_rows(tgt, rows, mix, mo, tok, sub, (step - EXPERTS) * count, count)


def experts_forward(tgt, held, src, share, win, wdn, count=256):
    tok, width = src.shape
    sub = width // LN
    ff = wdn.shape[1]
    mid = by_expert((1, CAP, ff))
    return pl.pallas_call(
        functools.partial(forward_kernel, tok, sub, count),
        grid_spec=pltpu.PrefetchScalarGridSpec(
            num_scalar_prefetch=2, grid=(EXPERTS + tok // count,),
            in_specs=[whole(src.shape), whole(share.shape), by_expert((1, 2, ff, width)), by_expert((1, ff, width))],
            out_specs=[by_expert((CAP, width)), by_expert((CAP, LN)), mid, mid, mid,
                       pl.BlockSpec((count, width), lambda i, *t: (jnp.maximum(i - EXPERTS, 0), 0))],
            scratch_shapes=[pltpu.VMEM((tok * sub, LN), F32), pltpu.VMEM(((SLOTS + 1) * sub, LN), F32),
                            pltpu.VMEM((SLOTS + 8, LN), F32), pltpu.VMEM((count * sub, LN), F32)]),
        out_shape=[jax.ShapeDtypeStruct((SLOTS, width), BF16), jax.ShapeDtypeStruct((SLOTS, LN), F32)]
        + [jax.ShapeDtypeStruct((EXPERTS, CAP, ff), F32)] * 2
        + [jax.ShapeDtypeStruct((EXPERTS, CAP, ff), BF16), jax.ShapeDtypeStruct((tok, width), F32)],
        compiler_params=pltpu.CompilerParams(vmem_limit_bytes=62 << 20),
        cost_estimate=pl.CostEstimate(flops=6 * SLOTS * width * ff, bytes_accessed=120 << 20, transcendentals=SLOTS * ff),
        name="experts_forward",
    )(tgt, held, src, share, win, wdn)


def backward_kernel(tok, chunk, ring, share, cot, tgt_row, tgt_col, sh, gate, up, act, win, wdn, part, hid,
                    y, dgu, mi, sg, res, dxs, aux, mask, *scratch):
    step = pl.program_id(0)
    last = EXPERTS + tok // chunk - 1
    ring.place()
    reduce = Reduce(ring, part, scratch)

    @pl.when(step == 0)
    def _():
        ring.barrier()
        reduce.start()

    @pl.when(step < EXPERTS)
    def _():
        first = pl.multiple_of(step * CAP, 8)
        slot = lax.broadcasted_iota(jnp.int32, (CAP, LN), 0) + first

        def fill(i, c):
            t0 = pl.multiple_of(i * LN, LN)
            held = (tgt_row[0:1, pl.ds(t0, LN)] == slot) | (tgt_row[1:2, pl.ds(t0, LN)] == slot)
            mask[:, pl.ds(t0, LN)] = jnp.where(held, 1.0, 0.0).astype(BF16)
            return c

        lax.fori_loop(0, tok // LN, fill, 0)
        rows = dot(mask[...], cot[...], 1, 0).astype(BF16)
        y[...] = rows
        h = dot(rows, wdn[0], 1, 1)
        g, u = gate[0], up[0]
        g2 = g * g
        t = jnp.tanh(GC * (g + 0.044715 * g2 * g))
        half = 0.5 * (1.0 + t)
        sgrow = jnp.sum(act[0].astype(F32) * h, axis=1, keepdims=True)
        da = sh[:, 0:1] * h
        slope = half + (0.5 * GC) * g * (1.0 - t * t) * (1.0 + (3 * 0.044715) * g2)
        dg = (da * u * slope).astype(BF16)
        du = (da * (g * half)).astype(BF16)
        dgu[0, 0] = dg
        dgu[0, 1] = du
        dxs[pl.ds(first, CAP), :] = (dot(dg, win[0, 0], 1, 0) + dot(du, win[0, 1], 1, 0)).astype(BF16)
        lane = lax.broadcasted_iota(jnp.int32, (CAP, LN), 1)
        high = sgrow.astype(BF16).astype(F32)
        low = jnp.where(lane == 2 * step + 1, sgrow - high, 0.0)
        aux[pl.ds(first, CAP), :] = jnp.where(lane == 2 * step, high, low).astype(BF16)

    @pl.when(step >= EXPERTS)
    def _():
        t0 = pl.multiple_of((step - EXPERTS) * chunk, chunk)
        span = 4 * CAP
        slots = lax.broadcasted_iota(jnp.int32, (chunk, span), 1)
        one, two = tgt_col[pl.ds(t0, chunk), 0:1], tgt_col[pl.ds(t0, chunk), 1:2]
        rows = jnp.zeros((chunk, cot.shape[1]), F32)
        value = jnp.zeros((chunk, LN), F32)
        for s0 in range(0, SLOTS, span):
            held = (one - s0 == slots) | (two - s0 == slots)
            both = jnp.where(held, 1.0, 0.0).astype(BF16)
            rows = rows + dot(both, dxs[s0:s0 + span, :], 1, 0)
            value = value + dot(both, aux[s0:s0 + span, :], 1, 0)
        mi[...] = rows
        lane = lax.broadcasted_iota(jnp.int32, (chunk, LN), 1)
        low = lax.div(lane, 2) * CAP
        sums = [jnp.sum(jnp.where((c >= low) & (c < low + CAP), value, 0.0), axis=1, keepdims=True) for c in (one, two)]
        sg[...] = jnp.where(lane == 0, sums[0], sums[1])

    def done_a(p, value):
        row, n = ring.pieces[p]
        res[pl.ds(row, n), :] = value + hid[pl.ds(row, n), :]

    def done_b(value):
        res[pl.ds(ring.rows_a, ring.rows_b), :] = value + hid[pl.ds(ring.rows_a, ring.rows_b), :]

    on_steps(step, reduce.events(done_a, done_b), share, last)

    @pl.when(step == last)
    def _():
        reduce.finish()


def experts_backward(tgt, cot, sh, gate, up, act, win, wdn, part, hid, n, cid, chunk=256, share=(1.2, 0.8)):
    tok, width = part.shape
    ff = wdn.shape[1]
    ring = Ring(n, tok // n)
    mid = by_expert((1, CAP, ff))
    tgt_row = tgt.reshape(2, tok)

    def by_chunk(lanes):
        return pl.BlockSpec((chunk, lanes), lambda i: (jnp.maximum(i - EXPERTS, 0), 0))

    return pl.pallas_call(
        functools.partial(backward_kernel, tok, chunk, ring, share),
        grid=(EXPERTS + tok // chunk,),
        in_specs=[whole(cot.shape), whole((2, tok)), whole((tok, 2)), by_expert((CAP, LN)), mid, mid, mid,
                  by_expert((1, 2, ff, width)), by_expert((1, ff, width)), whole(part.shape), whole(hid.shape)],
        out_specs=[by_expert((CAP, width)), by_expert((1, 2, CAP, ff)), by_chunk(width), by_chunk(LN),
                   pl.BlockSpec(hid.shape, lambda i: (0, 0))],
        scratch_shapes=[pltpu.VMEM((SLOTS, width), BF16), pltpu.VMEM((SLOTS, LN), BF16), pltpu.VMEM((CAP, tok), BF16)]
        + ring.reduce_scratch(width),
        out_shape=[jax.ShapeDtypeStruct((SLOTS, width), BF16), jax.ShapeDtypeStruct((EXPERTS, 2, CAP, ff), BF16),
                   jax.ShapeDtypeStruct((tok, width), F32), jax.ShapeDtypeStruct((tok, LN), F32),
                   jax.ShapeDtypeStruct(hid.shape, F32)],
        compiler_params=params(cid, 63 << 20),
        cost_estimate=wire(90),
        name="experts_backward",
    )(cot, tgt_row, tgt_row.T, sh, gate, up, act, win, wdn, part, hid)


def exclusive_or(a, b, bound):
    value, bit = 0, 1
    while bit < bound:
        value = value + lax.rem(lax.div(a, bit) + lax.div(b, bit), 2) * bit
        bit *= 2
    return value


def weights_kernel(parts, ring, n, share, x, y, sh, act, dgu, part, small, keep, give, out, small_out,
                   kept, gave, got, g_send, g_recv, sw_got, sw_send, sw_recv, *scratch):
    step = pl.program_id(0)
    dp = lax.axis_index("dp")
    mine = lax.rem(dp, 2)
    upper = lax.div(dp, 2)
    blocks = parts // 2
    half = blocks // 2
    ring.place()
    reduce = Reduce(ring, part, scratch)
    swap = Swap("tensor", n, lambda p: small.at[p], sw_got, sw_send, sw_recv)

    def to_partner(slot):
        return pltpu.make_async_remote_copy(
            src_ref=gave.at[slot], dst_ref=got.at[slot], send_sem=g_send.at[slot], recv_sem=g_recv.at[slot],
            device_id={"dp": dp + 1 - 2 * mine}, device_id_type=MESH)

    @pl.when(step == 0)
    def _():
        ring.barrier(everyone=True, others=[{"dp": dp + 1 - 2 * mine}])
        swap.start()
        reduce.start()

    @pl.when(step >= 1)
    def _():
        slot = lax.rem(step + 1, 2)
        to_partner(slot).wait()
        for q in range(blocks):
            to = exclusive_or(q, upper, blocks)

            @pl.when(to < half)
            def _():
                keep[to, 0] = kept[slot, q] + got[slot, q]

            @pl.when(to >= half)
            def _():
                give[to - half, 0] = kept[slot, q] + got[slot, q]

    @pl.when(step < EXPERTS)
    def _():
        slot = lax.rem(step, 2)
        og = (y[...].astype(F32) * sh[:, 0:1]).astype(BF16)
        wide = x.shape[1] // parts
        grads = [dot(dgu[0, 0], x[...], 0, 0), dot(dgu[0, 1], x[...], 0, 0), dot(act[0], og, 0, 0)]
        for bit in range(2):
            @pl.when(mine == bit)
            def _():
                for p in range(parts):
                    to = kept if p % 2 == bit else gave
                    for g in range(3):
                        to[slot, p // 2, g] = grads[g][:, p * wide:(p + 1) * wide]
        to_partner(slot).start()

    def done_a(p, value):
        row, count = ring.pieces[p]
        out[pl.ds(row, count), :] = value

    def done_b(value):
        out[pl.ds(ring.rows_a, ring.rows_b), :] = value

    on_steps(step, reduce.events(done_a, done_b), share, EXPERTS)

    @pl.when(step == EXPERTS)
    def _():
        small_out[...] = swap.total()
        reduce.finish()


def experts_weights(x, y, sh, act, dgu, part, small, n, parts, cid, share=(1.7, 0)):
    tok, width = part.shape
    ff = act.shape[2]
    wide = width // parts
    ring = Ring(n, tok // n)
    half = parts // 4
    o_w = jax.ShapeDtypeStruct((half, EXPERTS, 3, ff, wide), F32)
    b_w = pl.BlockSpec((half, 1, 3, ff, wide), lambda i, *t: (0, jnp.maximum(i - 1, 0), 0, 0, 0))
    slots = pltpu.VMEM((2, parts // 2, 3, ff, wide), F32)
    dma = pltpu.SemaphoreType.DMA
    return pl.pallas_call(
        functools.partial(weights_kernel, parts, ring, n, share),
        grid=(EXPERTS + 1,),
        in_specs=[by_expert((CAP, width)), by_expert((CAP, width)), by_expert((CAP, LN)),
                  by_expert((1, CAP, ff)), by_expert((1, 2, CAP, ff)), whole(part.shape), whole(small.shape)],
        out_specs=[b_w, b_w, pl.BlockSpec((tok // n, width), lambda i: (0, 0)),
                   pl.BlockSpec(small.shape[1:], lambda i: (0, 0))],
        scratch_shapes=[slots, slots, slots, dma((2,)), dma((2,))]
        + Swap.scratch(n, small.shape[1:]) + ring.reduce_scratch(width),
        out_shape=[o_w, o_w, jax.ShapeDtypeStruct((tok // n, width), F32), jax.ShapeDtypeStruct(small.shape[1:], F32)],
        compiler_params=params(cid, 63 << 20),
        cost_estimate=wire(90),
        name="experts_weights",
    )(x, y, sh, act, dgu, part, small)


def slot_targets(routes, order):
    tok = routes.shape[0]
    pos = jnp.arange(tok, dtype=jnp.int32)
    rank = jnp.sum(jnp.where(order[:, None] == pos[None, :], pos[:, None], 0), axis=0)
    earlier = (rank[:, None] > rank[None, :]).astype(BF16)
    ex = jnp.arange(EXPERTS, dtype=jnp.int32)
    onehot = (routes[:, :, None] == ex[None, None, :]).astype(BF16)
    before = dot(earlier, onehot.reshape(tok, 2 * EXPERTS), 1, 0).reshape(tok, 2, EXPERTS)
    first = jnp.sum(onehot[:, 0].astype(F32), axis=0)
    before = before + jnp.stack([jnp.zeros((EXPERTS,), F32), first])[None]
    slot = jnp.sum(before * onehot.astype(F32), axis=2).astype(jnp.int32)
    held = jnp.minimum(jnp.sum(onehot.astype(F32), axis=(0, 1)), CAP).astype(jnp.int32)
    return jnp.where(slot < CAP, routes * CAP + slot, SLOTS).T.reshape(-1), held


EPSILON = 1e-06
PRECISE = lax.Precision.HIGHEST


def rms_norm(values, gain):
    return values * lax.rsqrt(jnp.mean(values * values, axis=-1, keepdims=True) + EPSILON) * gain


def rms_back(values, gain, grad):
    rr = lax.rsqrt(jnp.mean(values * values, axis=-1, keepdims=True) + EPSILON)
    scaled = gain * grad
    back = rr * scaled - values * (rr * rr * rr) * jnp.mean(scaled * values, axis=-1, keepdims=True)
    return back, jnp.sum(grad * values * rr, axis=0)


def make_shards(mesh):
    n_tensor = mesh.shape["tensor"]
    n_dp = mesh.shape["dp"]

    def layer(tokens, cotangent, gain_attn, gain_moe, w_qkv, w_out, rel_bias, w_router, w_in, w_down,
              segment_ids, routes, order):
        tok, width = tokens.shape
        lanes = w_qkv.shape[2]
        share_rows = tok // n_tensor
        row0 = lax.axis_index("tensor") * share_rows

        def halve(keep, give):
            while True:
                blocks = keep.shape[0]
                came = lax.ppermute(give, "dp", [(d, d ^ (2 * blocks)) for d in range(n_dp)])
                if blocks == 1:
                    return keep[0], came[0]
                a = keep + came
                keep, give = a[:blocks // 2], a[blocks // 2:]

        def own(a):
            return lax.dynamic_slice_in_dim(a, row0, share_rows, 0)

        one = (order[0, 0] >= 0).astype(F32)
        w_out_cols = lax.dynamic_slice_in_dim(w_out, lax.axis_index("dp") * (width // n_dp), width // n_dp, 1).astype(F32)
        w_out_rows = lax.all_gather(w_out_cols, "tensor", axis=0, tiled=True)
        x = tokens.astype(F32)
        attn_input = rms_norm(x, gain_attn).astype(BF16)
        qkv = jnp.dot(attn_input, w_qkv.reshape(width, 3 * lanes), preferred_element_type=F32).astype(BF16)
        q, k, v = (qkv[:, i * lanes:(i + 1) * lanes] for i in range(3))
        rb = rel_bias.astype(F32).reshape(-1)
        attended = attention_fwd(q, k, v.T, segment_ids, rb, block=512)
        tgt, held = slot_targets(routes, order[0])

        attended, w_out_rows, tgt, held = lax.optimization_barrier((attended, w_out_rows, tgt, held))
        w_out_all = lax.all_gather(w_out_rows, "dp", axis=1, tiled=True) * one
        attended_all = gather_columns(attended, n_tensor, 0)
        hidden_one = x + jnp.dot(attended_all, w_out_all, preferred_element_type=F32)
        moe_input = rms_norm(hidden_one, gain_moe).astype(BF16)
        logits = jnp.dot(moe_input, w_router, preferred_element_type=F32)
        picked = (routes[:, :, None] == jnp.arange(EXPERTS, dtype=jnp.int32)[None, None, :]).astype(F32)

        def route(logit_rows, picked_rows):
            soft = jax.nn.softmax(logit_rows, axis=-1)
            chosen = jnp.sum(soft[:, None, :] * picked_rows, axis=-1)
            return soft, chosen, jnp.sum(chosen, axis=-1, keepdims=True)

        soft, chosen, both = route(logits, picked)
        pair_share = chosen / both
        w_in_t = jnp.swapaxes(w_in, 2, 3)
        share_rep = jnp.broadcast_to(pair_share.T.reshape(-1, 1), (2 * tok, LN))
        xs, slot_share, gate, up, act, moe_part = experts_forward(tgt, held, moe_input, share_rep, w_in_t, w_down)
        hidden_s = own(hidden_one)
        y, gate_up_grad, moe_in_part, share_part, result_s = experts_backward(
            tgt, cotangent, slot_share, gate, up, act, w_in_t, w_down, moe_part, hidden_s, n_tensor, 1)
        share_blocks = jnp.pad(share_part[:, :2].T.reshape(2, n_tensor, share_rows).transpose(1, 0, 2), ((0, 0), (0, 6), (0, 0)))
        keep, give, moe_in_sum, share_sum = experts_weights(
            xs, y, slot_share, act, gate_up_grad, moe_in_part, share_blocks, n_tensor, n_dp, 3)
        keep, came = halve(keep, give)
        share_grad = share_sum[0:2].T
        result_s, moe_in_sum = lax.optimization_barrier((result_s, moe_in_sum))
        result = lax.all_gather(result_s, "tensor", axis=0, tiled=True)

        soft_s, chosen_s, both_s, picked_s = own(soft), own(chosen), own(both), own(picked)
        chosen_grad = share_grad / both_s - jnp.sum(share_grad * chosen_s, axis=-1, keepdims=True) / (both_s * both_s)
        prob_grad = jnp.sum(chosen_grad[:, :, None] * picked_s, axis=1)
        logits_grad = soft_s * (prob_grad - jnp.sum(soft_s * prob_grad, axis=-1, keepdims=True))
        moe_input_s = own(moe_input)
        router_part = jnp.dot(moe_input_s.astype(F32).T, logits_grad, precision=PRECISE)
        moe_input_grad = moe_in_sum + jnp.dot(logits_grad, w_router.astype(F32).T, precision=PRECISE)
        norm_grad, gain_moe_part = rms_back(hidden_s, gain_moe, moe_input_grad)
        hidden_grad = own(cotangent).astype(F32) + norm_grad
        proj_grad = hidden_grad.astype(BF16)
        att_grad_s = lax.dot_general(proj_grad, w_out_all.astype(BF16), (((1,), (1,)), ((), ())), preferred_element_type=F32)
        att_grad_s = att_grad_s.astype(BF16).astype(F32)
        pieces = att_grad_s.reshape(share_rows, n_tensor, lanes).transpose(1, 0, 2)
        attended_grad = lax.all_to_all(pieces, "tensor", 0, 0, tiled=False).reshape(tok, lanes)
        w_out_part = lax.dot_general(own(attended_all).astype(BF16), proj_grad, (((0,), (0,)), ((), ())), preferred_element_type=F32)

        qkv_grad, bias_part = attention_bwd(q, k, v, k.T, attended_grad, segment_ids, rb)
        attn_in_part = lax.dot_general(qkv_grad, w_qkv.reshape(width, 3 * lanes), (((1,), (1,)), ((), ())), preferred_element_type=F32)
        w_qkv_part = lax.dot_general(attn_input, qkv_grad, (((0,), (0,)), ((), ())), preferred_element_type=F32)

        heads = lanes // HD
        wide = width // n_dp
        bias_rows = bias_part[:, :, 0].reshape(heads, n_dp, NB // n_dp).transpose(1, 0, 2)
        bias_rows = jnp.pad(bias_rows, ((0, 0), (0, 0), (0, wide - NB // n_dp)))
        sums = jnp.concatenate([jnp.zeros((1, width), F32), gain_moe_part[None], router_part.T], axis=0)
        sums = sums.reshape(sums.shape[0], n_dp, wide).transpose(1, 0, 2)
        small = jnp.concatenate([sums, jnp.zeros((n_dp, -(sums.shape[1] + heads) % 8, wide), F32), bias_rows], axis=1)
        input_grad, small, w_qkv_grad, w_out_grad = reduce_norm_gather(
            attn_in_part, own(tokens).astype(F32), hidden_grad, gain_attn, small, heads, w_qkv_part, w_out_part, n_tensor, n_dp, 2)

        small, keep = lax.optimization_barrier((small, keep))
        w_in_grad = jnp.swapaxes(keep[:, :2] + came[:, :2], 2, 3)
        w_down_grad = keep[:, 2] + came[:, 2]
        w_qkv_grad = w_qkv_grad.reshape(width // n_dp, 3, lanes)
        rel_bias_grad = small[small.shape[0] - heads:, :NB // n_dp].T
        return (result, input_grad, small[0], small[1], w_qkv_grad, w_out_grad, rel_bias_grad,
                small[2:2 + EXPERTS].T, w_in_grad, w_down_grad)

    return layer


def solution(mesh):
    return jax.shard_map(
        make_shards(mesh),
        mesh=mesh,
        in_specs=(
            P("dp", None),
            P("dp", None),
            P(),
            P(),
            P(None, None, "tensor"),
            P("tensor", None),
            P(None, "tensor"),
            P(),
            P(None, None, None, "tensor"),
            P(None, "tensor", None),
            P("dp", None),
            P("dp", None),
            P("dp", None),
        ),
        out_specs=(
            P("dp", None),
            P("dp", None),
            P("dp"),
            P("dp"),
            P("dp", None, "tensor"),
            P("tensor", "dp"),
            P("dp", "tensor"),
            P("dp", None),
            P(None, None, "dp", "tensor"),
            P(None, "tensor", "dp"),
        ),
        check_vma=False,
    )
```
